32 devices in a mesh: grp: 2 (over y), slab: 4 (over z), row: 2 (over x), col: 2 (over core).
Axes of the slice: x: 2, y: 2, z: 4, core: 2. Of those that a mesh axis runs over, the one named last changes fastest.
Arguments:
- image: float32 [3, 64, 32, 256], P(None, ('grp', 'slab'), 'row', 'col'), parts along dimension 1, may hold values from -28 to 28, as said below
- brain_mask: int32 [64, 32, 256], P(('grp', 'slab'), 'row', 'col'), parts along dimension 0, may hold values from 0 to 1, as said below
- labels: int32 [64, 32, 256], P(('grp', 'slab'), 'row', 'col'), parts along dimension 0, may hold values from 0 to 7
Outputs:
- posterior: bfloat16 [8, 64, 32, 256], P(None, ('grp', 'slab'), 'row', 'col'), parts along dimension 1
- bias_field: float32 [3, 64, 32, 256], P(None, ('grp', 'slab'), 'row', 'col'), parts along dimension 1
- class_means: float32 [16, 3], P('grp'), parts along dimension 0
The draws below stay inside these ranges and needn't reach their ends.
There are 2 independent parts, one for each index of `grp`. The reference program is written for one: setup_inputs(seed, part) draws one part's arguments, and reference() takes and returns one part's arrays. A program takes and returns all parts, laid end to end along the dimension named above; each array names one. Nothing has to cross between parts.
Inputs may be any that keep to these rules, and one draw needn't show every extreme that they name: `image`: log intensities of 3 modalities. `brain_mask`: 1 marks a brain cell, 0 a cell outside.
All inputs are finite; a program needn't handle non-finite values.
Results may differ from the reference program's by a relative error of at most 0.001.
Values sent between devices are 32-bit elements; how exact they have to be, the bound alone decides.
No kernel may reach another device: no remote copies, remote signals or barrier semaphores. Data moves between devices by JAX's collectives and lax.ppermute only.
A program may use at most 64 MiB of HBM per device.

```python
import math
import jax
import jax.numpy as jnp
from jax import lax

M = 3
K = 8
EM_ITERS = 2
MF_PASSES = 2
NS = 32
NR = 32
NC = 256


def class_draw(key):
    return jax.random.randint(jax.random.fold_in(key, 31), (NS, NR, NC), 0, K)


def draw_labels(key, part):
    return class_draw(key)


def draw_image(key, part):
    classes = class_draw(key)
    key_base = jax.random.fold_in(jax.random.fold_in(key, 11), 0)
    key_center = jax.random.fold_in(jax.random.fold_in(key, 11), 3)
    key_phase = jax.random.fold_in(jax.random.fold_in(key, 11), 4)
    extent = (M, NS, NR, NC)
    offsets = jnp.arange(M, dtype=jnp.float32).reshape(M, 1, 1, 1) * 0.5
    centers = jax.random.uniform(key_center, (K, M), jnp.float32, -2.0, 2.0)
    level = jnp.moveaxis(jnp.take(centers, classes, axis=0), 3, 0)
    phases = jax.random.uniform(key_phase, (M, 3), jnp.float32, -math.pi, math.pi)
    slab_pos = jnp.arange(NS, dtype=jnp.float32) / NS
    row_pos = jnp.arange(NR, dtype=jnp.float32) / NR
    col_pos = jnp.arange(NC, dtype=jnp.float32) / NC
    slab_wave = jnp.cos(2.0 * math.pi * slab_pos[None, :] + phases[:, 0:1])
    row_wave = jnp.cos(2.0 * math.pi * row_pos[None, :] + phases[:, 1:2])
    col_wave = jnp.cos(2.0 * math.pi * col_pos[None, :] + phases[:, 2:3])
    smooth = 0.7 * (slab_wave[:, :, None, None] + row_wave[:, None, :, None] + col_wave[:, None, None, :])
    return jnp.clip(jax.random.normal(key_base, extent, jnp.float32), -6.0, 6.0) + offsets + level + smooth


def draw_brain_mask(key, part):
    scores = jax.random.randint(jax.random.fold_in(key, 23), (NS, NR, NC), 0, 1000)
    levels = 250 + 650 * jnp.arange(NS, dtype=jnp.int32) // max(NS - 1, 1)
    return (scores < levels[:, None, None]).astype(jnp.int32)


def setup_inputs(seed: int = 0, part: int = 0) -> dict:
    splits = jax.random.split(jax.random.key(seed), 4)
    own_keys = jax.random.split(jax.random.fold_in(splits[3], part), 4)
    image = draw_image(jax.random.fold_in(jax.random.fold_in(splits[3], part), 71), part)
    brain_mask = draw_brain_mask(jax.random.fold_in(jax.random.fold_in(splits[3], part), 71), part)
    labels = draw_labels(jax.random.fold_in(jax.random.fold_in(splits[3], part), 71), part)
    return dict(image=image, brain_mask=brain_mask, labels=labels)


highest = lax.Precision.HIGHEST
coupling = 1.0
breadth = 8.0


def smooth_field(residual):
    spectrum = jnp.fft.fftn(residual, axes=(1, 2, 3))
    for axis_number, length in ((1, NS), (2, NR), (3, NC)):
        frequency = jnp.fft.fftfreq(length)
        response = jnp.exp(-2.0 * math.pi ** 2 * (length / breadth) ** 2 * frequency * frequency)
        target = [1, 1, 1, 1]
        target[axis_number] = length
        spectrum = spectrum * response.reshape(target)
    return jnp.real(jnp.fft.ifftn(spectrum, axes=(1, 2, 3))).astype(jnp.float32)


def neighbour_sum(belief):
    padded = jnp.pad(belief, ((0, 0), (1, 1), (1, 1), (1, 1)))
    total = padded[:, 2:, 1:-1, 1:-1] + padded[:, :-2, 1:-1, 1:-1]
    total = total + padded[:, 1:-1, 2:, 1:-1] + padded[:, 1:-1, :-2, 1:-1]
    total = total + padded[:, 1:-1, 1:-1, 2:] + padded[:, 1:-1, 1:-1, :-2]
    return total


def class_moments(belief, corrected):
    flat = belief.reshape(K, -1)
    values = corrected.reshape(M, -1)
    count = jnp.sum(flat, axis=1)
    first = jnp.dot(flat, values.T, precision=highest)
    means = first / (count + 1.0)[:, None]

    def one_class(inputs):
        weight, center = inputs
        offset = values - center[:, None]
        return jnp.sum(weight[None, :] * offset * offset, axis=1)

    spread = lax.map(one_class, (flat, means))
    variance = (spread + 1.0) / (count + 1.0)[:, None]
    return count, means, variance


def log_density(corrected, means, variance, prior):
    def one_class(inputs):
        center, scale, weight = inputs
        offset = corrected - center[:, None, None, None]
        terms = offset * offset / scale[:, None, None, None] + jnp.log(scale)[:, None, None, None]
        return jnp.log(weight) - 0.5 * jnp.sum(terms, axis=0)

    return lax.map(one_class, (means, variance, prior))


def reference(image, brain_mask, labels):
    inside = brain_mask.astype(jnp.float32)
    kinds = jnp.arange(K, dtype=jnp.int32)
    belief = (labels[None] == kinds[:, None, None, None]).astype(jnp.float32) * inside[None]
    bias_field = jnp.zeros_like(image)
    means = jnp.zeros((K, M), jnp.float32)
    for iteration in range(EM_ITERS):
        corrected = image - bias_field
        count, means, variance = class_moments(belief, corrected)
        prior = (count + 1.0) / (jnp.sum(count) + K)
        total = jnp.sum(belief, axis=0)
        removed = jnp.dot(means.T, belief.reshape(K, -1), precision=highest).reshape(image.shape)
        residual = image * total[None] - removed
        bias_field = smooth_field(residual)
        corrected = image - bias_field
        density = log_density(corrected, means, variance, prior)
        for sweep_index in range(MF_PASSES):
            belief = jax.nn.softmax(density + coupling * neighbour_sum(belief), axis=0) * inside[None]
    return belief.astype(jnp.bfloat16), bias_field, means
```

```python
import functools
import math

import jax
import jax.numpy as jnp
import numpy as np
from jax import lax
from jax.experimental import pallas as pl
from jax.experimental.pallas import tpu as pltpu
from jax.sharding import PartitionSpec as P

M = 3
K = 8
EM_ITERS = 2
MF_PASSES = 2


highest = lax.Precision.HIGHEST
coupling = 1.0
breadth = 8.0


def extended(cells, sides, width):
    for axis, dim in sides:
        count = lax.axis_size(axis)
        ends = count - 1
        head = lax.slice_in_dim(cells, 0, width, axis=dim)
        tail = lax.slice_in_dim(cells, cells.shape[dim] - width, cells.shape[dim], axis=dim)
        cells = jnp.concatenate(
            [
                lax.ppermute(tail, axis, [(i, (i + 1) % count) for i in range(ends)]),
                cells,
                lax.ppermute(head, axis, [((i + 1) % count, i) for i in range(ends)]),
            ],
            axis=dim,
        )
    return cells


def circulant(length):
    index = jnp.arange(length, dtype=jnp.int32)
    folded = jnp.minimum(index, length - index).astype(jnp.float32) / length
    response = jnp.exp(-2.0 * math.pi**2 * (length / breadth) ** 2 * folded * folded)
    product = index[:, None] * index[None, :] % length
    angles = 2.0 * math.pi / length * product.astype(jnp.float32)
    cosine = jnp.cos(angles)
    sine = jnp.sin(angles)
    even_part = jnp.dot(cosine * response[None, :], cosine.T, precision=highest)
    odd_part = jnp.dot(sine * response[None, :], sine.T, precision=highest)
    return (even_part + odd_part) / length


def neighbour_sum(belief):
    padded = extended(belief, (("slab", 1), ("row", 2), ("col", 3)), 1)
    total = padded[:, 2:, 1:-1, 1:-1] + padded[:, :-2, 1:-1, 1:-1]
    total = total + padded[:, 1:-1, 2:, 1:-1] + padded[:, 1:-1, :-2, 1:-1]
    total = total + padded[:, 1:-1, 1:-1, 2:] + padded[:, 1:-1, 1:-1, :-2]
    return total


def class_moments(belief, corrected):
    flat = belief.reshape(K, -1)
    values = corrected.reshape(M, -1)
    count, first, squares = lax.psum(
        (
            jnp.sum(flat, axis=1),
            jnp.dot(flat, values.T, precision=highest),
            jnp.dot(flat, (values * values).T, precision=highest),
        ),
        ("slab", "row", "col"),
    )
    means = first / (count + 1.0)[:, None]
    spread = squares - 2.0 * means * first + means * means * count[:, None]
    variance = (spread + 1.0) / (count + 1.0)[:, None]
    return (count, means, variance)


def log_density(corrected, means, variance, prior):
    offset = corrected[None] - means[:, :, None, None, None]
    terms = (
        offset * offset / variance[:, :, None, None, None]
        + jnp.log(variance)[:, :, None, None, None]
    )
    return jnp.log(prior)[:, None, None, None] - 0.5 * jnp.sum(terms, axis=1)


def smoothed(residual, column_local, row_table, slab_table):
    across = jnp.einsum(
        "msrc,cd->msrd",
        lax.all_gather(residual, "col", axis=3, tiled=True),
        column_local,
        precision=highest,
    )
    mixed = jnp.einsum(
        "msrc,rq->msqc",
        lax.all_to_all(across, "row", split_axis=1, concat_axis=2, tiled=True),
        row_table,
        precision=highest,
    )
    across = lax.all_to_all(mixed, "row", split_axis=2, concat_axis=1, tiled=True)
    mixed = jnp.einsum(
        "msrc,sq->mqrc",
        lax.all_to_all(across, "slab", split_axis=2, concat_axis=1, tiled=True),
        slab_table,
        precision=highest,
    )
    return lax.all_to_all(mixed, "slab", split_axis=1, concat_axis=2, tiled=True)


def general(image, brain_mask, labels):
    channels, slabs, rows, columns = image.shape
    inside = brain_mask.astype(jnp.float32)
    kinds = jnp.arange(K, dtype=jnp.int32)
    belief = (labels[None] == kinds[:, None, None, None]).astype(jnp.float32) * inside[None]
    column_table = circulant(columns * lax.axis_size("col"))
    column_local = lax.dynamic_slice_in_dim(
        column_table, lax.axis_index("col") * columns, columns, 1
    )
    row_table = circulant(rows * lax.axis_size("row"))
    slab_table = circulant(slabs * lax.axis_size("slab"))
    bias_field = jnp.zeros_like(image)
    means = jnp.zeros((K, channels), jnp.float32)
    for iteration in range(EM_ITERS):
        corrected = image - bias_field
        count, means, variance = class_moments(belief, corrected)
        prior = (count + 1.0) / (jnp.sum(count) + K)
        total = jnp.sum(belief, axis=0)
        removed = jnp.dot(means.T, belief.reshape(K, -1), precision=highest).reshape(image.shape)
        residual = image * total[None] - removed
        bias_field = smoothed(residual, column_local, row_table, slab_table)
        corrected = image - bias_field
        density = log_density(corrected, means, variance, prior)
        for sweep_index in range(MF_PASSES):
            belief = (
                jax.nn.softmax(density + coupling * neighbour_sum(belief), axis=0) * inside[None]
            )
    return (belief.astype(jnp.bfloat16), bias_field, means)


LANES = 128
SUB = 8
EDGE = 4
MARGIN = 8
STATS = 1 + 2 * M


def impulse(length):
    index = np.arange(length)
    folded = np.minimum(index, length - index) / length
    response = np.exp(-2.0 * np.pi**2 * (length / breadth) ** 2 * folded * folded)
    angles = 2.0 * np.pi / length * (index[:, None] * index[None, :] % length)
    return np.cos(angles) @ response / length


def dense(length):
    index = np.arange(length)
    return impulse(length)[(index[:, None] - index[None, :]) % length]


def dot(left, right, dims=((1,), (0,))):
    return lax.dot_general(
        left, right, (dims, ((), ())), precision=highest, preferred_element_type=jnp.float32
    )


def wide(row, shape=(SUB, LANES)):
    return jnp.broadcast_to(row, shape)


def stat_tile(sums):
    sub = lax.broadcasted_iota(jnp.int32, (SUB, LANES), 0)
    lane = lax.broadcasted_iota(jnp.int32, (SUB, LANES), 1)
    tile = jnp.zeros((SUB, LANES), jnp.float32)
    for q in range(STATS):
        rows = jnp.zeros((SUB, LANES), jnp.float32)
        for k in range(K):
            line = jnp.sum(sums[k][q], axis=0, keepdims=True)
            rows = jnp.where(sub == k, line, rows)
        tile = jnp.where(lane == q, jnp.sum(rows, axis=1, keepdims=True), tile)
    return tile


def fold(x):
    return jnp.sum(x.reshape(x.shape[0] // SUB, SUB, LANES), axis=0)


def class_stats(tile):
    count = tile[:, 0:1]
    means, halves = [], []
    shift = jnp.zeros_like(count)
    for m in range(M):
        first = tile[:, 1 + m : 2 + m]
        squares = tile[:, 1 + M + m : 2 + M + m]
        mean = first / (count + 1.0)
        spread = squares - 2.0 * mean * first + mean * mean * count
        variance = (spread + 1.0) / (count + 1.0)
        means.append(wide(mean))
        halves.append(wide(0.5 / variance))
        shift = shift - 0.5 * jnp.log(variance)
    prior = (count + 1.0) / (jnp.sum(count, axis=0, keepdims=True) + K)
    return means, halves, wide(jnp.log(prior) + shift)


def mean_rows(tile):
    return [wide(tile[:, 1 + m : 2 + m] / (tile[:, 0:1] + 1.0)) for m in range(M)]


def log_terms(corrected, means, halves, shift):
    out = []
    for k in range(K):
        total = wide(shift[k : k + 1, :], corrected[0].shape)
        for m in range(M):
            offset = corrected[m] - means[m][k : k + 1, :]
            total = total - offset * offset * halves[m][k : k + 1, :]
        out.append(total)
    return out


def soft(logits, inside):
    top = functools.reduce(jnp.maximum, logits)
    exps = [jnp.exp(x - top) for x in logits]
    scale = inside / functools.reduce(jnp.add, exps)
    return [x * scale for x in exps]


def prepare_kernel(own, oth, place, send, ext):
    window = send.shape[1] // (M + 1) // SUB * SUB
    peers = send.shape[0]
    step = LANES // peers
    first = jnp.full((SUB, LANES), place[2], jnp.int32) == 0
    for f in range(M + 1):
        blank = jnp.full((SUB, LANES), float(K) if f == M else 0.0, jnp.float32)
        other = oth[f].T
        ext[f, 0:MARGIN, :] = jnp.where(first, blank, other[LANES - MARGIN :, :])
        ext[f, MARGIN : MARGIN + LANES, :] = own[f].T
        ext[f, MARGIN + LANES :, :] = jnp.where(first, other[:MARGIN, :], blank)
    sums = []
    for k in range(K):
        line = [jnp.zeros((SUB, LANES), jnp.float32) for _ in range(STATS)]
        for ref in (own, oth):
            flag = (ref[M] == float(k)).astype(jnp.float32)
            line[0] = line[0] + fold(flag)
            for m in range(M):
                value = flag * ref[m]
                line[1 + m] = line[1 + m] + fold(value)
                line[1 + M + m] = line[1 + M + m] + fold(value * ref[m])
        sums.append(line)
    tile = stat_tile(sums)
    for p in range(peers):
        for f in range(M + 1):
            base = MARGIN - EDGE + step * p
            send[p, f * window : (f + 1) * window, :] = ext[f, base : base + window, :]
        send[p, (M + 1) * window :, :] = tile


def column_kernel(own, oth, got, table, send, flat, out):
    peers = send.shape[0]
    window = send.shape[1] // M
    step = LANES // peers
    tile = got[0, (M + 1) * window :, :]
    for j in range(1, peers):
        tile = tile + got[j, (M + 1) * window :, :]
    means = mean_rows(tile)
    for h, ref in enumerate((own, oth)):
        code = ref[M]
        flags = [code == float(k) for k in range(K)]
        for m in range(M):
            center = jnp.zeros_like(code)
            for k in range(K):
                center = jnp.where(flags[k], means[m][k : k + 1, :], center)
            flat[m * LANES : (m + 1) * LANES, h * LANES : (h + 1) * LANES] = jnp.where(
                code < float(K), ref[m] - center, 0.0
            )
    out[...] = dot(table[...], flat[...], ((1,), (1,)))
    for p in range(peers):
        base = MARGIN - EDGE + step * p
        for m in range(M):
            send[p, m * window : (m + 1) * window, :] = out[
                base : base + window, m * LANES : (m + 1) * LANES
            ]


def slab_row_filter(pieces, slab_table, row_table, first, second, grid):
    ns, nr = grid
    rows = pieces[0].shape[0]
    for sb in range(ns):
        for rb in range(nr):
            first[rb * rows : (rb + 1) * rows, sb * LANES : (sb + 1) * LANES] = pieces[sb * nr + rb]
    mixed = dot(first[...], slab_table[...])
    for sb in range(ns):
        for rb in range(nr):
            second[sb * rows : (sb + 1) * rows, rb * LANES : (rb + 1) * LANES] = mixed[
                rb * rows : (rb + 1) * rows, sb * LANES : (sb + 1) * LANES
            ]
    return dot(second[...], row_table[...])


def around(get, sb, rb, grid, rows, fill):
    ns, nr = grid
    lane = lax.broadcasted_iota(jnp.int32, (1, LANES), 1)
    place = lane % rows
    here = get(sb, rb)
    empty = jnp.full_like(here, fill)
    above = get(sb + 1, rb) if sb + 1 < ns else empty
    below = get(sb - 1, rb) if sb > 0 else empty
    out = [
        pltpu.roll(jnp.where(lane >= rows, here, above), LANES - rows, 1),
        pltpu.roll(jnp.where(lane < LANES - rows, here, below), rows, 1),
    ]
    right = pltpu.roll(get(sb, rb + 1), rows - 1, 1) if rb + 1 < nr else empty
    left = pltpu.roll(get(sb, rb - 1), LANES - rows + 1, 1) if rb > 0 else empty
    out.append(jnp.where(place < rows - 1, pltpu.roll(here, LANES - 1, 1), right))
    out.append(jnp.where(place > 0, pltpu.roll(here, 1, 1), left))
    return out


def pencil_kernel(grid, rows, got, raw, slab_table, row_table, send, keep, first, second, bias, dens, one, two):
    ns, nr = grid
    peers = ns * nr
    window = got.shape[1] // M
    core = window - 2 * EDGE
    tile = raw[0, (M + 1) * window :, :]
    for j in range(1, peers):
        tile = tile + raw[j, (M + 1) * window :, :]
    means, halves, shift = class_stats(tile)
    bias[...] = slab_row_filter(
        [got[j] for j in range(peers)], slab_table, row_table, first, second, grid
    )

    def shade(sb, rb, m, low=0, size=window):
        j = sb * nr + rb
        base = (sb * M + m) * window + low
        field = raw[j, m * window + low : m * window + low + size, :]
        return field - bias[base : base + size, rb * LANES : (rb + 1) * LANES]

    def code_at(sb, rb):
        return raw[sb * nr + rb, M * window : (M + 1) * window, :]

    for sb in range(ns):
        for rb in range(nr):
            j = sb * nr + rb
            logits = log_terms([shade(sb, rb, m) for m in range(M)], means, halves, shift)
            code = code_at(sb, rb)
            near = around(code_at, sb, rb, grid, rows, float(K))
            near = near + [pltpu.roll(code, 1, 0), pltpu.roll(code, window - 1, 0)]
            for k in range(K):
                dens[k, j] = logits[k]
                for x in near:
                    logits[k] = logits[k] + (x == float(k)).astype(jnp.float32)
            inside = (code < float(K)).astype(jnp.float32)
            for k, value in enumerate(soft(logits, inside)):
                one[k, j] = value
    for sb in range(ns):
        for rb in range(nr):
            j = sb * nr + rb
            logits = []
            for k in range(K):
                here = one[k, j]
                near = around(lambda a, b: one[k, a * nr + b], sb, rb, grid, rows, 0.0)
                near = near + [pltpu.roll(here, 1, 0), pltpu.roll(here, window - 1, 0)]
                logits.append(dens[k, j] + functools.reduce(jnp.add, near))
            inside = (code_at(sb, rb) < float(K)).astype(jnp.float32)
            for k, value in enumerate(soft(logits, inside)):
                two[k, j] = value
    sums = [[jnp.zeros((SUB, LANES), jnp.float32) for _ in range(STATS)] for _ in range(K)]
    for sb in range(ns):
        for rb in range(nr):
            j = sb * nr + rb
            values = [shade(sb, rb, m, EDGE, core) for m in range(M)]
            for k in range(K):
                here = two[k, j, EDGE : EDGE + core, :]
                keep[k, j] = here
                line = sums[k]
                line[0] = line[0] + fold(here)
                for m in range(M):
                    value = here * values[m]
                    line[1 + m] = line[1 + m] + fold(value)
                    line[1 + M + m] = line[1 + M + m] + fold(value * values[m])
                near = around(
                    lambda a, b: two[k, a * nr + b, EDGE : EDGE + core, :], sb, rb, grid, rows, 0.0
                )
                near = near + [
                    two[k, j, EDGE - 1 : EDGE - 1 + core, :],
                    two[k, j, EDGE + 1 : EDGE + 1 + core, :],
                ]
                send[j, k * core : (k + 1) * core, :] = functools.reduce(jnp.add, near)
    tile = stat_tile(sums)
    for p in range(peers):
        send[p, K * core :, :] = tile


def residual_kernel(grid, stat_a, stat_b, keep, raw, slab_table, row_table, send, first, second):
    ns, nr = grid
    core = keep.shape[2]
    window = core + 2 * EDGE
    means = mean_rows(stat_a[...] + stat_b[...])
    pieces = []
    for j in range(ns * nr):
        parts = []
        for m in range(M):
            field = raw[j, m * window + EDGE : m * window + EDGE + core, :]
            total = jnp.zeros_like(field)
            for k in range(K):
                total = total + keep[k, j] * (field - means[m][k : k + 1, :])
            parts.append(total)
        pieces.append(jnp.concatenate(parts, axis=0))
    done = slab_row_filter(pieces, slab_table, row_table, first, second, grid)
    rows = M * core
    for sb in range(ns):
        for rb in range(nr):
            send[sb * nr + rb] = done[sb * rows : (sb + 1) * rows, rb * LANES : (rb + 1) * LANES]


def third_kernel(rows, got, oth, near, own, stat_a, stat_b, table, place, bias, centers, dens, belief, up, down, side, edge):
    peers = got.shape[0]
    core = got.shape[1] // M
    tile = stat_a[...] + stat_b[...]
    means, halves, shift = class_stats(tile)
    centers[...] = tile[:, 1 : 1 + M] / (tile[:, 0:1] + 1.0)
    corrected = []
    for m in range(M):
        mine = got[:, m * core : (m + 1) * core, :].reshape(LANES, LANES).T
        yours = oth[:, m * core : (m + 1) * core, :].reshape(LANES, LANES).T
        field = dot(jnp.concatenate([mine, yours], axis=1), table[...])
        bias[m] = field
        corrected.append(own[m] - field)
    logits = log_terms(corrected, means, halves, shift)
    for k in range(K):
        dens[k] = logits[k]
        logits[k] = logits[k] + near[:, k * core : (k + 1) * core, :].reshape(LANES, LANES).T
    inside = (own[M] < float(K)).astype(jnp.float32)
    lane = lax.broadcasted_iota(jnp.int32, (1, LANES), 1)
    odd = place[0] % 2
    column = jnp.zeros((LANES, LANES), jnp.float32)
    for k, value in enumerate(soft(logits, inside)):
        belief[k] = value
        low = value[:rows, :]
        high = value[LANES - rows :, :]
        even = jnp.full(low.shape, odd, jnp.int32) == 0
        up[k] = jnp.where(even, high, low)
        down[k] = jnp.where(even, low, high)
        amount = jnp.where(place[2] == 0, k + 1, k)
        column = jnp.where(lane == k, pltpu.roll(value, amount, 1), column)
    edge[...] = column
    lead = jnp.full((LANES // rows, LANES), place[1], jnp.int32) == 0
    for k in range(K):
        head = belief[k, pl.ds(0, LANES // rows, rows), :]
        tail = belief[k, pl.ds(rows - 1, LANES // rows, rows), :]
        side[k] = jnp.where(lead, tail, head)


def last_kernel(rows, dens, belief, own, up, down, side, edge, place, post):
    lane = lax.broadcasted_iota(jnp.int32, (1, LANES), 1)
    line = lax.broadcasted_iota(jnp.int32, (LANES, 1), 0) % rows
    even = jnp.full((rows, LANES), place[0] % 2, jnp.int32) == 0
    spot = jnp.where(place[2] == 0, LANES - 1, 0)
    face = jnp.where(place[1] == 0, rows - 1, 0)
    column = edge[...]
    logits = []
    for k in range(K):
        here = belief[k]
        high = jnp.where(even, up[k], down[k])
        low = jnp.where(even, down[k], up[k])
        total = jnp.concatenate([low, here[: LANES - rows, :]], axis=0)
        total = total + jnp.concatenate([here[rows:, :], high], axis=0)
        beside = jnp.broadcast_to(side[k][:, None, :], (LANES // rows, rows, LANES))
        total = total + jnp.where(line == face, beside.reshape(LANES, LANES), 0.0)
        total = total + jnp.where(line > 0, pltpu.roll(here, 1, 0), 0.0)
        total = total + jnp.where(line < rows - 1, pltpu.roll(here, LANES - 1, 0), 0.0)
        shifted = pltpu.roll(column, jnp.where(place[2] == 0, LANES - 1 - k, (LANES - k) % LANES), 1)
        total = total + jnp.where(lane == spot, shifted, 0.0)
        total = total + jnp.where(lane > 0, pltpu.roll(here, 1, 1), 0.0)
        total = total + jnp.where(lane < LANES - 1, pltpu.roll(here, LANES - 1, 1), 0.0)
        logits.append(dens[k] + total)
    inside = (own[M] < float(K)).astype(jnp.float32)
    for k, value in enumerate(soft(logits, inside)):
        post[k] = value.astype(jnp.bfloat16)


def call(kernel, outs, scratch=(), scalars=()):
    vmem = pl.BlockSpec(memory_space=pltpu.VMEM)
    smem = pl.BlockSpec(memory_space=pltpu.SMEM)
    shapes = [jax.ShapeDtypeStruct(shape, kind) for shape, kind in outs]

    def run(*args):
        return pl.pallas_call(
            kernel,
            out_shape=shapes,
            in_specs=[smem if i in scalars else vmem for i in range(len(args))],
            out_specs=[vmem] * len(shapes),
            scratch_shapes=[pltpu.VMEM(shape, jnp.float32) for shape in scratch],
            name=(kernel.func if isinstance(kernel, functools.partial) else kernel).__name__,
        )(*args)

    return run


def pencils(image, brain_mask, labels):
    _, slabs, rows, columns = image.shape
    ns, nr, nc = (lax.axis_size(a) for a in ("slab", "row", "col"))
    grid = (ns, nr)
    peers = ns * nr
    core = columns // peers
    window = core + 2 * EDGE
    f32 = jnp.float32
    place = jnp.stack([lax.axis_index(a) for a in ("slab", "row", "col")]).astype(jnp.int32)
    swap = [(0, 1), (1, 0)]

    taps = impulse(columns * nc)
    reach = np.arange(-MARGIN, columns + MARGIN)
    source = np.concatenate([np.arange(columns), np.arange(columns) + columns])
    spread = taps[(reach[:, None] - source[None, :]) % (columns * nc)].astype(np.float32)
    gather = np.ascontiguousarray(spread[MARGIN : MARGIN + columns].T)
    slab_table = np.kron(dense(slabs * ns), np.eye(rows)).astype(np.float32)
    row_table = np.einsum(
        "arbq,st->asrbtq", dense(rows * nr).reshape(nr, rows, nr, rows), np.eye(slabs)
    )
    row_table = row_table.reshape(nr * LANES, nr * LANES).astype(np.float32)

    code = jnp.where(brain_mask > 0, labels, K).astype(f32)
    own = jnp.concatenate([image, code[None]]).reshape(M + 1, LANES, columns)
    oth = lax.ppermute(own, "col", swap)

    def trade(x):
        return lax.all_to_all(x, ("slab", "row"), split_axis=0, concat_axis=0, tiled=True)

    (sent,) = call(
        prepare_kernel,
        [((peers, (M + 1) * window + SUB, LANES), f32)],
        [(M + 1, columns + 2 * MARGIN, LANES)],
        (2,),
    )(own, oth, place)
    raw = trade(sent)
    (sent,) = call(
        column_kernel,
        [((peers, M * window, LANES), f32)],
        [(M * LANES, 2 * columns), (columns + 2 * MARGIN, M * LANES)],
    )(own, oth, raw, spread)
    got = trade(sent)
    sent, keep = call(
        functools.partial(pencil_kernel, grid, rows),
        [((peers, K * core + SUB, LANES), f32), ((K, peers, core, LANES), f32)],
        [
            (nr * M * window, ns * LANES),
            (ns * M * window, nr * LANES),
            (ns * M * window, nr * LANES),
            (K, peers, window, LANES),
            (K, peers, window, LANES),
            (K, peers, window, LANES),
        ],
    )(got, raw, slab_table, row_table)
    near = trade(sent)
    stat_a = jnp.sum(near[:, K * core :, :], axis=0)
    stat_b = lax.ppermute(stat_a, "col", swap)
    (sent,) = call(
        functools.partial(residual_kernel, grid),
        [((peers, M * core, LANES), f32)],
        [(nr * M * core, ns * LANES), (ns * M * core, nr * LANES)],
    )(stat_a, stat_b, keep, raw, slab_table, row_table)
    got = trade(sent)
    yours = lax.ppermute(got, "col", swap)
    bias, centers, dens, belief, up, down, side, edge = call(
        functools.partial(third_kernel, rows),
        [
            ((M, LANES, columns), f32),
            ((K, M), f32),
            ((K, LANES, columns), f32),
            ((K, LANES, columns), f32),
            ((K, rows, columns), f32),
            ((K, rows, columns), f32),
            ((K, slabs, columns), f32),
            ((LANES, LANES), f32),
        ],
        (),
        (7,),
    )(got, yours, near, own, stat_a, stat_b, gather, place)
    pairs = [(i, i + 1) for i in range(0, ns - 1, 2)]
    between = [(i, i + 1) for i in range(1, ns - 1, 2)]
    up = lax.ppermute(up, "slab", pairs + [(b, a) for a, b in pairs])
    down = lax.ppermute(down, "slab", between + [(b, a) for a, b in between])
    side = lax.ppermute(side, "row", swap)
    edge = lax.ppermute(edge, "col", swap)
    (post,) = call(
        functools.partial(last_kernel, rows), [((K, LANES, columns), jnp.bfloat16)], (), (7,)
    )(dens, belief, own, up, down, side, edge, place)
    shape = (slabs, rows, columns)
    return post.reshape((K,) + shape), bias.reshape((M,) + shape), centers


def local(image, brain_mask, labels):
    _, slabs, rows, columns = image.shape
    peers = lax.axis_size("slab") * lax.axis_size("row")
    fits = slabs * rows == LANES and columns == LANES and slabs % SUB == 0 and rows % SUB == 0
    fits = fits and lax.axis_size("row") == 2 and lax.axis_size("col") == 2
    fits = fits and columns % (SUB * peers) == 0
    return (pencils if fits else general)(image, brain_mask, labels)


def solution(mesh):
    placed = (
        P(None, ("grp", "slab"), "row", "col"),
        P(("grp", "slab"), "row", "col"),
        P(("grp", "slab"), "row", "col"),
    )
    return jax.shard_map(
        local,
        mesh=mesh,
        in_specs=placed,
        out_specs=(
            P(None, ("grp", "slab"), "row", "col"),
            P(None, ("grp", "slab"), "row", "col"),
            P("grp", None),
        ),
        check_vma=False,
    )
```

```python
import functools
import math

import jax
import jax.numpy as jnp
import numpy as np
from jax import lax
from jax.experimental import pallas as pl
from jax.experimental.pallas import tpu as pltpu
from jax.sharding import PartitionSpec as P

M = 3
K = 8
EM_ITERS = 2
MF_PASSES = 2


highest = lax.Precision.HIGHEST
coupling = 1.0
breadth = 8.0


def extended(cells, sides, width):
    for axis, dim in sides:
        count = lax.axis_size(axis)
        ends = count - 1
        head = lax.slice_in_dim(cells, 0, width, axis=dim)
        tail = lax.slice_in_dim(cells, cells.shape[dim] - width, cells.shape[dim], axis=dim)
        cells = jnp.concatenate(
            [
                lax.ppermute(tail, axis, [(i, (i + 1) % count) for i in range(ends)]),
                cells,
                lax.ppermute(head, axis, [((i + 1) % count, i) for i in range(ends)]),
            ],
            axis=dim,
        )
    return cells


def circulant(length):
    index = jnp.arange(length, dtype=jnp.int32)
    folded = jnp.minimum(index, length - index).astype(jnp.float32) / length
    response = jnp.exp(-2.0 * math.pi**2 * (length / breadth) ** 2 * folded * folded)
    product = index[:, None] * index[None, :] % length
    angles = 2.0 * math.pi / length * product.astype(jnp.float32)
    cosine = jnp.cos(angles)
    sine = jnp.sin(angles)
    even_part = jnp.dot(cosine * response[None, :], cosine.T, precision=highest)
    odd_part = jnp.dot(sine * response[None, :], sine.T, precision=highest)
    return (even_part + odd_part) / length


def neighbour_sum(belief):
    padded = extended(belief, (("slab", 1), ("row", 2), ("col", 3)), 1)
    total = padded[:, 2:, 1:-1, 1:-1] + padded[:, :-2, 1:-1, 1:-1]
    total = total + padded[:, 1:-1, 2:, 1:-1] + padded[:, 1:-1, :-2, 1:-1]
    total = total + padded[:, 1:-1, 1:-1, 2:] + padded[:, 1:-1, 1:-1, :-2]
    return total


def class_moments(belief, corrected):
    flat = belief.reshape(K, -1)
    values = corrected.reshape(M, -1)
    count, first, squares = lax.psum(
        (
            jnp.sum(flat, axis=1),
            jnp.dot(flat, values.T, precision=highest),
            jnp.dot(flat, (values * values).T, precision=highest),
        ),
        ("slab", "row", "col"),
    )
    means = first / (count + 1.0)[:, None]
    spread = squares - 2.0 * means * first + means * means * count[:, None]
    variance = (spread + 1.0) / (count + 1.0)[:, None]
    return (count, means, variance)


def log_density(corrected, means, variance, prior):
    offset = corrected[None] - means[:, :, None, None, None]
    terms = (
        offset * offset / variance[:, :, None, None, None]
        + jnp.log(variance)[:, :, None, None, None]
    )
    return jnp.log(prior)[:, None, None, None] - 0.5 * jnp.sum(terms, axis=1)


def smoothed(residual, column_local, row_table, slab_table):
    across = jnp.einsum(
        "msrc,cd->msrd",
        lax.all_gather(residual, "col", axis=3, tiled=True),
        column_local,
        precision=highest,
    )
    mixed = jnp.einsum(
        "msrc,rq->msqc",
        lax.all_to_all(across, "row", split_axis=1, concat_axis=2, tiled=True),
        row_table,
        precision=highest,
    )
    across = lax.all_to_all(mixed, "row", split_axis=2, concat_axis=1, tiled=True)
    mixed = jnp.einsum(
        "msrc,sq->mqrc",
        lax.all_to_all(across, "slab", split_axis=2, concat_axis=1, tiled=True),
        slab_table,
        precision=highest,
    )
    return lax.all_to_all(mixed, "slab", split_axis=1, concat_axis=2, tiled=True)


def general(image, brain_mask, labels):
    channels, slabs, rows, columns = image.shape
    inside = brain_mask.astype(jnp.float32)
    kinds = jnp.arange(K, dtype=jnp.int32)
    belief = (labels[None] == kinds[:, None, None, None]).astype(jnp.float32) * inside[None]
    column_table = circulant(columns * lax.axis_size("col"))
    column_local = lax.dynamic_slice_in_dim(
        column_table, lax.axis_index("col") * columns, columns, 1
    )
    row_table = circulant(rows * lax.axis_size("row"))
    slab_table = circulant(slabs * lax.axis_size("slab"))
    bias_field = jnp.zeros_like(image)
    means = jnp.zeros((K, channels), jnp.float32)
    for iteration in range(EM_ITERS):
        corrected = image - bias_field
        count, means, variance = class_moments(belief, corrected)
        prior = (count + 1.0) / (jnp.sum(count) + K)
        total = jnp.sum(belief, axis=0)
        removed = jnp.dot(means.T, belief.reshape(K, -1), precision=highest).reshape(image.shape)
        residual = image * total[None] - removed
        bias_field = smoothed(residual, column_local, row_table, slab_table)
        corrected = image - bias_field
        density = log_density(corrected, means, variance, prior)
        for sweep_index in range(MF_PASSES):
            belief = (
                jax.nn.softmax(density + coupling * neighbour_sum(belief), axis=0) * inside[None]
            )
    return (belief.astype(jnp.bfloat16), bias_field, means)


LANES = 128
SUB = 8
EDGE = 4
MARGIN = 8
STATS = 1 + 2 * M
VMEM_BYTES = 16 * 2**20


def impulse(length):
    index = np.arange(length)
    folded = np.minimum(index, length - index) / length
    response = np.exp(-2.0 * np.pi**2 * (length / breadth) ** 2 * folded * folded)
    angles = 2.0 * np.pi / length * (index[:, None] * index[None, :] % length)
    return np.cos(angles) @ response / length


def dense(length):
    index = np.arange(length)
    return impulse(length)[(index[:, None] - index[None, :]) % length]


def dot(left, right, dims=((1,), (0,))):
    return lax.dot_general(
        left, right, (dims, ((), ())), precision=highest, preferred_element_type=jnp.float32
    )


def wide(row, shape=(SUB, LANES)):
    return jnp.broadcast_to(row, shape)


def stat_tile(sums):
    sub = lax.broadcasted_iota(jnp.int32, (SUB, LANES), 0)
    lane = lax.broadcasted_iota(jnp.int32, (SUB, LANES), 1)
    tile = jnp.zeros((SUB, LANES), jnp.float32)
    for q in range(STATS):
        rows = jnp.zeros((SUB, LANES), jnp.float32)
        for k in range(K):
            line = jnp.sum(sums[k][q], axis=0, keepdims=True)
            rows = jnp.where(sub == k, line, rows)
        tile = jnp.where(lane == q, jnp.sum(rows, axis=1, keepdims=True), tile)
    return tile


def fold(x):
    return jnp.sum(x.reshape(x.shape[0] // SUB, SUB, LANES), axis=0)


def class_stats(tile):
    count = tile[:, 0:1]
    means, halves = [], []
    shift = jnp.zeros_like(count)
    for m in range(M):
        first = tile[:, 1 + m : 2 + m]
        squares = tile[:, 1 + M + m : 2 + M + m]
        mean = first / (count + 1.0)
        spread = squares - 2.0 * mean * first + mean * mean * count
        variance = (spread + 1.0) / (count + 1.0)
        means.append(wide(mean))
        halves.append(wide(0.5 / variance))
        shift = shift - 0.5 * jnp.log(variance)
    prior = (count + 1.0) / (jnp.sum(count, axis=0, keepdims=True) + K)
    return means, halves, wide(jnp.log(prior) + shift)


def mean_rows(tile):
    return [wide(tile[:, 1 + m : 2 + m] / (tile[:, 0:1] + 1.0)) for m in range(M)]


def log_terms(corrected, means, halves, shift):
    out = []
    for k in range(K):
        total = wide(shift[k : k + 1, :], corrected[0].shape)
        for m in range(M):
            offset = corrected[m] - means[m][k : k + 1, :]
            total = total - offset * offset * halves[m][k : k + 1, :]
        out.append(total)
    return out


def soft(logits, inside):
    top = functools.reduce(jnp.maximum, logits)
    exps = [jnp.exp(x - top) for x in logits]
    scale = inside / functools.reduce(jnp.add, exps)
    return [x * scale for x in exps]


def prepare_kernel(own, oth, place, send, ext):
    window = send.shape[1] // (M + 1) // SUB * SUB
    peers = send.shape[0]
    step = LANES // peers
    first = jnp.full((SUB, LANES), place[2], jnp.int32) == 0
    for f in range(M + 1):
        blank = jnp.full((SUB, LANES), float(K) if f == M else 0.0, jnp.float32)
        other = oth[f].T
        ext[f, 0:MARGIN, :] = jnp.where(first, blank, other[LANES - MARGIN :, :])
        ext[f, MARGIN : MARGIN + LANES, :] = own[f].T
        ext[f, MARGIN + LANES :, :] = jnp.where(first, other[:MARGIN, :], blank)
    sums = []
    for k in range(K):
        line = [jnp.zeros((SUB, LANES), jnp.float32) for _ in range(STATS)]
        for ref in (own, oth):
            flag = (ref[M] == float(k)).astype(jnp.float32)
            line[0] = line[0] + fold(flag)
            for m in range(M):
                value = flag * ref[m]
                line[1 + m] = line[1 + m] + fold(value)
                line[1 + M + m] = line[1 + M + m] + fold(value * ref[m])
        sums.append(line)
    tile = stat_tile(sums)
    for p in range(peers):
        for f in range(M + 1):
            base = MARGIN - EDGE + step * p
            send[p, f * window : (f + 1) * window, :] = ext[f, base : base + window, :]
        send[p, (M + 1) * window :, :] = tile


def column_kernel(own, oth, got, table, send, flat, out):
    peers = send.shape[0]
    window = send.shape[1] // M
    step = LANES // peers
    tile = got[0, (M + 1) * window :, :]
    for j in range(1, peers):
        tile = tile + got[j, (M + 1) * window :, :]
    means = mean_rows(tile)
    for h, ref in enumerate((own, oth)):
        code = ref[M]
        flags = [code == float(k) for k in range(K)]
        for m in range(M):
            center = jnp.zeros_like(code)
            for k in range(K):
                center = jnp.where(flags[k], means[m][k : k + 1, :], center)
            flat[m * LANES : (m + 1) * LANES, h * LANES : (h + 1) * LANES] = jnp.where(
                code < float(K), ref[m] - center, 0.0
            )
    out[...] = dot(table[...], flat[...], ((1,), (1,)))
    for p in range(peers):
        base = MARGIN - EDGE + step * p
        for m in range(M):
            send[p, m * window : (m + 1) * window, :] = out[
                base : base + window, m * LANES : (m + 1) * LANES
            ]


def slab_row_filter(pieces, slab_table, row_table, first, second, grid):
    ns, nr = grid
    rows = pieces[0].shape[0]
    for sb in range(ns):
        for rb in range(nr):
            first[rb * rows : (rb + 1) * rows, sb * LANES : (sb + 1) * LANES] = pieces[sb * nr + rb]
    mixed = dot(first[...], slab_table[...])
    for sb in range(ns):
        for rb in range(nr):
            second[sb * rows : (sb + 1) * rows, rb * LANES : (rb + 1) * LANES] = mixed[
                rb * rows : (rb + 1) * rows, sb * LANES : (sb + 1) * LANES
            ]
    return dot(second[...], row_table[...])


def around(get, sb, rb, grid, rows, fill):
    ns, nr = grid
    lane = lax.broadcasted_iota(jnp.int32, (1, LANES), 1)
    place = lane % rows
    here = get(sb, rb)
    empty = jnp.full_like(here, fill)
    above = get(sb + 1, rb) if sb + 1 < ns else empty
    below = get(sb - 1, rb) if sb > 0 else empty
    out = [
        pltpu.roll(jnp.where(lane >= rows, here, above), LANES - rows, 1),
        pltpu.roll(jnp.where(lane < LANES - rows, here, below), rows, 1),
    ]
    right = pltpu.roll(get(sb, rb + 1), rows - 1, 1) if rb + 1 < nr else empty
    left = pltpu.roll(get(sb, rb - 1), LANES - rows + 1, 1) if rb > 0 else empty
    out.append(jnp.where(place < rows - 1, pltpu.roll(here, LANES - 1, 1), right))
    out.append(jnp.where(place > 0, pltpu.roll(here, 1, 1), left))
    return out


def pencil_kernel(grid, rows, got, raw, slab_table, row_table, send, keep, first, second, bias, dens, one, two):
    ns, nr = grid
    peers = ns * nr
    window = got.shape[1] // M
    core = window - 2 * EDGE
    tile = raw[0, (M + 1) * window :, :]
    for j in range(1, peers):
        tile = tile + raw[j, (M + 1) * window :, :]
    means, halves, shift = class_stats(tile)
    bias[...] = slab_row_filter(
        [got[j] for j in range(peers)], slab_table, row_table, first, second, grid
    )

    def shade(sb, rb, m, low=0, size=window):
        j = sb * nr + rb
        base = (sb * M + m) * window + low
        field = raw[j, m * window + low : m * window + low + size, :]
        return field - bias[base : base + size, rb * LANES : (rb + 1) * LANES]

    def code_at(sb, rb):
        return raw[sb * nr + rb, M * window : (M + 1) * window, :]

    for sb in range(ns):
        for rb in range(nr):
            j = sb * nr + rb
            logits = log_terms([shade(sb, rb, m) for m in range(M)], means, halves, shift)
            code = code_at(sb, rb)
            near = around(code_at, sb, rb, grid, rows, float(K))
            near = near + [pltpu.roll(code, 1, 0), pltpu.roll(code, window - 1, 0)]
            for k in range(K):
                dens[k, j] = logits[k]
                for x in near:
                    logits[k] = logits[k] + (x == float(k)).astype(jnp.float32)
            inside = (code < float(K)).astype(jnp.float32)
            for k, value in enumerate(soft(logits, inside)):
                one[k, j] = value
    for sb in range(ns):
        for rb in range(nr):
            j = sb * nr + rb
            logits = []
            for k in range(K):
                here = one[k, j]
                near = around(lambda a, b: one[k, a * nr + b], sb, rb, grid, rows, 0.0)
                near = near + [pltpu.roll(here, 1, 0), pltpu.roll(here, window - 1, 0)]
                logits.append(dens[k, j] + functools.reduce(jnp.add, near))
            inside = (code_at(sb, rb) < float(K)).astype(jnp.float32)
            for k, value in enumerate(soft(logits, inside)):
                two[k, j] = value
    sums = [[jnp.zeros((SUB, LANES), jnp.float32) for _ in range(STATS)] for _ in range(K)]
    for sb in range(ns):
        for rb in range(nr):
            j = sb * nr + rb
            values = [shade(sb, rb, m, EDGE, core) for m in range(M)]
            for k in range(K):
                here = two[k, j, EDGE : EDGE + core, :]
                keep[k, j] = here
                line = sums[k]
                line[0] = line[0] + fold(here)
                for m in range(M):
                    value = here * values[m]
                    line[1 + m] = line[1 + m] + fold(value)
                    line[1 + M + m] = line[1 + M + m] + fold(value * values[m])
                near = around(
                    lambda a, b: two[k, a * nr + b, EDGE : EDGE + core, :], sb, rb, grid, rows, 0.0
                )
                near = near + [
                    two[k, j, EDGE - 1 : EDGE - 1 + core, :],
                    two[k, j, EDGE + 1 : EDGE + 1 + core, :],
                ]
                send[j, k * core : (k + 1) * core, :] = functools.reduce(jnp.add, near)
    tile = stat_tile(sums)
    for p in range(peers):
        send[p, K * core :, :] = tile


def residual_kernel(grid, stat_a, stat_b, keep, raw, slab_table, row_table, send, first, second):
    ns, nr = grid
    core = keep.shape[2]
    window = core + 2 * EDGE
    means = mean_rows(stat_a[...] + stat_b[...])
    pieces = []
    for j in range(ns * nr):
        parts = []
        for m in range(M):
            field = raw[j, m * window + EDGE : m * window + EDGE + core, :]
            total = jnp.zeros_like(field)
            for k in range(K):
                total = total + keep[k, j] * (field - means[m][k : k + 1, :])
            parts.append(total)
        pieces.append(jnp.concatenate(parts, axis=0))
    done = slab_row_filter(pieces, slab_table, row_table, first, second, grid)
    rows = M * core
    for sb in range(ns):
        for rb in range(nr):
            send[sb * nr + rb] = done[sb * rows : (sb + 1) * rows, rb * LANES : (rb + 1) * LANES]


def third_kernel(rows, got, oth, near, own, stat_a, stat_b, table, place, bias, centers, dens, belief, up, down, side, edge):
    peers = got.shape[0]
    core = got.shape[1] // M
    tile = stat_a[...] + stat_b[...]
    means, halves, shift = class_stats(tile)
    centers[...] = tile[:, 1 : 1 + M] / (tile[:, 0:1] + 1.0)
    corrected = []
    for m in range(M):
        mine = got[:, m * core : (m + 1) * core, :].reshape(LANES, LANES).T
        yours = oth[:, m * core : (m + 1) * core, :].reshape(LANES, LANES).T
        field = dot(jnp.concatenate([mine, yours], axis=1), table[...])
        bias[m] = field
        corrected.append(own[m] - field)
    logits = log_terms(corrected, means, halves, shift)
    for k in range(K):
        dens[k] = logits[k]
        logits[k] = logits[k] + near[:, k * core : (k + 1) * core, :].reshape(LANES, LANES).T
    inside = (own[M] < float(K)).astype(jnp.float32)
    lane = lax.broadcasted_iota(jnp.int32, (1, LANES), 1)
    odd = place[0] % 2
    column = jnp.zeros((LANES, LANES), jnp.float32)
    for k, value in enumerate(soft(logits, inside)):
        belief[k] = value
        low = value[:rows, :]
        high = value[LANES - rows :, :]
        even = jnp.full(low.shape, odd, jnp.int32) == 0
        up[k] = jnp.where(even, high, low)
        down[k] = jnp.where(even, low, high)
        amount = jnp.where(place[2] == 0, k + 1, k)
        column = jnp.where(lane == k, pltpu.roll(value, amount, 1), column)
    edge[...] = column
    lead = jnp.full((LANES // rows, LANES), place[1], jnp.int32) == 0
    for k in range(K):
        head = belief[k, pl.ds(0, LANES // rows, rows), :]
        tail = belief[k, pl.ds(rows - 1, LANES // rows, rows), :]
        side[k] = jnp.where(lead, tail, head)


def last_kernel(rows, dens, belief, own, up, down, side, edge, place, post):
    lane = lax.broadcasted_iota(jnp.int32, (1, LANES), 1)
    line = lax.broadcasted_iota(jnp.int32, (LANES, 1), 0) % rows
    even = jnp.full((rows, LANES), place[0] % 2, jnp.int32) == 0
    spot = jnp.where(place[2] == 0, LANES - 1, 0)
    face = jnp.where(place[1] == 0, rows - 1, 0)
    column = edge[...]
    logits = []
    for k in range(K):
        here = belief[k]
        high = jnp.where(even, up[k], down[k])
        low = jnp.where(even, down[k], up[k])
        total = jnp.concatenate([low, here[: LANES - rows, :]], axis=0)
        total = total + jnp.concatenate([here[rows:, :], high], axis=0)
        beside = jnp.broadcast_to(side[k][:, None, :], (LANES // rows, rows, LANES))
        total = total + jnp.where(line == face, beside.reshape(LANES, LANES), 0.0)
        total = total + jnp.where(line > 0, pltpu.roll(here, 1, 0), 0.0)
        total = total + jnp.where(line < rows - 1, pltpu.roll(here, LANES - 1, 0), 0.0)
        shifted = pltpu.roll(column, jnp.where(place[2] == 0, LANES - 1 - k, (LANES - k) % LANES), 1)
        total = total + jnp.where(lane == spot, shifted, 0.0)
        total = total + jnp.where(lane > 0, pltpu.roll(here, 1, 1), 0.0)
        total = total + jnp.where(lane < LANES - 1, pltpu.roll(here, LANES - 1, 1), 0.0)
        logits.append(dens[k] + total)
    inside = (own[M] < float(K)).astype(jnp.float32)
    for k, value in enumerate(soft(logits, inside)):
        post[k] = value.astype(jnp.bfloat16)


def call(kernel, outs, scratch=(), scalars=()):
    vmem = pl.BlockSpec(memory_space=pltpu.VMEM)
    smem = pl.BlockSpec(memory_space=pltpu.SMEM)
    shapes = [jax.ShapeDtypeStruct(shape, kind) for shape, kind in outs]

    def run(*args):
        return pl.pallas_call(
            kernel,
            out_shape=shapes,
            in_specs=[smem if i in scalars else vmem for i in range(len(args))],
            out_specs=[vmem] * len(shapes),
            scratch_shapes=[pltpu.VMEM(shape, jnp.float32) for shape in scratch],
            compiler_params=pltpu.CompilerParams(vmem_limit_bytes=VMEM_BYTES),
            name=(kernel.func if isinstance(kernel, functools.partial) else kernel).__name__,
        )(*args)

    return run


def pencils(image, brain_mask, labels):
    _, slabs, rows, columns = image.shape
    ns, nr, nc = (lax.axis_size(a) for a in ("slab", "row", "col"))
    grid = (ns, nr)
    peers = ns * nr
    core = columns // peers
    window = core + 2 * EDGE
    f32 = jnp.float32
    place = jnp.stack([lax.axis_index(a) for a in ("slab", "row", "col")]).astype(jnp.int32)
    swap = [(0, 1), (1, 0)]

    taps = impulse(columns * nc)
    reach = np.arange(-MARGIN, columns + MARGIN)
    source = np.concatenate([np.arange(columns), np.arange(columns) + columns])
    spread = taps[(reach[:, None] - source[None, :]) % (columns * nc)].astype(np.float32)
    gather = np.ascontiguousarray(spread[MARGIN : MARGIN + columns].T)
    slab_table = np.kron(dense(slabs * ns), np.eye(rows)).astype(np.float32)
    row_table = np.einsum(
        "arbq,st->asrbtq", dense(rows * nr).reshape(nr, rows, nr, rows), np.eye(slabs)
    )
    row_table = row_table.reshape(nr * LANES, nr * LANES).astype(np.float32)

    code = jnp.where(brain_mask > 0, labels, K).astype(f32)
    own = jnp.concatenate([image, code[None]]).reshape(M + 1, LANES, columns)
    oth = lax.ppermute(own, "col", swap)

    def trade(x):
        return lax.all_to_all(x, ("slab", "row"), split_axis=0, concat_axis=0, tiled=True)

    (sent,) = call(
        prepare_kernel,
        [((peers, (M + 1) * window + SUB, LANES), f32)],
        [(M + 1, columns + 2 * MARGIN, LANES)],
        (2,),
    )(own, oth, place)
    raw = trade(sent)
    (sent,) = call(
        column_kernel,
        [((peers, M * window, LANES), f32)],
        [(M * LANES, 2 * columns), (columns + 2 * MARGIN, M * LANES)],
    )(own, oth, raw, spread)
    got = trade(sent)
    sent, keep = call(
        functools.partial(pencil_kernel, grid, rows),
        [((peers, K * core + SUB, LANES), f32), ((K, peers, core, LANES), f32)],
        [
            (nr * M * window, ns * LANES),
            (ns * M * window, nr * LANES),
            (ns * M * window, nr * LANES),
            (K, peers, window, LANES),
            (K, peers, window, LANES),
            (K, peers, window, LANES),
        ],
    )(got, raw, slab_table, row_table)
    near = trade(sent)
    stat_a = jnp.sum(near[:, K * core :, :], axis=0)
    stat_b = lax.ppermute(stat_a, "col", swap)
    (sent,) = call(
        functools.partial(residual_kernel, grid),
        [((peers, M * core, LANES), f32)],
        [(nr * M * core, ns * LANES), (ns * M * core, nr * LANES)],
    )(stat_a, stat_b, keep, raw, slab_table, row_table)
    got = trade(sent)
    yours = lax.ppermute(got, "col", swap)
    bias, centers, dens, belief, up, down, side, edge = call(
        functools.partial(third_kernel, rows),
        [
            ((M, LANES, columns), f32),
            ((K, M), f32),
            ((K, LANES, columns), f32),
            ((K, LANES, columns), f32),
            ((K, rows, columns), f32),
            ((K, rows, columns), f32),
            ((K, slabs, columns), f32),
            ((LANES, LANES), f32),
        ],
        (),
        (7,),
    )(got, yours, near, own, stat_a, stat_b, gather, place)
    pairs = [(i, i + 1) for i in range(0, ns - 1, 2)]
    between = [(i, i + 1) for i in range(1, ns - 1, 2)]
    up = lax.ppermute(up, "slab", pairs + [(b, a) for a, b in pairs])
    down = lax.ppermute(down, "slab", between + [(b, a) for a, b in between])
    side = lax.ppermute(side, "row", swap)
    edge = lax.ppermute(edge, "col", swap)
    (post,) = call(
        functools.partial(last_kernel, rows), [((K, LANES, columns), jnp.bfloat16)], (), (7,)
    )(dens, belief, own, up, down, side, edge, place)
    shape = (slabs, rows, columns)
    return post.reshape((K,) + shape), bias.reshape((M,) + shape), centers


def local(image, brain_mask, labels):
    _, slabs, rows, columns = image.shape
    peers = lax.axis_size("slab") * lax.axis_size("row")
    fits = slabs * rows == LANES and columns == LANES and slabs % SUB == 0 and rows % SUB == 0
    fits = fits and lax.axis_size("row") == 2 and lax.axis_size("col") == 2
    fits = fits and columns % (SUB * peers) == 0
    return (pencils if fits else general)(image, brain_mask, labels)


def solution(mesh):
    placed = (
        P(None, ("grp", "slab"), "row", "col"),
        P(("grp", "slab"), "row", "col"),
        P(("grp", "slab"), "row", "col"),
    )
    return jax.shard_map(
        local,
        mesh=mesh,
        in_specs=placed,
        out_specs=(
            P(None, ("grp", "slab"), "row", "col"),
            P(None, ("grp", "slab"), "row", "col"),
            P("grp", None),
        ),
        check_vma=False,
    )
```

```python
import functools
import math
import typing

import jax
import jax.numpy as jnp
import numpy as np
from jax import lax
from jax.experimental import pallas as pl
from jax.experimental.pallas import tpu as pltpu
from jax.sharding import PartitionSpec as P

M = 3
K = 8
EM_ITERS = 2
MF_PASSES = 2


highest = lax.Precision.HIGHEST
coupling = 1.0
breadth = 8.0


def extended(cells, sides, width):
    for axis, dim in sides:
        count = lax.axis_size(axis)
        ends = count - 1
        head = lax.slice_in_dim(cells, 0, width, axis=dim)
        tail = lax.slice_in_dim(cells, cells.shape[dim] - width, cells.shape[dim], axis=dim)
        cells = jnp.concatenate(
            [
                lax.ppermute(tail, axis, [(i, (i + 1) % count) for i in range(ends)]),
                cells,
                lax.ppermute(head, axis, [((i + 1) % count, i) for i in range(ends)]),
            ],
            axis=dim,
        )
    return cells


def circulant(length):
    index = jnp.arange(length, dtype=jnp.int32)
    folded = jnp.minimum(index, length - index).astype(jnp.float32) / length
    response = jnp.exp(-2.0 * math.pi**2 * (length / breadth) ** 2 * folded * folded)
    product = index[:, None] * index[None, :] % length
    angles = 2.0 * math.pi / length * product.astype(jnp.float32)
    cosine = jnp.cos(angles)
    sine = jnp.sin(angles)
    even_part = jnp.dot(cosine * response[None, :], cosine.T, precision=highest)
    odd_part = jnp.dot(sine * response[None, :], sine.T, precision=highest)
    return (even_part + odd_part) / length


def neighbour_sum(belief):
    padded = extended(belief, (("slab", 1), ("row", 2), ("col", 3)), 1)
    total = padded[:, 2:, 1:-1, 1:-1] + padded[:, :-2, 1:-1, 1:-1]
    total = total + padded[:, 1:-1, 2:, 1:-1] + padded[:, 1:-1, :-2, 1:-1]
    total = total + padded[:, 1:-1, 1:-1, 2:] + padded[:, 1:-1, 1:-1, :-2]
    return total


def class_moments(belief, corrected):
    flat = belief.reshape(K, -1)
    values = corrected.reshape(M, -1)
    count, first, squares = lax.psum(
        (
            jnp.sum(flat, axis=1),
            jnp.dot(flat, values.T, precision=highest),
            jnp.dot(flat, (values * values).T, precision=highest),
        ),
        ("slab", "row", "col"),
    )
    means = first / (count + 1.0)[:, None]
    spread = squares - 2.0 * means * first + means * means * count[:, None]
    variance = (spread + 1.0) / (count + 1.0)[:, None]
    return (count, means, variance)


def log_density(corrected, means, variance, prior):
    offset = corrected[None] - means[:, :, None, None, None]
    terms = (
        offset * offset / variance[:, :, None, None, None]
        + jnp.log(variance)[:, :, None, None, None]
    )
    return jnp.log(prior)[:, None, None, None] - 0.5 * jnp.sum(terms, axis=1)


def smoothed(residual, column_local, row_table, slab_table):
    across = jnp.einsum(
        "msrc,cd->msrd",
        lax.all_gather(residual, "col", axis=3, tiled=True),
        column_local,
        precision=highest,
    )
    mixed = jnp.einsum(
        "msrc,rq->msqc",
        lax.all_to_all(across, "row", split_axis=1, concat_axis=2, tiled=True),
        row_table,
        precision=highest,
    )
    across = lax.all_to_all(mixed, "row", split_axis=2, concat_axis=1, tiled=True)
    mixed = jnp.einsum(
        "msrc,sq->mqrc",
        lax.all_to_all(across, "slab", split_axis=2, concat_axis=1, tiled=True),
        slab_table,
        precision=highest,
    )
    return lax.all_to_all(mixed, "slab", split_axis=1, concat_axis=2, tiled=True)


def general(image, brain_mask, labels):
    channels, slabs, rows, columns = image.shape
    inside = brain_mask.astype(jnp.float32)
    kinds = jnp.arange(K, dtype=jnp.int32)
    belief = (labels[None] == kinds[:, None, None, None]).astype(jnp.float32) * inside[None]
    column_table = circulant(columns * lax.axis_size("col"))
    column_local = lax.dynamic_slice_in_dim(
        column_table, lax.axis_index("col") * columns, columns, 1
    )
    row_table = circulant(rows * lax.axis_size("row"))
    slab_table = circulant(slabs * lax.axis_size("slab"))
    bias_field = jnp.zeros_like(image)
    means = jnp.zeros((K, channels), jnp.float32)
    for iteration in range(EM_ITERS):
        corrected = image - bias_field
        count, means, variance = class_moments(belief, corrected)
        prior = (count + 1.0) / (jnp.sum(count) + K)
        total = jnp.sum(belief, axis=0)
        removed = jnp.dot(means.T, belief.reshape(K, -1), precision=highest).reshape(image.shape)
        residual = image * total[None] - removed
        bias_field = smoothed(residual, column_local, row_table, slab_table)
        corrected = image - bias_field
        density = log_density(corrected, means, variance, prior)
        for sweep_index in range(MF_PASSES):
            belief = (
                jax.nn.softmax(density + coupling * neighbour_sum(belief), axis=0) * inside[None]
            )
    return (belief.astype(jnp.bfloat16), bias_field, means)


LANES = 128
SUB = 8
EDGE = 4
MARGIN = 8
FIELD = 4
STATS = 1 + 2 * M
VMEM_BYTES = 16 * 2**20


def impulse(length):
    index = np.arange(length)
    folded = np.minimum(index, length - index) / length
    response = np.exp(-2.0 * np.pi**2 * (length / breadth) ** 2 * folded * folded)
    angles = 2.0 * np.pi / length * (index[:, None] * index[None, :] % length)
    return np.cos(angles) @ response / length


def dense(length):
    index = np.arange(length)
    return impulse(length)[(index[:, None] - index[None, :]) % length]


def dot(left, right, dims=((1,), (0,))):
    return lax.dot_general(
        left, right, (dims, ((), ())), precision=highest, preferred_element_type=jnp.float32
    )


def wide(row, shape=(SUB, LANES)):
    return jnp.broadcast_to(row, shape)


def stat_row(sums):
    sub = lax.broadcasted_iota(jnp.int32, (SUB, LANES), 0)
    lane = lax.broadcasted_iota(jnp.int32, (SUB, LANES), 1)
    tile = jnp.zeros((SUB, LANES), jnp.float32)
    for q in range(STATS):
        rows = jnp.zeros((SUB, LANES), jnp.float32)
        for k in range(K):
            line = jnp.sum(sums[k][q], axis=0, keepdims=True)
            rows = jnp.where(sub == k, line, rows)
        tile = jnp.where(lane == q * K + sub, jnp.sum(rows, axis=1, keepdims=True), tile)
    return jnp.sum(tile, axis=0, keepdims=True)


def stat_columns(row, number):
    sub = lax.broadcasted_iota(jnp.int32, (SUB, LANES), 0)
    lane = lax.broadcasted_iota(jnp.int32, (SUB, LANES), 1)
    return [
        jnp.sum(jnp.where(lane == q * K + sub, row, 0.0), axis=1, keepdims=True)
        for q in range(number)
    ]


def fold(x):
    return jnp.sum(x.reshape(x.shape[0] // SUB, SUB, LANES), axis=0)


def class_stats(row):
    count, *rest = stat_columns(row, STATS)
    means, halves = [], []
    shift = jnp.zeros_like(count)
    for m in range(M):
        first, squares = rest[m], rest[M + m]
        mean = first / (count + 1.0)
        spread = squares - 2.0 * mean * first + mean * mean * count
        variance = (spread + 1.0) / (count + 1.0)
        means.append(wide(mean))
        halves.append(wide(0.5 / variance))
        shift = shift - 0.5 * jnp.log(variance)
    prior = (count + 1.0) / (jnp.sum(count, axis=0, keepdims=True) + K)
    return means, halves, wide(jnp.log(prior) + shift)


def mean_rows(row):
    count, *rest = stat_columns(row, 1 + M)
    return [wide(x / (count + 1.0)) for x in rest]


def log_terms(corrected, means, halves, shift):
    out = []
    for k in range(K):
        total = wide(shift[k : k + 1, :], corrected[0].shape)
        for m in range(M):
            offset = corrected[m] - means[m][k : k + 1, :]
            total = total - offset * offset * halves[m][k : k + 1, :]
        out.append(total)
    return out


def soft(logits, inside):
    top = functools.reduce(jnp.maximum, logits)
    exps = [jnp.exp(x - top) for x in logits]
    scale = inside / functools.reduce(jnp.add, exps)
    return [x * scale for x in exps]


def peer_sum(ref, line):
    row = ref[0, line : line + 1, :]
    for j in range(1, ref.shape[0]):
        row = row + ref[j, line : line + 1, :]
    return row


def class_sums(code, image):
    sums = []
    for k in range(K):
        flag = (code == float(k)).astype(jnp.float32)
        line = [fold(flag)]
        weighted = [flag * image[m] for m in range(M)]
        line += [fold(x) for x in weighted]
        line += [fold(x * image[m]) for m, x in enumerate(weighted)]
        sums.append(line)
    return sums


def own_kernel(own, turned, stat):
    stat[...] = wide(stat_row(class_sums(own[M], own)))
    for f in range(M + 1):
        turned[f] = own[f].T


def prepare_kernel(pack, turned, stat, oth, place, send, rest, ext):
    peers = send.shape[0]
    step = LANES // peers
    first = jnp.full((SUB, LANES), place[2], jnp.int32) == 0
    row = stat[0:1, :] + stat_row(class_sums(oth[M], oth))
    for f in range(M + 1):
        blank = jnp.full((SUB, LANES), float(K) if f == M else 0.0, jnp.float32)
        other = oth[f].T
        ext[f, 0:MARGIN, :] = jnp.where(first, blank, other[LANES - MARGIN :, :])
        ext[f, MARGIN : MARGIN + LANES, :] = turned[f]
        ext[f, MARGIN + LANES :, :] = jnp.where(first, other[:MARGIN, :], blank)
    for p in range(peers):
        at = MARGIN + step * p
        for m in range(M):
            send[p, pack.wide * m : pack.wide * (m + 1), :] = ext[m, at - 2 : at + step + 2, :]
        send[p, pack.code : pack.stat, :] = ext[M, at - 1 : at + step + 1, :]
        send[p, pack.stat : pack.stat + 1, :] = row
        rest[p, 0:2, :] = ext[M, at - 3 : at - 1, :]
        rest[p, 2:4, :] = ext[M, at + step + 1 : at + step + 3, :]


def column_kernel(pack, own, oth, got, rest, table, send, flat, out):
    peers = send.shape[0]
    step = LANES // peers
    means = mean_rows(peer_sum(got, pack.stat))
    for h, ref in enumerate((own, oth)):
        code = ref[M]
        flags = [code == float(k) for k in range(K)]
        for m in range(M):
            center = jnp.zeros_like(code)
            for k in range(K):
                center = jnp.where(flags[k], means[m][k : k + 1, :], center)
            flat[m * LANES : (m + 1) * LANES, h * LANES : (h + 1) * LANES] = jnp.where(
                code < float(K), ref[m] - center, 0.0
            )
    out[...] = dot(table[...], flat[...], ((1,), (1,)))
    for p in range(peers):
        at = MARGIN + step * p
        send[p, pack.code : pack.code + 4, :] = rest[p, 0:4, :]
        for m in range(M):
            send[p, pack.wide * m : pack.wide * (m + 1), :] = out[
                at - 2 : at + step + 2, m * LANES : (m + 1) * LANES
            ]


def slab_row_filter(rows, slab_table, row_table, first, second, grid):
    ns, nr = grid
    mixed = dot(first[...], slab_table[...])
    for sb in range(ns):
        for rb in range(nr):
            second[sb * rows : (sb + 1) * rows, rb * LANES : (rb + 1) * LANES] = mixed[
                rb * rows : (rb + 1) * rows, sb * LANES : (sb + 1) * LANES
            ]
    return dot(second[...], row_table[...])


def around(get, sb, rb, grid, rows, fill):
    ns, nr = grid
    lane = lax.broadcasted_iota(jnp.int32, (1, LANES), 1)
    place = lane % rows
    here = get(sb, rb)
    empty = jnp.full_like(here, fill)
    above = get(sb + 1, rb) if sb + 1 < ns else empty
    below = get(sb - 1, rb) if sb > 0 else empty
    out = [
        pltpu.roll(jnp.where(lane >= rows, here, above), LANES - rows, 1),
        pltpu.roll(jnp.where(lane < LANES - rows, here, below), rows, 1),
    ]
    right = pltpu.roll(get(sb, rb + 1), rows - 1, 1) if rb + 1 < nr else empty
    left = pltpu.roll(get(sb, rb - 1), LANES - rows + 1, 1) if rb > 0 else empty
    out.append(jnp.where(place < rows - 1, pltpu.roll(here, LANES - 1, 1), right))
    out.append(jnp.where(place > 0, pltpu.roll(here, 1, 1), left))
    return out


def pencil_kernel(
    pack,
    grid,
    rows,
    got,
    raw,
    slab_table,
    row_table,
    send,
    keep,
    first,
    second,
    bias,
    codes,
    marks,
    shaded,
    dens,
    one,
    two,
):
    ns, nr = grid
    peers = ns * nr
    core = pack.core
    window = core + 2 * EDGE
    means, halves, shift = class_stats(peer_sum(raw, pack.stat))
    first[...] = jnp.zeros_like(first)
    for sb in range(ns):
        for rb in range(nr):
            for m in range(M):
                base = (rb * M + m) * window + EDGE - 2
                first[base : base + pack.wide, sb * LANES : (sb + 1) * LANES] = got[
                    sb * nr + rb, m * pack.wide : (m + 1) * pack.wide, :
                ]
    bias[...] = slab_row_filter(M * window, slab_table, row_table, first, second, grid)
    blank = jnp.full((window, LANES), float(K), jnp.float32)
    for sb in range(ns):
        for rb in range(nr):
            j = sb * nr + rb
            codes[j] = blank
            codes[j, EDGE - 3 : EDGE - 1, :] = got[j, pack.code : pack.code + 2, :]
            codes[j, EDGE - 1 : EDGE + core + 1, :] = raw[j, pack.code : pack.stat, :]
            codes[j, EDGE + core + 1 : EDGE + core + 3, :] = got[j, pack.code + 2 : pack.code + 4, :]
            for m in range(M):
                base = (sb * M + m) * window
                shaded[j, m] = -bias[base : base + window, rb * LANES : (rb + 1) * LANES]
                shaded[j, m, EDGE - 2 : EDGE - 2 + pack.wide, :] += raw[
                    j, m * pack.wide : (m + 1) * pack.wide, :
                ]

    def bits(x):
        whole = x.astype(jnp.int32)
        return jnp.where(whole < K, lax.shift_left(jnp.ones_like(whole), whole * FIELD), 0)

    for j in range(peers):
        marks[j] = bits(codes[j])

    for sb in range(ns):
        for rb in range(nr):
            j = sb * nr + rb
            logits = log_terms([shaded[j, m] for m in range(M)], means, halves, shift)
            code = codes[j]
            here = marks[j]
            near = around(lambda a, b: marks[a * nr + b], sb, rb, grid, rows, 0)
            near = near + [pltpu.roll(here, 1, 0), pltpu.roll(here, window - 1, 0)]
            near = functools.reduce(jnp.add, near)
            for k in range(K):
                dens[k, j] = logits[k]
                number = lax.shift_right_logical(near, jnp.full_like(near, k * FIELD))
                logits[k] = logits[k] + (number & (2**FIELD - 1)).astype(jnp.float32)
            inside = (code < float(K)).astype(jnp.float32)
            for k, value in enumerate(soft(logits, inside)):
                one[k, j] = value
    for sb in range(ns):
        for rb in range(nr):
            j = sb * nr + rb
            logits = []
            for k in range(K):
                here = one[k, j]
                near = around(lambda a, b: one[k, a * nr + b], sb, rb, grid, rows, 0.0)
                near = near + [pltpu.roll(here, 1, 0), pltpu.roll(here, window - 1, 0)]
                logits.append(dens[k, j] + functools.reduce(jnp.add, near))
            inside = (codes[j] < float(K)).astype(jnp.float32)
            for k, value in enumerate(soft(logits, inside)):
                two[k, j] = value
    sums = [[jnp.zeros((SUB, LANES), jnp.float32) for _ in range(STATS)] for _ in range(K)]
    for sb in range(ns):
        for rb in range(nr):
            j = sb * nr + rb
            values = [shaded[j, m, EDGE : EDGE + core, :] for m in range(M)]
            totals = []
            for k in range(K):
                here = two[k, j, EDGE : EDGE + core, :]
                keep[k, j] = here
                line = sums[k]
                line[0] = line[0] + fold(here)
                for m in range(M):
                    value = here * values[m]
                    line[1 + m] = line[1 + m] + fold(value)
                    line[1 + M + m] = line[1 + M + m] + fold(value * values[m])
                near = around(
                    lambda a, b: two[k, a * nr + b, EDGE : EDGE + core, :], sb, rb, grid, rows, 0.0
                )
                near = near + [
                    two[k, j, EDGE - 1 : EDGE - 1 + core, :],
                    two[k, j, EDGE + 1 : EDGE + 1 + core, :],
                ]
                totals.append(functools.reduce(jnp.add, near))
            for k in range(K - 1):
                send[j, k * core : (k + 1) * core, :] = totals[k] - totals[K - 1]
    row = stat_row(sums)
    for p in range(peers):
        send[p, (K - 1) * core : (K - 1) * core + 1, :] = row


def residual_kernel(
    pack, grid, stat_a, stat_b, keep, raw, slab_table, row_table, send, first, second
):
    ns, nr = grid
    core = pack.core
    means = mean_rows(stat_a[...] + stat_b[...])
    for sb in range(ns):
        for rb in range(nr):
            j = sb * nr + rb
            for m in range(M):
                base = m * pack.wide + 2
                field = raw[j, base : base + core, :]
                total = jnp.zeros_like(field)
                for k in range(K):
                    total = total + keep[k, j] * (field - means[m][k : k + 1, :])
                base = (rb * M + m) * core
                first[base : base + core, sb * LANES : (sb + 1) * LANES] = total
    rows = M * core
    done = slab_row_filter(rows, slab_table, row_table, first, second, grid)
    for sb in range(ns):
        for rb in range(nr):
            send[sb * nr + rb] = done[sb * rows : (sb + 1) * rows, rb * LANES : (rb + 1) * LANES]


def columns_of(ref, m, core):
    return ref[:, m * core : (m + 1) * core, :].reshape(LANES, LANES).T


def half_kernel(got, near, table, field, around):
    core = got.shape[1] // M
    for m in range(M):
        field[m] = dot(columns_of(got, m, core), table[:LANES, :])
    for k in range(K - 1):
        around[k] = columns_of(near, k, core)


def third_kernel(
    rows,
    field,
    got,
    near,
    own,
    stat_a,
    stat_b,
    table,
    place,
    bias_h,
    centers,
    dens,
    belief,
    up,
    down,
    side,
    edge,
    bias,
    sems,
):
    core = got.shape[1] // M
    slabs = LANES // rows
    means, halves, shift = class_stats(stat_a[...] + stat_b[...])
    for m in range(M):
        centers[:, m : m + 1] = means[m][:, :1]
        bias[m] = field[m] + dot(columns_of(got, m, core), table[LANES:, :])
    copy = pltpu.make_async_copy(bias, bias_h, sems.at[0])
    copy.start()
    lane = lax.broadcasted_iota(jnp.int32, (1, LANES), 1)
    even = jnp.full((rows, LANES), place[0] % 2, jnp.int32) == 0
    amounts = [jnp.where(place[2] == 0, k + 1, k) for k in range(K)]
    for s in range(slabs):
        low, high = s * rows, (s + 1) * rows
        corrected = [own[m, low:high, :] - bias[m, low:high, :] for m in range(M)]
        logits = log_terms(corrected, means, halves, shift)
        for k in range(K):
            dens[k, low:high, :] = logits[k]
            if k < K - 1:
                logits[k] = logits[k] + near[k, low:high, :]
        inside = (own[M, low:high, :] < float(K)).astype(jnp.float32)
        column = jnp.zeros((rows, LANES), jnp.float32)
        for k, value in enumerate(soft(logits, inside)):
            belief[k, low:high, :] = value
            column = jnp.where(lane == k, pltpu.roll(value, amounts[k], 1), column)
        edge[low:high, :] = column
    for k in range(K):
        first = belief[k, :rows, :]
        final = belief[k, LANES - rows :, :]
        up[k] = jnp.where(even, final, first)
        down[k] = jnp.where(even, first, final)
    lead = jnp.full((slabs, LANES), place[1], jnp.int32) == 0
    for k in range(K):
        head = belief[k, pl.ds(0, slabs, rows), :]
        tail = belief[k, pl.ds(rows - 1, slabs, rows), :]
        side[k] = jnp.where(lead, tail, head)
    copy.wait()


def inner_kernel(rows, dens, belief, logits):
    lane = lax.broadcasted_iota(jnp.int32, (1, LANES), 1)
    line = lax.broadcasted_iota(jnp.int32, (rows, 1), 0)
    for k in range(K):
        for low in range(0, LANES, rows):
            here = belief[k, low : low + rows, :]
            total = dens[k, low : low + rows, :]
            if low > 0:
                total = total + belief[k, low - rows : low, :]
            if low + rows < LANES:
                total = total + belief[k, low + rows : low + 2 * rows, :]
            total = total + jnp.where(line > 0, pltpu.roll(here, 1, 0), 0.0)
            total = total + jnp.where(line < rows - 1, pltpu.roll(here, rows - 1, 0), 0.0)
            total = total + jnp.where(lane > 0, pltpu.roll(here, 1, 1), 0.0)
            total = total + jnp.where(lane < LANES - 1, pltpu.roll(here, LANES - 1, 1), 0.0)
            logits[k, low : low + rows, :] = total


def last_kernel(rows, inner, own, up, down, side, edge, place, post_h, post, sems):
    slabs = LANES // rows
    lane = lax.broadcasted_iota(jnp.int32, (1, LANES), 1)
    line = lax.broadcasted_iota(jnp.int32, (rows, 1), 0)
    even = jnp.full((rows, LANES), place[0] % 2, jnp.int32) == 0
    spot = jnp.where(place[2] == 0, LANES - 1, 0)
    face = jnp.where(place[1] == 0, rows - 1, 0)
    amounts = [jnp.where(place[2] == 0, LANES - 1 - k, (LANES - k) % LANES) for k in range(K)]
    copies = []
    for s in range(slabs):
        low, high = s * rows, (s + 1) * rows
        column = edge[low:high, :]
        logits = []
        for k in range(K):
            total = inner[k, low:high, :]
            if s == 0:
                total = total + jnp.where(even, down[k], up[k])
            if s == slabs - 1:
                total = total + jnp.where(even, up[k], down[k])
            total = total + jnp.where(line == face, side[k, s : s + 1, :], 0.0)
            total = total + jnp.where(lane == spot, pltpu.roll(column, amounts[k], 1), 0.0)
            logits.append(total)
        inside = (own[M, low:high, :] < float(K)).astype(jnp.float32)
        for k, value in enumerate(soft(logits, inside)):
            post[k, low:high, :] = value.astype(jnp.bfloat16)
        if s % 2:
            span = pl.ds(low - rows, 2 * rows)
            copies.append(
                pltpu.make_async_copy(post.at[:, span, :], post_h.at[:, span, :], sems.at[s // 2])
            )
            copies[-1].start()
    for copy in copies:
        copy.wait()


class Pack(typing.NamedTuple):
    core: int
    wide: int
    code: int
    stat: int


def padded(rows):
    return -(-rows // SUB) * SUB


def call(kernel, outs, scratch=(), scalars=(), micros=1, far_out=()):
    vmem = pl.BlockSpec(memory_space=pltpu.VMEM)
    smem = pl.BlockSpec(memory_space=pltpu.SMEM)
    far = pl.BlockSpec(memory_space=pltpu.HBM)
    shapes = [jax.ShapeDtypeStruct(shape, kind) for shape, kind in outs]

    def run(*args):
        return pl.pallas_call(
            kernel,
            out_shape=shapes,
            in_specs=[smem if i in scalars else vmem for i in range(len(args))],
            out_specs=[far if i in far_out else vmem for i in range(len(shapes))],
            scratch_shapes=[
                pltpu.VMEM(x, jnp.float32) if isinstance(x, tuple) else x for x in scratch
            ],
            compiler_params=pltpu.CompilerParams(vmem_limit_bytes=VMEM_BYTES),
            cost_estimate=pl.CostEstimate(
                flops=micros * 10_000_000, bytes_accessed=2**20, transcendentals=0
            ),
            name=(kernel.func if isinstance(kernel, functools.partial) else kernel).__name__,
        )(*args)

    return run


def pencils(image, brain_mask, labels):
    _, slabs, rows, columns = image.shape
    ns, nr, nc = (lax.axis_size(a) for a in ("slab", "row", "col"))
    grid = (ns, nr)
    peers = ns * nr
    core = columns // peers
    window = core + 2 * EDGE
    wide_rows = core + 4
    pack = Pack(core, wide_rows, M * wide_rows, M * wide_rows + core + 2)
    f32 = jnp.float32
    place = jnp.stack([lax.axis_index(a) for a in ("slab", "row", "col")]).astype(jnp.int32)
    swap = [(0, 1), (1, 0)]

    taps = impulse(columns * nc)
    reach = np.arange(-MARGIN, columns + MARGIN)
    source = np.concatenate([np.arange(columns), np.arange(columns) + columns])
    spread = taps[(reach[:, None] - source[None, :]) % (columns * nc)].astype(np.float32)
    gather = np.ascontiguousarray(spread[MARGIN : MARGIN + columns].T)
    slab_table = np.kron(dense(slabs * ns), np.eye(rows)).astype(np.float32)
    row_table = np.einsum(
        "arbq,st->asrbtq", dense(rows * nr).reshape(nr, rows, nr, rows), np.eye(slabs)
    )
    row_table = row_table.reshape(nr * LANES, nr * LANES).astype(np.float32)

    code = jnp.where(brain_mask > 0, labels, K).astype(f32)
    own = jnp.concatenate([image, code[None]]).reshape(M + 1, LANES, columns)
    oth = lax.ppermute(own, "col", swap)

    def trade(x):
        return lax.all_to_all(x, ("slab", "row"), split_axis=0, concat_axis=0, tiled=True)

    turned, stat = call(
        own_kernel, [((M + 1, columns, LANES), f32), ((SUB, LANES), f32)]
    )(own)
    sent, rest = call(
        functools.partial(prepare_kernel, pack),
        [((peers, padded(pack.stat + 1), LANES), f32), ((peers, SUB, LANES), f32)],
        [(M + 1, columns + 2 * MARGIN, LANES)],
        (3,),
    )(turned, stat, oth, place)
    raw = trade(sent)
    (sent,) = call(
        functools.partial(column_kernel, pack),
        [((peers, padded(pack.code + 4), LANES), f32)],
        [(M * LANES, 2 * columns), (columns + 2 * MARGIN, M * LANES)],
    )(own, oth, raw, rest, spread)
    got = trade(sent)
    sent, keep = call(
        functools.partial(pencil_kernel, pack, grid, rows),
        [
            ((peers, padded((K - 1) * core + 1), LANES), f32),
            ((K, peers, core, LANES), f32),
        ],
        [
            (nr * M * window, ns * LANES),
            (ns * M * window, nr * LANES),
            (ns * M * window, nr * LANES),
            (peers, window, LANES),
            pltpu.VMEM((peers, window, LANES), jnp.int32),
            (peers, M, window, LANES),
            (K, peers, window, LANES),
            (K, peers, window, LANES),
            (K, peers, window, LANES),
        ],
        micros=4,
    )(got, raw, slab_table, row_table)
    near = trade(sent)
    stat_a = jnp.sum(near[:, (K - 1) * core : (K - 1) * core + 1, :], axis=0)
    stat_b = lax.ppermute(stat_a, "col", swap)
    (sent,) = call(
        functools.partial(residual_kernel, pack, grid),
        [((peers, M * core, LANES), f32)],
        [(nr * M * core, ns * LANES), (ns * M * core, nr * LANES)],
    )(stat_a, stat_b, keep, raw, slab_table, row_table)
    got = trade(sent)
    yours = lax.ppermute(got, "col", swap)
    field, near = call(
        half_kernel, [((M, LANES, columns), f32), ((K - 1, LANES, columns), f32)]
    )(got, near, gather)
    bias, centers, dens, belief, up, down, side, edge = call(
        functools.partial(third_kernel, rows),
        [
            ((M, LANES, columns), f32),
            ((K, M), f32),
            ((K, LANES, columns), f32),
            ((K, LANES, columns), f32),
            ((K, rows, columns), f32),
            ((K, rows, columns), f32),
            ((K, slabs, columns), f32),
            ((LANES, LANES), f32),
        ],
        [(M, LANES, columns), pltpu.SemaphoreType.DMA((1,))],
        (7,),
        2,
        far_out=(0,),
    )(field, yours, near, own, stat_a, stat_b, gather, place)
    pairs = [(i, i + 1) for i in range(0, ns - 1, 2)]
    between = [(i, i + 1) for i in range(1, ns - 1, 2)]
    up = lax.ppermute(up, "slab", pairs + [(b, a) for a, b in pairs])
    down = lax.ppermute(down, "slab", between + [(b, a) for a, b in between])
    side = lax.ppermute(side, "row", swap)
    edge = lax.ppermute(edge, "col", swap)
    (inner,) = call(functools.partial(inner_kernel, rows), [((K, LANES, columns), f32)])(
        dens, belief
    )
    (post,) = call(
        functools.partial(last_kernel, rows),
        [((K, LANES, columns), jnp.bfloat16)],
        [
            pltpu.VMEM((K, LANES, columns), jnp.bfloat16),
            pltpu.SemaphoreType.DMA((slabs // 2,)),
        ],
        (6,),
        far_out=(0,),
    )(inner, own, up, down, side, edge, place)
    shape = (slabs, rows, columns)
    return post.reshape((K,) + shape), bias.reshape((M,) + shape), centers


def local(image, brain_mask, labels):
    _, slabs, rows, columns = image.shape
    peers = lax.axis_size("slab") * lax.axis_size("row")
    fits = slabs * rows == LANES and columns == LANES and slabs % SUB == 0 and rows % SUB == 0
    fits = fits and lax.axis_size("row") == 2 and lax.axis_size("col") == 2
    fits = fits and columns % (SUB * peers) == 0
    return (pencils if fits else general)(image, brain_mask, labels)


def solution(mesh):
    placed = (
        P(None, ("grp", "slab"), "row", "col"),
        P(("grp", "slab"), "row", "col"),
        P(("grp", "slab"), "row", "col"),
    )
    return jax.shard_map(
        local,
        mesh=mesh,
        in_specs=placed,
        out_specs=(
            P(None, ("grp", "slab"), "row", "col"),
            P(None, ("grp", "slab"), "row", "col"),
            P("grp", None),
        ),
        check_vma=False,
    )
```

```python
import functools
import math
import typing

import jax
import jax.numpy as jnp
import numpy as np
from jax import lax
from jax.experimental import pallas as pl
from jax.experimental.pallas import tpu as pltpu
from jax.sharding import PartitionSpec as P

M = 3
K = 8
EM_ITERS = 2
MF_PASSES = 2


highest = lax.Precision.HIGHEST
coupling = 1.0
breadth = 8.0


def extended(cells, sides, width):
    for axis, dim in sides:
        count = lax.axis_size(axis)
        ends = count - 1
        head = lax.slice_in_dim(cells, 0, width, axis=dim)
        tail = lax.slice_in_dim(cells, cells.shape[dim] - width, cells.shape[dim], axis=dim)
        cells = jnp.concatenate(
            [
                lax.ppermute(tail, axis, [(i, (i + 1) % count) for i in range(ends)]),
                cells,
                lax.ppermute(head, axis, [((i + 1) % count, i) for i in range(ends)]),
            ],
            axis=dim,
        )
    return cells


def circulant(length):
    index = jnp.arange(length, dtype=jnp.int32)
    folded = jnp.minimum(index, length - index).astype(jnp.float32) / length
    response = jnp.exp(-2.0 * math.pi**2 * (length / breadth) ** 2 * folded * folded)
    product = index[:, None] * index[None, :] % length
    angles = 2.0 * math.pi / length * product.astype(jnp.float32)
    cosine = jnp.cos(angles)
    sine = jnp.sin(angles)
    even_part = jnp.dot(cosine * response[None, :], cosine.T, precision=highest)
    odd_part = jnp.dot(sine * response[None, :], sine.T, precision=highest)
    return (even_part + odd_part) / length


def neighbour_sum(belief):
    padded = extended(belief, (("slab", 1), ("row", 2), ("col", 3)), 1)
    total = padded[:, 2:, 1:-1, 1:-1] + padded[:, :-2, 1:-1, 1:-1]
    total = total + padded[:, 1:-1, 2:, 1:-1] + padded[:, 1:-1, :-2, 1:-1]
    total = total + padded[:, 1:-1, 1:-1, 2:] + padded[:, 1:-1, 1:-1, :-2]
    return total


def class_moments(belief, corrected):
    flat = belief.reshape(K, -1)
    values = corrected.reshape(M, -1)
    count, first, squares = lax.psum(
        (
            jnp.sum(flat, axis=1),
            jnp.dot(flat, values.T, precision=highest),
            jnp.dot(flat, (values * values).T, precision=highest),
        ),
        ("slab", "row", "col"),
    )
    means = first / (count + 1.0)[:, None]
    spread = squares - 2.0 * means * first + means * means * count[:, None]
    variance = (spread + 1.0) / (count + 1.0)[:, None]
    return (count, means, variance)


def log_density(corrected, means, variance, prior):
    offset = corrected[None] - means[:, :, None, None, None]
    terms = (
        offset * offset / variance[:, :, None, None, None]
        + jnp.log(variance)[:, :, None, None, None]
    )
    return jnp.log(prior)[:, None, None, None] - 0.5 * jnp.sum(terms, axis=1)


def smoothed(residual, column_local, row_table, slab_table):
    across = jnp.einsum(
        "msrc,cd->msrd",
        lax.all_gather(residual, "col", axis=3, tiled=True),
        column_local,
        precision=highest,
    )
    mixed = jnp.einsum(
        "msrc,rq->msqc",
        lax.all_to_all(across, "row", split_axis=1, concat_axis=2, tiled=True),
        row_table,
        precision=highest,
    )
    across = lax.all_to_all(mixed, "row", split_axis=2, concat_axis=1, tiled=True)
    mixed = jnp.einsum(
        "msrc,sq->mqrc",
        lax.all_to_all(across, "slab", split_axis=2, concat_axis=1, tiled=True),
        slab_table,
        precision=highest,
    )
    return lax.all_to_all(mixed, "slab", split_axis=1, concat_axis=2, tiled=True)


def general(image, brain_mask, labels):
    channels, slabs, rows, columns = image.shape
    inside = brain_mask.astype(jnp.float32)
    kinds = jnp.arange(K, dtype=jnp.int32)
    belief = (labels[None] == kinds[:, None, None, None]).astype(jnp.float32) * inside[None]
    column_table = circulant(columns * lax.axis_size("col"))
    column_local = lax.dynamic_slice_in_dim(
        column_table, lax.axis_index("col") * columns, columns, 1
    )
    row_table = circulant(rows * lax.axis_size("row"))
    slab_table = circulant(slabs * lax.axis_size("slab"))
    bias_field = jnp.zeros_like(image)
    means = jnp.zeros((K, channels), jnp.float32)
    for iteration in range(EM_ITERS):
        corrected = image - bias_field
        count, means, variance = class_moments(belief, corrected)
        prior = (count + 1.0) / (jnp.sum(count) + K)
        total = jnp.sum(belief, axis=0)
        removed = jnp.dot(means.T, belief.reshape(K, -1), precision=highest).reshape(image.shape)
        residual = image * total[None] - removed
        bias_field = smoothed(residual, column_local, row_table, slab_table)
        corrected = image - bias_field
        density = log_density(corrected, means, variance, prior)
        for sweep_index in range(MF_PASSES):
            belief = (
                jax.nn.softmax(density + coupling * neighbour_sum(belief), axis=0) * inside[None]
            )
    return (belief.astype(jnp.bfloat16), bias_field, means)


LANES = 128
SUB = 8
EDGE = 4
MARGIN = 8
FIELD = 4
STATS = 1 + 2 * M
VMEM_BYTES = 16 * 2**20


def impulse(length):
    index = np.arange(length)
    folded = np.minimum(index, length - index) / length
    response = np.exp(-2.0 * np.pi**2 * (length / breadth) ** 2 * folded * folded)
    angles = 2.0 * np.pi / length * (index[:, None] * index[None, :] % length)
    return np.cos(angles) @ response / length


def dense(length):
    index = np.arange(length)
    return impulse(length)[(index[:, None] - index[None, :]) % length]


def halves_of(x):
    high = x.astype(jnp.bfloat16)
    return high, (x - high.astype(jnp.float32)).astype(jnp.bfloat16)


def table_of(x):
    high = x.astype(jnp.bfloat16)
    low = (x - high.astype(np.float64)).astype(jnp.bfloat16)
    return np.stack([high, low])


def dot(left, right, dims=((1,), (0,))):
    left, right = (x if isinstance(x, tuple) else halves_of(x) for x in (left, right))

    def one(a, b):
        return lax.dot_general(a, b, (dims, ((), ())), preferred_element_type=jnp.float32)

    return one(left[0], right[0]) + (one(left[1], right[0]) + one(left[0], right[1]))


def wide(row, shape=(SUB, LANES)):
    return jnp.broadcast_to(row, shape)


def stat_row(sums):
    sub = lax.broadcasted_iota(jnp.int32, (SUB, LANES), 0)
    lane = lax.broadcasted_iota(jnp.int32, (SUB, LANES), 1)
    tile = jnp.zeros((SUB, LANES), jnp.float32)
    for q in range(STATS):
        rows = jnp.zeros((SUB, LANES), jnp.float32)
        for k in range(K):
            line = jnp.sum(sums[k][q], axis=0, keepdims=True)
            rows = jnp.where(sub == k, line, rows)
        tile = jnp.where(lane == q * K + sub, jnp.sum(rows, axis=1, keepdims=True), tile)
    return jnp.sum(tile, axis=0, keepdims=True)


def stat_columns(row, number):
    sub = lax.broadcasted_iota(jnp.int32, (SUB, LANES), 0)
    lane = lax.broadcasted_iota(jnp.int32, (SUB, LANES), 1)
    return [
        jnp.sum(jnp.where(lane == q * K + sub, row, 0.0), axis=1, keepdims=True)
        for q in range(number)
    ]


def fold(x):
    return jnp.sum(x.reshape(x.shape[0] // SUB, SUB, LANES), axis=0)


def class_stats(row):
    count, *rest = stat_columns(row, STATS)
    means, halves = [], []
    shift = jnp.zeros_like(count)
    for m in range(M):
        first, squares = rest[m], rest[M + m]
        mean = first / (count + 1.0)
        spread = squares - 2.0 * mean * first + mean * mean * count
        variance = (spread + 1.0) / (count + 1.0)
        means.append(wide(mean))
        halves.append(wide(0.5 / variance))
        shift = shift - 0.5 * jnp.log(variance)
    prior = (count + 1.0) / (jnp.sum(count, axis=0, keepdims=True) + K)
    return means, halves, wide(jnp.log(prior) + shift)


def mean_rows(row):
    count, *rest = stat_columns(row, 1 + M)
    return [wide(x / (count + 1.0)) for x in rest]


def log_terms(corrected, means, halves, shift):
    out = []
    for k in range(K):
        total = wide(shift[k : k + 1, :], corrected[0].shape)
        for m in range(M):
            offset = corrected[m] - means[m][k : k + 1, :]
            total = total - offset * offset * halves[m][k : k + 1, :]
        out.append(total)
    return out


def soft(logits, inside):
    top = functools.reduce(jnp.maximum, logits)
    exps = [jnp.exp(x - top) for x in logits]
    scale = inside / functools.reduce(jnp.add, exps)
    return [x * scale for x in exps]


def peer_sum(ref, line):
    row = ref[0, line : line + 1, :]
    for j in range(1, ref.shape[0]):
        row = row + ref[j, line : line + 1, :]
    return row


def class_sums(code, image):
    sums = []
    for k in range(K):
        flag = (code == float(k)).astype(jnp.float32)
        line = [fold(flag)]
        weighted = [flag * image[m] for m in range(M)]
        line += [fold(x) for x in weighted]
        line += [fold(x * image[m]) for m, x in enumerate(weighted)]
        sums.append(line)
    return sums


def own_kernel(own, turned, stat):
    stat[...] = wide(stat_row(class_sums(own[M], own)))
    for f in range(M + 1):
        turned[f] = own[f].T


def prepare_kernel(pack, turned, stat, oth, place, send, rest, ext):
    peers = send.shape[0]
    step = LANES // peers
    first = place[2] == 0
    row = stat[0:1, :] + stat_row(class_sums(oth[M], oth))
    for f in range(M + 1):
        blank = jnp.full((SUB, LANES), float(K) if f == M else 0.0, jnp.float32)
        other = oth[f].T
        ext[f, 0:MARGIN, :] = jnp.where(first, blank, other[LANES - MARGIN :, :])
        ext[f, MARGIN : MARGIN + LANES, :] = turned[f]
        ext[f, MARGIN + LANES :, :] = jnp.where(first, other[:MARGIN, :], blank)
    for p in range(peers):
        at = MARGIN + step * p
        for m in range(M):
            send[p, pack.wide * m : pack.wide * (m + 1), :] = ext[m, at - 2 : at + step + 2, :]
        send[p, pack.code : pack.stat, :] = ext[M, at - 1 : at + step + 1, :]
        send[p, pack.stat : pack.stat + 1, :] = row
        rest[p, 0:2, :] = ext[M, at - 3 : at - 1, :]
        rest[p, 2:4, :] = ext[M, at + step + 1 : at + step + 3, :]


def column_kernel(pack, own, oth, got, rest, table, send, flat, out):
    peers = send.shape[0]
    step = LANES // peers
    means = mean_rows(peer_sum(got, pack.stat))
    for h, ref in enumerate((own, oth)):
        code = ref[M]
        flags = [code == float(k) for k in range(K)]
        for m in range(M):
            center = jnp.zeros_like(code)
            for k in range(K):
                center = jnp.where(flags[k], means[m][k : k + 1, :], center)
            flat[m * LANES : (m + 1) * LANES, h * LANES : (h + 1) * LANES] = jnp.where(
                code < float(K), ref[m] - center, 0.0
            )
    out[...] = dot((table[0], table[1]), flat[...], ((1,), (1,)))
    for p in range(peers):
        at = MARGIN + step * p
        send[p, pack.code : pack.code + 4, :] = rest[p, 0:4, :]
        for m in range(M):
            send[p, pack.wide * m : pack.wide * (m + 1), :] = out[
                at - 2 : at + step + 2, m * LANES : (m + 1) * LANES
            ]


def slab_row_filter(rows, slab_table, row_table, first, second, grid):
    ns, nr = grid
    mixed = dot(first[...], (slab_table[0], slab_table[1]))
    for sb in range(ns):
        for rb in range(nr):
            second[sb * rows : (sb + 1) * rows, rb * LANES : (rb + 1) * LANES] = mixed[
                rb * rows : (rb + 1) * rows, sb * LANES : (sb + 1) * LANES
            ]
    return dot(second[...], (row_table[0], row_table[1]))


def around(get, sb, rb, grid, rows, fill):
    ns, nr = grid
    lane = lax.broadcasted_iota(jnp.int32, (1, LANES), 1)
    place = lane % rows
    here = get(sb, rb)
    empty = jnp.full_like(here, fill)
    above = get(sb + 1, rb) if sb + 1 < ns else empty
    below = get(sb - 1, rb) if sb > 0 else empty
    out = [
        pltpu.roll(jnp.where(lane >= rows, here, above), LANES - rows, 1),
        pltpu.roll(jnp.where(lane < LANES - rows, here, below), rows, 1),
    ]
    right = pltpu.roll(get(sb, rb + 1), rows - 1, 1) if rb + 1 < nr else empty
    left = pltpu.roll(get(sb, rb - 1), LANES - rows + 1, 1) if rb > 0 else empty
    out.append(jnp.where(place < rows - 1, pltpu.roll(here, LANES - 1, 1), right))
    out.append(jnp.where(place > 0, pltpu.roll(here, 1, 1), left))
    return out


def pencil_kernel(
    pack,
    grid,
    rows,
    got,
    raw,
    slab_table,
    row_table,
    send,
    keep,
    first,
    second,
    bias,
    codes,
    marks,
    shaded,
    dens,
    one,
    two,
):
    ns, nr = grid
    peers = ns * nr
    core = pack.core
    window = core + 2 * EDGE
    means, halves, shift = class_stats(peer_sum(raw, pack.stat))
    first[...] = jnp.zeros_like(first)
    for sb in range(ns):
        for rb in range(nr):
            for m in range(M):
                base = (rb * M + m) * window + EDGE - 2
                first[base : base + pack.wide, sb * LANES : (sb + 1) * LANES] = got[
                    rb * ns + sb, m * pack.wide : (m + 1) * pack.wide, :
                ]
    bias[...] = slab_row_filter(M * window, slab_table, row_table, first, second, grid)
    blank = jnp.full((window, LANES), float(K), jnp.float32)
    for sb in range(ns):
        for rb in range(nr):
            j = rb * ns + sb
            codes[j] = blank
            codes[j, EDGE - 3 : EDGE - 1, :] = got[j, pack.code : pack.code + 2, :]
            codes[j, EDGE - 1 : EDGE + core + 1, :] = raw[j, pack.code : pack.stat, :]
            codes[j, EDGE + core + 1 : EDGE + core + 3, :] = got[j, pack.code + 2 : pack.code + 4, :]
            for m in range(M):
                base = (sb * M + m) * window
                shaded[j, m] = -bias[base : base + window, rb * LANES : (rb + 1) * LANES]
                shaded[j, m, EDGE - 2 : EDGE - 2 + pack.wide, :] += raw[
                    j, m * pack.wide : (m + 1) * pack.wide, :
                ]

    def bits(x):
        whole = x.astype(jnp.int32)
        return jnp.where(whole < K, lax.shift_left(jnp.ones_like(whole), whole * FIELD), 0)

    for j in range(peers):
        marks[j] = bits(codes[j])

    for sb in range(ns):
        for rb in range(nr):
            j = rb * ns + sb
            logits = log_terms([shaded[j, m] for m in range(M)], means, halves, shift)
            code = codes[j]
            here = marks[j]
            near = around(lambda a, b: marks[b * ns + a], sb, rb, grid, rows, 0)
            near = near + [pltpu.roll(here, 1, 0), pltpu.roll(here, window - 1, 0)]
            near = functools.reduce(jnp.add, near)
            for k in range(K):
                dens[k, j] = logits[k]
                number = lax.shift_right_logical(near, jnp.full_like(near, k * FIELD))
                logits[k] = logits[k] + (number & (2**FIELD - 1)).astype(jnp.float32)
            inside = (code < float(K)).astype(jnp.float32)
            for k, value in enumerate(soft(logits, inside)):
                one[k, j] = value
    for sb in range(ns):
        for rb in range(nr):
            j = rb * ns + sb
            logits = []
            for k in range(K):
                here = one[k, j]
                near = around(lambda a, b: one[k, b * ns + a], sb, rb, grid, rows, 0.0)
                near = near + [pltpu.roll(here, 1, 0), pltpu.roll(here, window - 1, 0)]
                logits.append(dens[k, j] + functools.reduce(jnp.add, near))
            inside = (codes[j] < float(K)).astype(jnp.float32)
            for k, value in enumerate(soft(logits, inside)):
                two[k, j] = value
    sums = [[jnp.zeros((SUB, LANES), jnp.float32) for _ in range(STATS)] for _ in range(K)]
    for sb in range(ns):
        for rb in range(nr):
            j = rb * ns + sb
            values = [shaded[j, m, EDGE : EDGE + core, :] for m in range(M)]
            totals = []
            for k in range(K):
                here = two[k, j, EDGE : EDGE + core, :]
                keep[k, j] = here
                line = sums[k]
                line[0] = line[0] + fold(here)
                for m in range(M):
                    value = here * values[m]
                    line[1 + m] = line[1 + m] + fold(value)
                    line[1 + M + m] = line[1 + M + m] + fold(value * values[m])
                near = around(
                    lambda a, b: two[k, b * ns + a, EDGE : EDGE + core, :], sb, rb, grid, rows, 0.0
                )
                near = near + [
                    two[k, j, EDGE - 1 : EDGE - 1 + core, :],
                    two[k, j, EDGE + 1 : EDGE + 1 + core, :],
                ]
                totals.append(functools.reduce(jnp.add, near))
            for k in range(K - 1):
                send[j, k * core : (k + 1) * core, :] = totals[k] - totals[K - 1]
    row = stat_row(sums)
    for p in range(peers):
        send[p, (K - 1) * core : (K - 1) * core + 1, :] = row


def residual_kernel(
    pack, grid, stat_a, stat_b, keep, raw, slab_table, row_table, send, first, second
):
    ns, nr = grid
    core = pack.core
    means = mean_rows(stat_a[...] + stat_b[...])
    for sb in range(ns):
        for rb in range(nr):
            j = rb * ns + sb
            for m in range(M):
                base = m * pack.wide + 2
                field = raw[j, base : base + core, :]
                total = jnp.zeros_like(field)
                for k in range(K):
                    total = total + keep[k, j] * (field - means[m][k : k + 1, :])
                base = (rb * M + m) * core
                first[base : base + core, sb * LANES : (sb + 1) * LANES] = total
    rows = M * core
    done = slab_row_filter(rows, slab_table, row_table, first, second, grid)
    for sb in range(ns):
        for rb in range(nr):
            send[rb * ns + sb] = done[sb * rows : (sb + 1) * rows, rb * LANES : (rb + 1) * LANES]


def columns_of(ref, m, core):
    return ref[:, m * core : (m + 1) * core, :].reshape(LANES, LANES).T


def half_kernel(got, near, table, field, around):
    core = got.shape[1] // M
    for m in range(M):
        field[m] = dot(columns_of(got, m, core), (table[0, :LANES, :], table[1, :LANES, :]))
    for k in range(K - 1):
        around[k] = columns_of(near, k, core)


def third_kernel(
    rows,
    field,
    got,
    near,
    own,
    stat_a,
    stat_b,
    table,
    place,
    bias,
    centers,
    dens,
    belief,
    up,
    down,
    side,
    edge,
):
    core = got.shape[1] // M
    slabs = LANES // rows
    means, halves, shift = class_stats(stat_a[...] + stat_b[...])
    for m in range(M):
        centers[:, m : m + 1] = means[m][:, :1]
        bias[m] = field[m] + dot(
            columns_of(got, m, core), (table[0, LANES:, :], table[1, LANES:, :])
        )
    lane = lax.broadcasted_iota(jnp.int32, (1, LANES), 1)
    even = place[0, 0:1, :] == 0
    shiftback = jnp.where(place[2, 0:1, :] == 0, 1, 0)
    marks = [(lane + shiftback) % LANES == k for k in range(K)]
    for s in range(slabs):
        low, high = s * rows, (s + 1) * rows
        corrected = [own[m, low:high, :] - bias[m, low:high, :] for m in range(M)]
        logits = log_terms(corrected, means, halves, shift)
        for k in range(K):
            dens[k, low:high, :] = logits[k]
            if k < K - 1:
                logits[k] = logits[k] + near[k, low:high, :]
        inside = (own[M, low:high, :] < float(K)).astype(jnp.float32)
        column = jnp.zeros((rows, LANES), jnp.float32)
        for k, value in enumerate(soft(logits, inside)):
            belief[k, low:high, :] = value
            column = jnp.where(marks[k], pltpu.roll(value, k, 1), column)
        edge[low:high, :] = column
    for k in range(K):
        first = belief[k, :rows, :]
        final = belief[k, LANES - rows :, :]
        up[k] = jnp.where(even, final, first)
        down[k] = jnp.where(even, first, final)
    lead = place[1, 0:1, :] == 0
    for k in range(K):
        head = belief[k, pl.ds(0, slabs, rows), :]
        tail = belief[k, pl.ds(rows - 1, slabs, rows), :]
        side[k] = jnp.where(lead, tail, head)


def inner_kernel(rows, dens, belief, bias, logits, bias_h, sems):
    copy = pltpu.make_async_copy(bias, bias_h, sems.at[0])
    copy.start()
    lane = lax.broadcasted_iota(jnp.int32, (1, LANES), 1)
    line = lax.broadcasted_iota(jnp.int32, (rows, 1), 0)
    for k in range(K):
        for low in range(0, LANES, rows):
            here = belief[k, low : low + rows, :]
            total = dens[k, low : low + rows, :]
            if low > 0:
                total = total + belief[k, low - rows : low, :]
            if low + rows < LANES:
                total = total + belief[k, low + rows : low + 2 * rows, :]
            total = total + jnp.where(line > 0, pltpu.roll(here, 1, 0), 0.0)
            total = total + jnp.where(line < rows - 1, pltpu.roll(here, rows - 1, 0), 0.0)
            total = total + jnp.where(lane > 0, pltpu.roll(here, 1, 1), 0.0)
            total = total + jnp.where(lane < LANES - 1, pltpu.roll(here, LANES - 1, 1), 0.0)
            logits[k, low : low + rows, :] = total
    copy.wait()


def last_kernel(rows, inner, own, up, down, side, edge, place, post_h, post, sems):
    slabs = LANES // rows
    lane = lax.broadcasted_iota(jnp.int32, (1, LANES), 1)
    line = lax.broadcasted_iota(jnp.int32, (rows, 1), 0)
    even = place[0, 0:1, :] == 0
    left = place[2, 0:1, :] == 0
    spot = lane == jnp.where(left, LANES - 1, 0)
    face = line == jnp.where(place[1, 0:1, :] == 0, rows - 1, 0)
    copies = []
    for s in range(slabs):
        low, high = s * rows, (s + 1) * rows
        column = edge[low:high, :]
        column = jnp.where(left, column, pltpu.roll(column, 2, 1))
        logits = []
        for k in range(K):
            total = inner[k, low:high, :]
            if s == 0:
                total = total + jnp.where(even, down[k], up[k])
            if s == slabs - 1:
                total = total + jnp.where(even, up[k], down[k])
            total = total + jnp.where(face, side[k, s : s + 1, :], 0.0)
            total = total + jnp.where(spot, pltpu.roll(column, LANES - 1 - k, 1), 0.0)
            logits.append(total)
        inside = (own[M, low:high, :] < float(K)).astype(jnp.float32)
        for k, value in enumerate(soft(logits, inside)):
            post[k, low:high, :] = value.astype(jnp.bfloat16)
        if s % 2:
            span = pl.ds(low - rows, 2 * rows)
            copies.append(
                pltpu.make_async_copy(post.at[:, span, :], post_h.at[:, span, :], sems.at[s // 2])
            )
            copies[-1].start()
    for copy in copies:
        copy.wait()


class Pack(typing.NamedTuple):
    core: int
    wide: int
    code: int
    stat: int


def padded(rows):
    return -(-rows // SUB) * SUB


def call(kernel, outs, scratch=(), micros=1, far_out=()):
    vmem = pl.BlockSpec(memory_space=pltpu.VMEM)
    far = pl.BlockSpec(memory_space=pltpu.HBM)
    shapes = [jax.ShapeDtypeStruct(shape, kind) for shape, kind in outs]

    def run(*args):
        return pl.pallas_call(
            kernel,
            out_shape=shapes,
            in_specs=[vmem] * len(args),
            out_specs=[far if i in far_out else vmem for i in range(len(shapes))],
            scratch_shapes=[
                pltpu.VMEM(x, jnp.float32) if isinstance(x, tuple) else x for x in scratch
            ],
            compiler_params=pltpu.CompilerParams(vmem_limit_bytes=VMEM_BYTES),
            cost_estimate=pl.CostEstimate(
                flops=micros * 10_000_000, bytes_accessed=2**20, transcendentals=0
            ),
            name=(kernel.func if isinstance(kernel, functools.partial) else kernel).__name__,
        )(*args)

    return run


def pencils(image, brain_mask, labels):
    _, slabs, rows, columns = image.shape
    ns, nr, nc = (lax.axis_size(a) for a in ("slab", "row", "col"))
    grid = (ns, nr)
    peers = ns * nr
    core = columns // peers
    window = core + 2 * EDGE
    wide_rows = core + 4
    pack = Pack(core, wide_rows, M * wide_rows, M * wide_rows + core + 2)
    f32 = jnp.float32
    place = jnp.stack([lax.axis_index("slab") % 2, lax.axis_index("row"), lax.axis_index("col")])
    place = jnp.broadcast_to(place.astype(jnp.int32)[:, None, None], (3, SUB, LANES))
    swap = [(0, 1), (1, 0)]

    taps = impulse(columns * nc)
    reach = np.arange(-MARGIN, columns + MARGIN)
    source = np.concatenate([np.arange(columns), np.arange(columns) + columns])
    spread = taps[(reach[:, None] - source[None, :]) % (columns * nc)]
    gather = table_of(spread[MARGIN : MARGIN + columns].T)
    spread = table_of(spread)
    slab_table = table_of(np.kron(dense(slabs * ns), np.eye(rows)))
    row_table = np.einsum(
        "arbq,st->asrbtq", dense(rows * nr).reshape(nr, rows, nr, rows), np.eye(slabs)
    )
    row_table = table_of(row_table.reshape(nr * LANES, nr * LANES))

    code = jnp.where(brain_mask > 0, labels, K).astype(f32)
    own = jnp.concatenate([image, code[None]]).reshape(M + 1, LANES, columns)
    oth = lax.ppermute(own, "col", swap)

    def trade(x):
        return lax.all_to_all(x, ("row", "slab"), split_axis=0, concat_axis=0, tiled=True)

    turned, stat = call(
        own_kernel, [((M + 1, columns, LANES), f32), ((SUB, LANES), f32)]
    )(own)
    sent, rest = call(
        functools.partial(prepare_kernel, pack),
        [((peers, padded(pack.stat + 1), LANES), f32), ((peers, SUB, LANES), f32)],
        [(M + 1, columns + 2 * MARGIN, LANES)],
    )(turned, stat, oth, place)
    raw = trade(sent)
    (sent,) = call(
        functools.partial(column_kernel, pack),
        [((peers, padded(pack.code + 4), LANES), f32)],
        [(M * LANES, 2 * columns), (columns + 2 * MARGIN, M * LANES)],
    )(own, oth, raw, rest, spread)
    got = trade(sent)
    sent, keep = call(
        functools.partial(pencil_kernel, pack, grid, rows),
        [
            ((peers, padded((K - 1) * core + 1), LANES), f32),
            ((K, peers, core, LANES), f32),
        ],
        [
            (nr * M * window, ns * LANES),
            (ns * M * window, nr * LANES),
            (ns * M * window, nr * LANES),
            (peers, window, LANES),
            pltpu.VMEM((peers, window, LANES), jnp.int32),
            (peers, M, window, LANES),
            (K, peers, window, LANES),
            (K, peers, window, LANES),
            (K, peers, window, LANES),
        ],
        micros=4,
    )(got, raw, slab_table, row_table)
    near = trade(sent)
    stat_a = jnp.sum(near[:, (K - 1) * core : (K - 1) * core + 1, :], axis=0)
    stat_b = lax.ppermute(stat_a, "col", swap)
    (sent,) = call(
        functools.partial(residual_kernel, pack, grid),
        [((peers, M * core, LANES), f32)],
        [(nr * M * core, ns * LANES), (ns * M * core, nr * LANES)],
    )(stat_a, stat_b, keep, raw, slab_table, row_table)
    got = trade(sent)
    yours = lax.ppermute(got, "col", swap)
    field, near = call(
        half_kernel, [((M, LANES, columns), f32), ((K - 1, LANES, columns), f32)]
    )(got, near, gather)
    bias, centers, dens, belief, up, down, side, edge = call(
        functools.partial(third_kernel, rows),
        [
            ((M, LANES, columns), f32),
            ((K, M), f32),
            ((K, LANES, columns), f32),
            ((K, LANES, columns), f32),
            ((K, rows, columns), f32),
            ((K, rows, columns), f32),
            ((K, slabs, columns), f32),
            ((LANES, LANES), f32),
        ],
        micros=2,
    )(field, yours, near, own, stat_a, stat_b, gather, place)
    pairs = [(i, i + 1) for i in range(0, ns - 1, 2)]
    between = [(i, i + 1) for i in range(1, ns - 1, 2)]
    up = lax.ppermute(up, "slab", pairs + [(b, a) for a, b in pairs])
    down = lax.ppermute(down, "slab", between + [(b, a) for a, b in between])
    side = lax.ppermute(side, "row", swap)
    edge = lax.ppermute(edge, "col", swap)
    inner, bias = call(
        functools.partial(inner_kernel, rows),
        [((K, LANES, columns), f32), ((M, LANES, columns), f32)],
        [pltpu.SemaphoreType.DMA((1,))],
        far_out=(1,),
    )(dens, belief, bias)
    (post,) = call(
        functools.partial(last_kernel, rows),
        [((K, LANES, columns), jnp.bfloat16)],
        [
            pltpu.VMEM((K, LANES, columns), jnp.bfloat16),
            pltpu.SemaphoreType.DMA((slabs // 2,)),
        ],
        far_out=(0,),
    )(inner, own, up, down, side, edge, place)
    shape = (slabs, rows, columns)
    return post.reshape((K,) + shape), bias.reshape((M,) + shape), centers


def local(image, brain_mask, labels):
    _, slabs, rows, columns = image.shape
    peers = lax.axis_size("slab") * lax.axis_size("row")
    fits = slabs * rows == LANES and columns == LANES and slabs % SUB == 0 and rows % SUB == 0
    fits = fits and lax.axis_size("row") == 2 and lax.axis_size("col") == 2
    fits = fits and columns % (SUB * peers) == 0
    return (pencils if fits else general)(image, brain_mask, labels)


def solution(mesh):
    placed = (
        P(None, ("grp", "slab"), "row", "col"),
        P(("grp", "slab"), "row", "col"),
        P(("grp", "slab"), "row", "col"),
    )
    return jax.shard_map(
        local,
        mesh=mesh,
        in_specs=placed,
        out_specs=(
            P(None, ("grp", "slab"), "row", "col"),
            P(None, ("grp", "slab"), "row", "col"),
            P("grp", None),
        ),
        check_vma=False,
    )
```

```python
import functools
import math
import typing

import jax
import jax.numpy as jnp
import numpy as np
from jax import lax
from jax.experimental import pallas as pl
from jax.experimental.pallas import tpu as pltpu
from jax.sharding import PartitionSpec as P

M = 3
K = 8
EM_ITERS = 2
MF_PASSES = 2


highest = lax.Precision.HIGHEST
coupling = 1.0
breadth = 8.0


def extended(cells, sides, width):
    for axis, dim in sides:
        count = lax.axis_size(axis)
        ends = count - 1
        head = lax.slice_in_dim(cells, 0, width, axis=dim)
        tail = lax.slice_in_dim(cells, cells.shape[dim] - width, cells.shape[dim], axis=dim)
        cells = jnp.concatenate(
            [
                lax.ppermute(tail, axis, [(i, (i + 1) % count) for i in range(ends)]),
                cells,
                lax.ppermute(head, axis, [((i + 1) % count, i) for i in range(ends)]),
            ],
            axis=dim,
        )
    return cells


def circulant(length):
    index = jnp.arange(length, dtype=jnp.int32)
    folded = jnp.minimum(index, length - index).astype(jnp.float32) / length
    response = jnp.exp(-2.0 * math.pi**2 * (length / breadth) ** 2 * folded * folded)
    product = index[:, None] * index[None, :] % length
    angles = 2.0 * math.pi / length * product.astype(jnp.float32)
    cosine = jnp.cos(angles)
    sine = jnp.sin(angles)
    even_part = jnp.dot(cosine * response[None, :], cosine.T, precision=highest)
    odd_part = jnp.dot(sine * response[None, :], sine.T, precision=highest)
    return (even_part + odd_part) / length


def neighbour_sum(belief):
    padded = extended(belief, (("slab", 1), ("row", 2), ("col", 3)), 1)
    total = padded[:, 2:, 1:-1, 1:-1] + padded[:, :-2, 1:-1, 1:-1]
    total = total + padded[:, 1:-1, 2:, 1:-1] + padded[:, 1:-1, :-2, 1:-1]
    total = total + padded[:, 1:-1, 1:-1, 2:] + padded[:, 1:-1, 1:-1, :-2]
    return total


def class_moments(belief, corrected):
    flat = belief.reshape(K, -1)
    values = corrected.reshape(M, -1)
    count, first, squares = lax.psum(
        (
            jnp.sum(flat, axis=1),
            jnp.dot(flat, values.T, precision=highest),
            jnp.dot(flat, (values * values).T, precision=highest),
        ),
        ("slab", "row", "col"),
    )
    means = first / (count + 1.0)[:, None]
    spread = squares - 2.0 * means * first + means * means * count[:, None]
    variance = (spread + 1.0) / (count + 1.0)[:, None]
    return (count, means, variance)


def log_density(corrected, means, variance, prior):
    offset = corrected[None] - means[:, :, None, None, None]
    terms = (
        offset * offset / variance[:, :, None, None, None]
        + jnp.log(variance)[:, :, None, None, None]
    )
    return jnp.log(prior)[:, None, None, None] - 0.5 * jnp.sum(terms, axis=1)


def smoothed(residual, column_local, row_table, slab_table):
    across = jnp.einsum(
        "msrc,cd->msrd",
        lax.all_gather(residual, "col", axis=3, tiled=True),
        column_local,
        precision=highest,
    )
    mixed = jnp.einsum(
        "msrc,rq->msqc",
        lax.all_to_all(across, "row", split_axis=1, concat_axis=2, tiled=True),
        row_table,
        precision=highest,
    )
    across = lax.all_to_all(mixed, "row", split_axis=2, concat_axis=1, tiled=True)
    mixed = jnp.einsum(
        "msrc,sq->mqrc",
        lax.all_to_all(across, "slab", split_axis=2, concat_axis=1, tiled=True),
        slab_table,
        precision=highest,
    )
    return lax.all_to_all(mixed, "slab", split_axis=1, concat_axis=2, tiled=True)


def general(image, brain_mask, labels):
    channels, slabs, rows, columns = image.shape
    inside = brain_mask.astype(jnp.float32)
    kinds = jnp.arange(K, dtype=jnp.int32)
    belief = (labels[None] == kinds[:, None, None, None]).astype(jnp.float32) * inside[None]
    column_table = circulant(columns * lax.axis_size("col"))
    column_local = lax.dynamic_slice_in_dim(
        column_table, lax.axis_index("col") * columns, columns, 1
    )
    row_table = circulant(rows * lax.axis_size("row"))
    slab_table = circulant(slabs * lax.axis_size("slab"))
    bias_field = jnp.zeros_like(image)
    means = jnp.zeros((K, channels), jnp.float32)
    for iteration in range(EM_ITERS):
        corrected = image - bias_field
        count, means, variance = class_moments(belief, corrected)
        prior = (count + 1.0) / (jnp.sum(count) + K)
        total = jnp.sum(belief, axis=0)
        removed = jnp.dot(means.T, belief.reshape(K, -1), precision=highest).reshape(image.shape)
        residual = image * total[None] - removed
        bias_field = smoothed(residual, column_local, row_table, slab_table)
        corrected = image - bias_field
        density = log_density(corrected, means, variance, prior)
        for sweep_index in range(MF_PASSES):
            belief = (
                jax.nn.softmax(density + coupling * neighbour_sum(belief), axis=0) * inside[None]
            )
    return (belief.astype(jnp.bfloat16), bias_field, means)


LANES = 128
SUB = 8
EDGE = 4
MARGIN = 8
FIELD = 4
STATS = 1 + 2 * M
VMEM_BYTES = 16 * 2**20


def impulse(length):
    index = np.arange(length)
    folded = np.minimum(index, length - index) / length
    response = np.exp(-2.0 * np.pi**2 * (length / breadth) ** 2 * folded * folded)
    angles = 2.0 * np.pi / length * (index[:, None] * index[None, :] % length)
    return np.cos(angles) @ response / length


def dense(length):
    index = np.arange(length)
    return impulse(length)[(index[:, None] - index[None, :]) % length]


def halves_of(x):
    high = x.astype(jnp.bfloat16)
    return high, (x - high.astype(jnp.float32)).astype(jnp.bfloat16)


def table_of(x):
    high = x.astype(jnp.bfloat16)
    low = (x - high.astype(np.float64)).astype(jnp.bfloat16)
    return np.stack([high, low])


def dot(left, right, dims=((1,), (0,))):
    left, right = (x if isinstance(x, tuple) else halves_of(x) for x in (left, right))

    def one(a, b):
        return lax.dot_general(a, b, (dims, ((), ())), preferred_element_type=jnp.float32)

    return one(left[0], right[0]) + (one(left[1], right[0]) + one(left[0], right[1]))


def wide(row, shape=(SUB, LANES)):
    return jnp.broadcast_to(row, shape)


def stat_row(sums):
    sub = lax.broadcasted_iota(jnp.int32, (SUB, LANES), 0)
    lane = lax.broadcasted_iota(jnp.int32, (SUB, LANES), 1)
    tile = jnp.zeros((SUB, LANES), jnp.float32)
    for q in range(STATS):
        rows = jnp.zeros((SUB, LANES), jnp.float32)
        for k in range(K):
            line = jnp.sum(sums[k][q], axis=0, keepdims=True)
            rows = jnp.where(sub == k, line, rows)
        tile = jnp.where(lane == q * K + sub, jnp.sum(rows, axis=1, keepdims=True), tile)
    return jnp.sum(tile, axis=0, keepdims=True)


def stat_columns(row, number):
    sub = lax.broadcasted_iota(jnp.int32, (SUB, LANES), 0)
    lane = lax.broadcasted_iota(jnp.int32, (SUB, LANES), 1)
    return [
        jnp.sum(jnp.where(lane == q * K + sub, row, 0.0), axis=1, keepdims=True)
        for q in range(number)
    ]


def fold(x):
    return jnp.sum(x.reshape(x.shape[0] // SUB, SUB, LANES), axis=0)


def class_stats(row):
    count, *rest = stat_columns(row, STATS)
    means, halves = [], []
    shift = jnp.zeros_like(count)
    for m in range(M):
        first, squares = rest[m], rest[M + m]
        mean = first / (count + 1.0)
        spread = squares - 2.0 * mean * first + mean * mean * count
        variance = (spread + 1.0) / (count + 1.0)
        means.append(wide(mean))
        halves.append(wide(0.5 / variance))
        shift = shift - 0.5 * jnp.log(variance)
    prior = (count + 1.0) / (jnp.sum(count, axis=0, keepdims=True) + K)
    return means, halves, wide(jnp.log(prior) + shift)


def mean_rows(row):
    count, *rest = stat_columns(row, 1 + M)
    return [wide(x / (count + 1.0)) for x in rest]


def log_terms(corrected, means, halves, shift):
    out = []
    for k in range(K):
        total = wide(shift[k : k + 1, :], corrected[0].shape)
        for m in range(M):
            offset = corrected[m] - means[m][k : k + 1, :]
            total = total - offset * offset * halves[m][k : k + 1, :]
        out.append(total)
    return out


def soft(logits, inside):
    top = functools.reduce(jnp.maximum, logits)
    exps = [jnp.exp(x - top) for x in logits]
    scale = inside / functools.reduce(jnp.add, exps)
    return [x * scale for x in exps]


def peer_sum(ref, line):
    row = ref[0, line : line + 1, :]
    for j in range(1, ref.shape[0]):
        row = row + ref[j, line : line + 1, :]
    return row


def class_sums(code, image):
    sums = []
    for k in range(K):
        flag = (code == float(k)).astype(jnp.float32)
        line = [fold(flag)]
        weighted = [flag * image[m] for m in range(M)]
        line += [fold(x) for x in weighted]
        line += [fold(x * image[m]) for m, x in enumerate(weighted)]
        sums.append(line)
    return sums


def own_kernel(own, turned, stat):
    stat[...] = wide(stat_row(class_sums(own[M], own)))
    for f in range(M + 1):
        turned[f] = own[f].T


def prepare_kernel(
    pack, turned, stat, image_o, mask_o, labels_o, place, send, rest, code_o, ext
):
    peers = send.shape[0]
    step = LANES // peers
    first = place[2] == 0
    code_o[...] = jnp.where(mask_o[...] > 0, labels_o[...], K).astype(jnp.float32)
    row = stat[0:1, :] + stat_row(class_sums(code_o[...], image_o))
    for f in range(M + 1):
        blank = jnp.full((SUB, LANES), float(K) if f == M else 0.0, jnp.float32)
        other = (image_o[f] if f < M else code_o[...]).T
        ext[f, 0:MARGIN, :] = jnp.where(first, blank, other[LANES - MARGIN :, :])
        ext[f, MARGIN : MARGIN + LANES, :] = turned[f]
        ext[f, MARGIN + LANES :, :] = jnp.where(first, other[:MARGIN, :], blank)
    for p in range(peers):
        at = MARGIN + step * p
        for m in range(M):
            send[p, pack.wide * m : pack.wide * (m + 1), :] = ext[m, at - 2 : at + step + 2, :]
        send[p, pack.code : pack.stat, :] = ext[M, at - 1 : at + step + 1, :]
        send[p, pack.stat : pack.stat + 1, :] = row
        rest[p, 0:2, :] = ext[M, at - 3 : at - 1, :]
        rest[p, 2:4, :] = ext[M, at + step + 1 : at + step + 3, :]


def column_kernel(pack, own, image_o, code_o, got, rest, table, send, flat, out):
    peers = send.shape[0]
    step = LANES // peers
    means = mean_rows(peer_sum(got, pack.stat))
    for h, (ref, code) in enumerate(((own, own[M]), (image_o, code_o[...]))):
        flags = [code == float(k) for k in range(K)]
        for m in range(M):
            center = jnp.zeros_like(code)
            for k in range(K):
                center = jnp.where(flags[k], means[m][k : k + 1, :], center)
            flat[m * LANES : (m + 1) * LANES, h * LANES : (h + 1) * LANES] = jnp.where(
                code < float(K), ref[m] - center, 0.0
            )
    out[...] = dot((table[0], table[1]), flat[...], ((1,), (1,)))
    for p in range(peers):
        at = MARGIN + step * p
        send[p, pack.code : pack.code + 4, :] = rest[p, 0:4, :]
        for m in range(M):
            send[p, pack.wide * m : pack.wide * (m + 1), :] = out[
                at - 2 : at + step + 2, m * LANES : (m + 1) * LANES
            ]


def slab_row_filter(rows, slab_table, row_table, first, second, grid):
    ns, nr = grid
    mixed = dot(first[...], (slab_table[0], slab_table[1]))
    for sb in range(ns):
        for rb in range(nr):
            second[sb * rows : (sb + 1) * rows, rb * LANES : (rb + 1) * LANES] = mixed[
                rb * rows : (rb + 1) * rows, sb * LANES : (sb + 1) * LANES
            ]
    return dot(second[...], (row_table[0], row_table[1]))


def around(get, sb, rb, grid, rows, fill):
    ns, nr = grid
    lane = lax.broadcasted_iota(jnp.int32, (1, LANES), 1)
    place = lane % rows
    here = get(sb, rb)
    empty = jnp.full_like(here, fill)
    above = get(sb + 1, rb) if sb + 1 < ns else empty
    below = get(sb - 1, rb) if sb > 0 else empty
    out = [
        pltpu.roll(jnp.where(lane >= rows, here, above), LANES - rows, 1),
        pltpu.roll(jnp.where(lane < LANES - rows, here, below), rows, 1),
    ]
    right = pltpu.roll(get(sb, rb + 1), rows - 1, 1) if rb + 1 < nr else empty
    left = pltpu.roll(get(sb, rb - 1), LANES - rows + 1, 1) if rb > 0 else empty
    out.append(jnp.where(place < rows - 1, pltpu.roll(here, LANES - 1, 1), right))
    out.append(jnp.where(place > 0, pltpu.roll(here, 1, 1), left))
    return out


def pencil_kernel(
    pack,
    grid,
    rows,
    got,
    raw,
    slab_table,
    row_table,
    send,
    keep,
    first,
    second,
    bias,
    codes,
    marks,
    shaded,
    dens,
    one,
    two,
):
    ns, nr = grid
    peers = ns * nr
    core = pack.core
    window = core + 2 * EDGE
    means, halves, shift = class_stats(peer_sum(raw, pack.stat))
    first[...] = jnp.zeros_like(first)
    for sb in range(ns):
        for rb in range(nr):
            for m in range(M):
                base = (rb * M + m) * window + EDGE - 2
                first[base : base + pack.wide, sb * LANES : (sb + 1) * LANES] = got[
                    rb * ns + sb, m * pack.wide : (m + 1) * pack.wide, :
                ]
    bias[...] = slab_row_filter(M * window, slab_table, row_table, first, second, grid)
    blank = jnp.full((window, LANES), float(K), jnp.float32)
    for sb in range(ns):
        for rb in range(nr):
            j = rb * ns + sb
            codes[j] = blank
            codes[j, EDGE - 3 : EDGE - 1, :] = got[j, pack.code : pack.code + 2, :]
            codes[j, EDGE - 1 : EDGE + core + 1, :] = raw[j, pack.code : pack.stat, :]
            codes[j, EDGE + core + 1 : EDGE + core + 3, :] = got[j, pack.code + 2 : pack.code + 4, :]
            for m in range(M):
                base = (sb * M + m) * window
                shaded[j, m] = -bias[base : base + window, rb * LANES : (rb + 1) * LANES]
                shaded[j, m, EDGE - 2 : EDGE - 2 + pack.wide, :] += raw[
                    j, m * pack.wide : (m + 1) * pack.wide, :
                ]

    def bits(x):
        whole = x.astype(jnp.int32)
        return jnp.where(whole < K, lax.shift_left(jnp.ones_like(whole), whole * FIELD), 0)

    for j in range(peers):
        marks[j] = bits(codes[j])

    for sb in range(ns):
        for rb in range(nr):
            j = rb * ns + sb
            logits = log_terms([shaded[j, m] for m in range(M)], means, halves, shift)
            code = codes[j]
            here = marks[j]
            near = around(lambda a, b: marks[b * ns + a], sb, rb, grid, rows, 0)
            near = near + [pltpu.roll(here, 1, 0), pltpu.roll(here, window - 1, 0)]
            near = functools.reduce(jnp.add, near)
            for k in range(K):
                dens[k, j] = logits[k]
                number = lax.shift_right_logical(near, jnp.full_like(near, k * FIELD))
                logits[k] = logits[k] + (number & (2**FIELD - 1)).astype(jnp.float32)
            inside = (code < float(K)).astype(jnp.float32)
            for k, value in enumerate(soft(logits, inside)):
                one[k, j] = value
    for sb in range(ns):
        for rb in range(nr):
            j = rb * ns + sb
            logits = []
            for k in range(K):
                here = one[k, j]
                near = around(lambda a, b: one[k, b * ns + a], sb, rb, grid, rows, 0.0)
                near = near + [pltpu.roll(here, 1, 0), pltpu.roll(here, window - 1, 0)]
                logits.append(dens[k, j] + functools.reduce(jnp.add, near))
            inside = (codes[j] < float(K)).astype(jnp.float32)
            for k, value in enumerate(soft(logits, inside)):
                two[k, j] = value
    for sb in range(ns):
        for rb in range(nr):
            j = rb * ns + sb
            totals = []
            for k in range(K):
                near = around(
                    lambda a, b: two[k, b * ns + a, EDGE : EDGE + core, :], sb, rb, grid, rows, 0.0
                )
                near = near + [
                    two[k, j, EDGE - 1 : EDGE - 1 + core, :],
                    two[k, j, EDGE + 1 : EDGE + 1 + core, :],
                ]
                totals.append(functools.reduce(jnp.add, near))
            for k in range(K - 1):
                send[j, k * core : (k + 1) * core, :] = totals[k] - totals[K - 1]
    sums = []
    for k in range(K):
        line = [jnp.zeros((SUB, LANES), jnp.float32) for _ in range(STATS)]
        for j in range(peers):
            here = two[k, j, EDGE : EDGE + core, :]
            keep[k, j] = here
            line[0] = line[0] + fold(here)
            for m in range(M):
                field = shaded[j, m, EDGE : EDGE + core, :]
                value = here * field
                line[1 + m] = line[1 + m] + fold(value)
                line[1 + M + m] = line[1 + M + m] + fold(value * field)
        sums.append([jnp.sum(x, axis=0, keepdims=True) for x in line])
    row = stat_row(sums)
    for p in range(peers):
        send[p, (K - 1) * core : (K - 1) * core + 1, :] = row


def early_residual_kernel(pack, grid, keep, raw, slab_table, row_table, out, first, second):
    ns, nr = grid
    core = pack.core
    fields = M + K
    for sb in range(ns):
        for rb in range(nr):
            j = rb * ns + sb
            shares = [keep[k, j] for k in range(K)]
            total = functools.reduce(jnp.add, shares)
            span = slice(sb * LANES, (sb + 1) * LANES)
            for f in range(fields):
                line = (rb * fields + f) * core
                if f < M:
                    base = f * pack.wide + 2
                    value = raw[j, base : base + core, :] * total
                else:
                    value = shares[f - M]
                first[line : line + core, span] = value
    out[...] = slab_row_filter(fields * core, slab_table, row_table, first, second, grid)


def residual_kernel(pack, grid, stat_a, stat_b, early, send, stat):
    ns, nr = grid
    core = pack.core
    row = stat_a[...] + stat_b[...]
    stat[...] = wide(row)
    means = mean_rows(row)
    for sb in range(ns):
        for rb in range(nr):
            base = sb * (M + K) * core
            span = slice(rb * LANES, (rb + 1) * LANES)
            parts = [early[base + f * core : base + (f + 1) * core, span] for f in range(M + K)]
            for m in range(M):
                total = parts[m]
                for k in range(K):
                    total = total - parts[M + k] * means[m][k : k + 1, :]
                send[rb * ns + sb, m * core : (m + 1) * core, :] = total


def columns_of(ref, m, core):
    return ref[:, m * core : (m + 1) * core, :].reshape(LANES, LANES).T


def half_kernel(got, near, table, field, around):
    core = got.shape[1] // M
    for m in range(M):
        field[m] = dot(columns_of(got, m, core), (table[0, :LANES, :], table[1, :LANES, :]))
    for k in range(K - 1):
        around[k] = columns_of(near, k, core)


def third_kernel(
    rows,
    field,
    got,
    near,
    own,
    stat,
    table,
    place,
    bias,
    centers,
    dens,
    belief,
    up,
    down,
    side,
    edge,
):
    core = got.shape[1] // M
    slabs = LANES // rows
    means, halves, shift = class_stats(stat[0:1, :])
    for m in range(M):
        centers[:, m : m + 1] = means[m][:, :1]
        bias[m] = field[m] + dot(
            columns_of(got, m, core), (table[0, LANES:, :], table[1, LANES:, :])
        )
    lane = lax.broadcasted_iota(jnp.int32, (1, LANES), 1)
    even = place[0, 0:1, :] == 0
    shiftback = jnp.where(place[2, 0:1, :] == 0, 1, 0)
    marks = [(lane + shiftback) % LANES == k for k in range(K)]
    for s in range(slabs):
        low, high = s * rows, (s + 1) * rows
        corrected = [own[m, low:high, :] - bias[m, low:high, :] for m in range(M)]
        logits = log_terms(corrected, means, halves, shift)
        for k in range(K):
            dens[k, low:high, :] = logits[k]
            if k < K - 1:
                logits[k] = logits[k] + near[k, low:high, :]
        inside = (own[M, low:high, :] < float(K)).astype(jnp.float32)
        column = jnp.zeros((rows, LANES), jnp.float32)
        for k, value in enumerate(soft(logits, inside)):
            belief[k, low:high, :] = value
            column = jnp.where(marks[k], pltpu.roll(value, k, 1), column)
        edge[low:high, :] = column
    for k in range(K):
        first = belief[k, :rows, :]
        final = belief[k, LANES - rows :, :]
        up[k] = jnp.where(even, final, first)
        down[k] = jnp.where(even, first, final)
    lead = place[1, 0:1, :] == 0
    for k in range(K):
        head = belief[k, pl.ds(0, slabs, rows), :]
        tail = belief[k, pl.ds(rows - 1, slabs, rows), :]
        side[k] = jnp.where(lead, tail, head)


def inner_kernel(rows, dens, belief, bias, logits, bias_h, sems):
    copy = pltpu.make_async_copy(bias, bias_h, sems.at[0])
    copy.start()
    lane = lax.broadcasted_iota(jnp.int32, (1, LANES), 1)
    line = lax.broadcasted_iota(jnp.int32, (rows, 1), 0)
    for k in range(K):
        for low in range(0, LANES, rows):
            here = belief[k, low : low + rows, :]
            total = dens[k, low : low + rows, :]
            if low > 0:
                total = total + belief[k, low - rows : low, :]
            if low + rows < LANES:
                total = total + belief[k, low + rows : low + 2 * rows, :]
            total = total + jnp.where(line > 0, pltpu.roll(here, 1, 0), 0.0)
            total = total + jnp.where(line < rows - 1, pltpu.roll(here, rows - 1, 0), 0.0)
            total = total + jnp.where(lane > 0, pltpu.roll(here, 1, 1), 0.0)
            total = total + jnp.where(lane < LANES - 1, pltpu.roll(here, LANES - 1, 1), 0.0)
            logits[k, low : low + rows, :] = total
    copy.wait()


def last_kernel(rows, inner, own, up, down, side, edge, place, post_h, post, sems):
    slabs = LANES // rows
    lane = lax.broadcasted_iota(jnp.int32, (1, LANES), 1)
    line = lax.broadcasted_iota(jnp.int32, (rows, 1), 0)
    even = place[0, 0:1, :] == 0
    left = place[2, 0:1, :] == 0
    spot = lane == jnp.where(left, LANES - 1, 0)
    face = line == jnp.where(place[1, 0:1, :] == 0, rows - 1, 0)
    copies = []
    for s in range(slabs):
        low, high = s * rows, (s + 1) * rows
        column = edge[low:high, :]
        column = jnp.where(left, column, pltpu.roll(column, 2, 1))
        logits = []
        for k in range(K):
            total = inner[k, low:high, :]
            if s == 0:
                total = total + jnp.where(even, down[k], up[k])
            if s == slabs - 1:
                total = total + jnp.where(even, up[k], down[k])
            total = total + jnp.where(face, side[k, s : s + 1, :], 0.0)
            total = total + jnp.where(spot, pltpu.roll(column, LANES - 1 - k, 1), 0.0)
            logits.append(total)
        inside = (own[M, low:high, :] < float(K)).astype(jnp.float32)
        for k, value in enumerate(soft(logits, inside)):
            post[k, low:high, :] = value.astype(jnp.bfloat16)
        span = pl.ds(low, rows)
        copies.append(
            pltpu.make_async_copy(post.at[:, span, :], post_h.at[:, span, :], sems.at[s])
        )
        copies[-1].start()
    for copy in copies:
        copy.wait()


class Pack(typing.NamedTuple):
    core: int
    wide: int
    code: int
    stat: int


def padded(rows):
    return -(-rows // SUB) * SUB


def call(kernel, outs, scratch=(), micros=1, far_out=()):
    vmem = pl.BlockSpec(memory_space=pltpu.VMEM)
    far = pl.BlockSpec(memory_space=pltpu.HBM)
    shapes = [jax.ShapeDtypeStruct(shape, kind) for shape, kind in outs]

    def run(*args):
        return pl.pallas_call(
            kernel,
            out_shape=shapes,
            in_specs=[vmem] * len(args),
            out_specs=[far if i in far_out else vmem for i in range(len(shapes))],
            scratch_shapes=[
                pltpu.VMEM(x, jnp.float32) if isinstance(x, tuple) else x for x in scratch
            ],
            compiler_params=pltpu.CompilerParams(vmem_limit_bytes=VMEM_BYTES),
            cost_estimate=pl.CostEstimate(
                flops=micros * 10_000_000, bytes_accessed=2**20, transcendentals=0
            ),
            name=(kernel.func if isinstance(kernel, functools.partial) else kernel).__name__,
        )(*args)

    return run


def pencils(image, brain_mask, labels):
    _, slabs, rows, columns = image.shape
    ns, nr, nc = (lax.axis_size(a) for a in ("slab", "row", "col"))
    grid = (ns, nr)
    peers = ns * nr
    core = columns // peers
    window = core + 2 * EDGE
    wide_rows = core + 4
    pack = Pack(core, wide_rows, M * wide_rows, M * wide_rows + core + 2)
    f32 = jnp.float32
    place = jnp.stack([lax.axis_index("slab") % 2, lax.axis_index("row"), lax.axis_index("col")])
    place = jnp.broadcast_to(place.astype(jnp.int32)[:, None, None], (3, SUB, LANES))
    swap = [(0, 1), (1, 0)]

    taps = impulse(columns * nc)
    reach = np.arange(-MARGIN, columns + MARGIN)
    source = np.concatenate([np.arange(columns), np.arange(columns) + columns])
    spread = taps[(reach[:, None] - source[None, :]) % (columns * nc)]
    gather = table_of(spread[MARGIN : MARGIN + columns].T)
    spread = table_of(spread)
    slab_table = table_of(np.kron(dense(slabs * ns), np.eye(rows)))
    row_table = np.einsum(
        "arbq,st->asrbtq", dense(rows * nr).reshape(nr, rows, nr, rows), np.eye(slabs)
    )
    row_table = table_of(row_table.reshape(nr * LANES, nr * LANES))

    code = jnp.where(brain_mask > 0, labels, K).astype(f32)
    own = jnp.concatenate([image, code[None]]).reshape(M + 1, LANES, columns)
    image_o = lax.ppermute(image.reshape(M, LANES, columns), "col", swap)
    mask_o = lax.ppermute(brain_mask.reshape(LANES, columns), "col", swap)
    labels_o = lax.ppermute(labels.reshape(LANES, columns), "col", swap)

    def trade(x):
        return lax.all_to_all(x, ("row", "slab"), split_axis=0, concat_axis=0, tiled=True)

    turned, stat = call(
        own_kernel, [((M + 1, columns, LANES), f32), ((SUB, LANES), f32)]
    )(own)
    sent, rest, code_o = call(
        functools.partial(prepare_kernel, pack),
        [
            ((peers, padded(pack.stat + 1), LANES), f32),
            ((peers, SUB, LANES), f32),
            ((LANES, columns), f32),
        ],
        [(M + 1, columns + 2 * MARGIN, LANES)],
    )(turned, stat, image_o, mask_o, labels_o, place)
    raw = trade(sent)
    (sent,) = call(
        functools.partial(column_kernel, pack),
        [((peers, padded(pack.code + 4), LANES), f32)],
        [(M * LANES, 2 * columns), (columns + 2 * MARGIN, M * LANES)],
    )(own, image_o, code_o, raw, rest, spread)
    got = trade(sent)
    sent, keep = call(
        functools.partial(pencil_kernel, pack, grid, rows),
        [
            ((peers, padded((K - 1) * core + 1), LANES), f32),
            ((K, peers, core, LANES), f32),
        ],
        [
            (nr * M * window, ns * LANES),
            (ns * M * window, nr * LANES),
            (ns * M * window, nr * LANES),
            (peers, window, LANES),
            pltpu.VMEM((peers, window, LANES), jnp.int32),
            (peers, M, window, LANES),
            (K, peers, window, LANES),
            (K, peers, window, LANES),
            (K, peers, window, LANES),
        ],
        micros=4,
    )(got, raw, slab_table, row_table)
    near = trade(sent)
    (early,) = call(
        functools.partial(early_residual_kernel, pack, grid),
        [((ns * (M + K) * core, nr * LANES), f32)],
        [(nr * (M + K) * core, ns * LANES), (ns * (M + K) * core, nr * LANES)],
        micros=8,
    )(keep, raw, slab_table, row_table)
    stat_a = jnp.sum(near[:, (K - 1) * core : (K - 1) * core + 1, :], axis=0)
    stat_b = lax.ppermute(stat_a, "col", swap)
    sent, stat = call(
        functools.partial(residual_kernel, pack, grid),
        [((peers, M * core, LANES), f32), ((SUB, LANES), f32)],
    )(stat_a, stat_b, early)
    got = trade(sent)
    yours = lax.ppermute(got, "col", swap)
    field, near = call(
        half_kernel, [((M, LANES, columns), f32), ((K - 1, LANES, columns), f32)]
    )(got, near, gather)
    bias, centers, dens, belief, up, down, side, edge = call(
        functools.partial(third_kernel, rows),
        [
            ((M, LANES, columns), f32),
            ((K, M), f32),
            ((K, LANES, columns), f32),
            ((K, LANES, columns), f32),
            ((K, rows, columns), f32),
            ((K, rows, columns), f32),
            ((K, slabs, columns), f32),
            ((LANES, LANES), f32),
        ],
        micros=2,
    )(field, yours, near, own, stat, gather, place)
    pairs = [(i, i + 1) for i in range(0, ns - 1, 2)]
    between = [(i, i + 1) for i in range(1, ns - 1, 2)]
    up = lax.ppermute(up, "slab", pairs + [(b, a) for a, b in pairs])
    down = lax.ppermute(down, "slab", between + [(b, a) for a, b in between])
    side = lax.ppermute(side, "row", swap)
    edge = lax.ppermute(edge, "col", swap)
    inner, bias = call(
        functools.partial(inner_kernel, rows),
        [((K, LANES, columns), f32), ((M, LANES, columns), f32)],
        [pltpu.SemaphoreType.DMA((1,))],
        far_out=(1,),
    )(dens, belief, bias)
    (post,) = call(
        functools.partial(last_kernel, rows),
        [((K, LANES, columns), jnp.bfloat16)],
        [
            pltpu.VMEM((K, LANES, columns), jnp.bfloat16),
            pltpu.SemaphoreType.DMA((slabs,)),
        ],
        far_out=(0,),
    )(inner, own, up, down, side, edge, place)
    shape = (slabs, rows, columns)
    return post.reshape((K,) + shape), bias.reshape((M,) + shape), centers


def local(image, brain_mask, labels):
    _, slabs, rows, columns = image.shape
    peers = lax.axis_size("slab") * lax.axis_size("row")
    fits = slabs * rows == LANES and columns == LANES and slabs % SUB == 0 and rows % SUB == 0
    fits = fits and lax.axis_size("row") == 2 and lax.axis_size("col") == 2
    fits = fits and columns % (SUB * peers) == 0
    return (pencils if fits else general)(image, brain_mask, labels)


def solution(mesh):
    placed = (
        P(None, ("grp", "slab"), "row", "col"),
        P(("grp", "slab"), "row", "col"),
        P(("grp", "slab"), "row", "col"),
    )
    return jax.shard_map(
        local,
        mesh=mesh,
        in_specs=placed,
        out_specs=(
            P(None, ("grp", "slab"), "row", "col"),
            P(None, ("grp", "slab"), "row", "col"),
            P("grp", None),
        ),
        check_vma=False,
    )
```

```python
import functools
import math
import typing

import jax
import jax.numpy as jnp
import numpy as np
from jax import lax
from jax.experimental import pallas as pl
from jax.experimental.pallas import tpu as pltpu
from jax.sharding import PartitionSpec as P

M = 3
K = 8
EM_ITERS = 2
MF_PASSES = 2


highest = lax.Precision.HIGHEST
coupling = 1.0
breadth = 8.0


def extended(cells, sides, width):
    for axis, dim in sides:
        count = lax.axis_size(axis)
        ends = count - 1
        head = lax.slice_in_dim(cells, 0, width, axis=dim)
        tail = lax.slice_in_dim(cells, cells.shape[dim] - width, cells.shape[dim], axis=dim)
        cells = jnp.concatenate(
            [
                lax.ppermute(tail, axis, [(i, (i + 1) % count) for i in range(ends)]),
                cells,
                lax.ppermute(head, axis, [((i + 1) % count, i) for i in range(ends)]),
            ],
            axis=dim,
        )
    return cells


def circulant(length):
    index = jnp.arange(length, dtype=jnp.int32)
    folded = jnp.minimum(index, length - index).astype(jnp.float32) / length
    response = jnp.exp(-2.0 * math.pi**2 * (length / breadth) ** 2 * folded * folded)
    product = index[:, None] * index[None, :] % length
    angles = 2.0 * math.pi / length * product.astype(jnp.float32)
    cosine = jnp.cos(angles)
    sine = jnp.sin(angles)
    even_part = jnp.dot(cosine * response[None, :], cosine.T, precision=highest)
    odd_part = jnp.dot(sine * response[None, :], sine.T, precision=highest)
    return (even_part + odd_part) / length


def neighbour_sum(belief):
    padded = extended(belief, (("slab", 1), ("row", 2), ("col", 3)), 1)
    total = padded[:, 2:, 1:-1, 1:-1] + padded[:, :-2, 1:-1, 1:-1]
    total = total + padded[:, 1:-1, 2:, 1:-1] + padded[:, 1:-1, :-2, 1:-1]
    total = total + padded[:, 1:-1, 1:-1, 2:] + padded[:, 1:-1, 1:-1, :-2]
    return total


def class_moments(belief, corrected):
    flat = belief.reshape(K, -1)
    values = corrected.reshape(M, -1)
    count, first, squares = lax.psum(
        (
            jnp.sum(flat, axis=1),
            jnp.dot(flat, values.T, precision=highest),
            jnp.dot(flat, (values * values).T, precision=highest),
        ),
        ("slab", "row", "col"),
    )
    means = first / (count + 1.0)[:, None]
    spread = squares - 2.0 * means * first + means * means * count[:, None]
    variance = (spread + 1.0) / (count + 1.0)[:, None]
    return (count, means, variance)


def log_density(corrected, means, variance, prior):
    offset = corrected[None] - means[:, :, None, None, None]
    terms = (
        offset * offset / variance[:, :, None, None, None]
        + jnp.log(variance)[:, :, None, None, None]
    )
    return jnp.log(prior)[:, None, None, None] - 0.5 * jnp.sum(terms, axis=1)


def smoothed(residual, column_local, row_table, slab_table):
    across = jnp.einsum(
        "msrc,cd->msrd",
        lax.all_gather(residual, "col", axis=3, tiled=True),
        column_local,
        precision=highest,
    )
    mixed = jnp.einsum(
        "msrc,rq->msqc",
        lax.all_to_all(across, "row", split_axis=1, concat_axis=2, tiled=True),
        row_table,
        precision=highest,
    )
    across = lax.all_to_all(mixed, "row", split_axis=2, concat_axis=1, tiled=True)
    mixed = jnp.einsum(
        "msrc,sq->mqrc",
        lax.all_to_all(across, "slab", split_axis=2, concat_axis=1, tiled=True),
        slab_table,
        precision=highest,
    )
    return lax.all_to_all(mixed, "slab", split_axis=1, concat_axis=2, tiled=True)


def general(image, brain_mask, labels):
    channels, slabs, rows, columns = image.shape
    inside = brain_mask.astype(jnp.float32)
    kinds = jnp.arange(K, dtype=jnp.int32)
    belief = (labels[None] == kinds[:, None, None, None]).astype(jnp.float32) * inside[None]
    column_table = circulant(columns * lax.axis_size("col"))
    column_local = lax.dynamic_slice_in_dim(
        column_table, lax.axis_index("col") * columns, columns, 1
    )
    row_table = circulant(rows * lax.axis_size("row"))
    slab_table = circulant(slabs * lax.axis_size("slab"))
    bias_field = jnp.zeros_like(image)
    means = jnp.zeros((K, channels), jnp.float32)
    for iteration in range(EM_ITERS):
        corrected = image - bias_field
        count, means, variance = class_moments(belief, corrected)
        prior = (count + 1.0) / (jnp.sum(count) + K)
        total = jnp.sum(belief, axis=0)
        removed = jnp.dot(means.T, belief.reshape(K, -1), precision=highest).reshape(image.shape)
        residual = image * total[None] - removed
        bias_field = smoothed(residual, column_local, row_table, slab_table)
        corrected = image - bias_field
        density = log_density(corrected, means, variance, prior)
        for sweep_index in range(MF_PASSES):
            belief = (
                jax.nn.softmax(density + coupling * neighbour_sum(belief), axis=0) * inside[None]
            )
    return (belief.astype(jnp.bfloat16), bias_field, means)


LANES = 128
SUB = 8
EDGE = 4
MARGIN = 8
FIELD = 4
STATS = 1 + 2 * M
VMEM_BYTES = 16 * 2**20


def impulse(length):
    index = np.arange(length)
    folded = np.minimum(index, length - index) / length
    response = np.exp(-2.0 * np.pi**2 * (length / breadth) ** 2 * folded * folded)
    angles = 2.0 * np.pi / length * (index[:, None] * index[None, :] % length)
    return np.cos(angles) @ response / length


def dense(length):
    index = np.arange(length)
    return impulse(length)[(index[:, None] - index[None, :]) % length]


def halves_of(x):
    high = x.astype(jnp.bfloat16)
    return high, (x - high.astype(jnp.float32)).astype(jnp.bfloat16)


def table_of(x):
    high = x.astype(jnp.bfloat16)
    low = (x - high.astype(np.float64)).astype(jnp.bfloat16)
    return np.stack([high, low])


def dot(left, right, dims=((1,), (0,))):
    left, right = (x if isinstance(x, tuple) else halves_of(x) for x in (left, right))

    def one(a, b):
        return lax.dot_general(a, b, (dims, ((), ())), preferred_element_type=jnp.float32)

    return one(left[0], right[0]) + (one(left[1], right[0]) + one(left[0], right[1]))


def wide(row, shape=(SUB, LANES)):
    return jnp.broadcast_to(row, shape)


def stat_row(sums):
    sub = lax.broadcasted_iota(jnp.int32, (SUB, LANES), 0)
    lane = lax.broadcasted_iota(jnp.int32, (SUB, LANES), 1)
    tile = jnp.zeros((SUB, LANES), jnp.float32)
    for q in range(STATS):
        rows = jnp.zeros((SUB, LANES), jnp.float32)
        for k in range(K):
            line = jnp.sum(sums[k][q], axis=0, keepdims=True)
            rows = jnp.where(sub == k, line, rows)
        tile = jnp.where(lane == q * K + sub, jnp.sum(rows, axis=1, keepdims=True), tile)
    return jnp.sum(tile, axis=0, keepdims=True)


def stat_columns(row, number):
    sub = lax.broadcasted_iota(jnp.int32, (SUB, LANES), 0)
    lane = lax.broadcasted_iota(jnp.int32, (SUB, LANES), 1)
    return [
        jnp.sum(jnp.where(lane == q * K + sub, row, 0.0), axis=1, keepdims=True)
        for q in range(number)
    ]


def fold(x):
    return jnp.sum(x.reshape(x.shape[0] // SUB, SUB, LANES), axis=0)


def class_stats(row):
    count, *rest = stat_columns(row, STATS)
    means, halves = [], []
    shift = jnp.zeros_like(count)
    for m in range(M):
        first, squares = rest[m], rest[M + m]
        mean = first / (count + 1.0)
        spread = squares - 2.0 * mean * first + mean * mean * count
        variance = (spread + 1.0) / (count + 1.0)
        means.append(wide(mean))
        halves.append(wide(0.5 / variance))
        shift = shift - 0.5 * jnp.log(variance)
    prior = (count + 1.0) / (jnp.sum(count, axis=0, keepdims=True) + K)
    return means, halves, wide(jnp.log(prior) + shift)


def mean_rows(row):
    count, *rest = stat_columns(row, 1 + M)
    return [wide(x / (count + 1.0)) for x in rest]


def log_terms(corrected, means, halves, shift):
    out = []
    for k in range(K):
        total = wide(shift[k : k + 1, :], corrected[0].shape)
        for m in range(M):
            offset = corrected[m] - means[m][k : k + 1, :]
            total = total - offset * offset * halves[m][k : k + 1, :]
        out.append(total)
    return out


def soft(logits, inside):
    top = functools.reduce(jnp.maximum, logits)
    exps = [jnp.exp(x - top) for x in logits]
    scale = inside / functools.reduce(jnp.add, exps)
    return [x * scale for x in exps]


def peer_sum(ref, line):
    row = ref[0, line : line + 1, :]
    for j in range(1, ref.shape[0]):
        row = row + ref[j, line : line + 1, :]
    return row


def class_sums(code, image):
    sums = []
    for k in range(K):
        flag = (code == float(k)).astype(jnp.float32)
        line = [fold(flag)]
        weighted = [flag * image[m] for m in range(M)]
        line += [fold(x) for x in weighted]
        line += [fold(x * image[m]) for m, x in enumerate(weighted)]
        sums.append(line)
    return sums


def own_kernel(own, turned, stat):
    stat[...] = wide(stat_row(class_sums(own[M], own)))
    for f in range(M + 1):
        turned[f] = own[f].T


def prepare_kernel(
    pack, turned, stat, image_o, mask_o, labels_o, place, send, rest, code_o, ext
):
    peers = send.shape[0]
    step = LANES // peers
    first = place[2] == 0
    code_o[...] = jnp.where(mask_o[...] > 0, labels_o[...], K).astype(jnp.float32)
    row = stat[0:1, :] + stat_row(class_sums(code_o[...], image_o))
    for f in range(M + 1):
        blank = jnp.full((SUB, LANES), float(K) if f == M else 0.0, jnp.float32)
        other = (image_o[f] if f < M else code_o[...]).T
        ext[f, 0:MARGIN, :] = jnp.where(first, blank, other[LANES - MARGIN :, :])
        ext[f, MARGIN : MARGIN + LANES, :] = turned[f]
        ext[f, MARGIN + LANES :, :] = jnp.where(first, other[:MARGIN, :], blank)
    for p in range(peers):
        at = MARGIN + step * p
        for m in range(M):
            send[p, pack.wide * m : pack.wide * (m + 1), :] = ext[m, at - 2 : at + step + 2, :]
        send[p, pack.code : pack.stat, :] = ext[M, at - 1 : at + step + 1, :]
        send[p, pack.stat : pack.stat + 1, :] = row
        rest[p, 0:2, :] = ext[M, at - 3 : at - 1, :]
        rest[p, 2:4, :] = ext[M, at + step + 1 : at + step + 3, :]


def column_kernel(pack, own, image_o, code_o, got, rest, table, send, flat, out):
    peers = send.shape[0]
    step = LANES // peers
    means = mean_rows(peer_sum(got, pack.stat))
    for h, (ref, code) in enumerate(((own, own[M]), (image_o, code_o[...]))):
        flags = [code == float(k) for k in range(K)]
        for m in range(M):
            center = jnp.zeros_like(code)
            for k in range(K):
                center = jnp.where(flags[k], means[m][k : k + 1, :], center)
            flat[m * LANES : (m + 1) * LANES, h * LANES : (h + 1) * LANES] = jnp.where(
                code < float(K), ref[m] - center, 0.0
            )
    out[...] = dot((table[0], table[1]), flat[...], ((1,), (1,)))
    for p in range(peers):
        at = MARGIN + step * p
        send[p, pack.code : pack.code + 4, :] = rest[p, 0:4, :]
        for m in range(M):
            send[p, pack.wide * m : pack.wide * (m + 1), :] = out[
                at - 2 : at + step + 2, m * LANES : (m + 1) * LANES
            ]


def slab_row_filter(rows, slab_table, row_table, first, second, grid):
    ns, nr = grid
    mixed = dot(first[...], (slab_table[0], slab_table[1]))
    for sb in range(ns):
        for rb in range(nr):
            second[sb * rows : (sb + 1) * rows, rb * LANES : (rb + 1) * LANES] = mixed[
                rb * rows : (rb + 1) * rows, sb * LANES : (sb + 1) * LANES
            ]
    return dot(second[...], (row_table[0], row_table[1]))


def around(get, sb, rb, grid, rows, fill):
    ns, nr = grid
    lane = lax.broadcasted_iota(jnp.int32, (1, LANES), 1)
    place = lane % rows
    here = get(sb, rb)
    empty = jnp.full_like(here, fill)
    above = get(sb + 1, rb) if sb + 1 < ns else empty
    below = get(sb - 1, rb) if sb > 0 else empty
    out = [
        pltpu.roll(jnp.where(lane >= rows, here, above), LANES - rows, 1),
        pltpu.roll(jnp.where(lane < LANES - rows, here, below), rows, 1),
    ]
    right = pltpu.roll(get(sb, rb + 1), rows - 1, 1) if rb + 1 < nr else empty
    left = pltpu.roll(get(sb, rb - 1), LANES - rows + 1, 1) if rb > 0 else empty
    out.append(jnp.where(place < rows - 1, pltpu.roll(here, LANES - 1, 1), right))
    out.append(jnp.where(place > 0, pltpu.roll(here, 1, 1), left))
    return out


def pencil_kernel(
    pack,
    grid,
    rows,
    got,
    raw,
    slab_table,
    row_table,
    send,
    keep,
    first,
    second,
    bias,
    codes,
    marks,
    shaded,
    dens,
    one,
    two,
):
    ns, nr = grid
    peers = ns * nr
    core = pack.core
    window = core + 2 * EDGE
    means, halves, shift = class_stats(peer_sum(raw, pack.stat))
    first[...] = jnp.zeros_like(first)
    for sb in range(ns):
        for rb in range(nr):
            for m in range(M):
                base = (rb * M + m) * window + EDGE - 2
                first[base : base + pack.wide, sb * LANES : (sb + 1) * LANES] = got[
                    rb * ns + sb, m * pack.wide : (m + 1) * pack.wide, :
                ]
    bias[...] = slab_row_filter(M * window, slab_table, row_table, first, second, grid)
    blank = jnp.full((window, LANES), float(K), jnp.float32)
    for sb in range(ns):
        for rb in range(nr):
            j = rb * ns + sb
            codes[j] = blank
            codes[j, EDGE - 3 : EDGE - 1, :] = got[j, pack.code : pack.code + 2, :]
            codes[j, EDGE - 1 : EDGE + core + 1, :] = raw[j, pack.code : pack.stat, :]
            codes[j, EDGE + core + 1 : EDGE + core + 3, :] = got[j, pack.code + 2 : pack.code + 4, :]
            for m in range(M):
                base = (sb * M + m) * window
                shaded[j, m] = -bias[base : base + window, rb * LANES : (rb + 1) * LANES]
                shaded[j, m, EDGE - 2 : EDGE - 2 + pack.wide, :] += raw[
                    j, m * pack.wide : (m + 1) * pack.wide, :
                ]

    def bits(x):
        whole = x.astype(jnp.int32)
        return jnp.where(whole < K, lax.shift_left(jnp.ones_like(whole), whole * FIELD), 0)

    for j in range(peers):
        marks[j] = bits(codes[j])

    for sb in range(ns):
        for rb in range(nr):
            j = rb * ns + sb
            logits = log_terms([shaded[j, m] for m in range(M)], means, halves, shift)
            code = codes[j]
            here = marks[j]
            near = around(lambda a, b: marks[b * ns + a], sb, rb, grid, rows, 0)
            near = near + [pltpu.roll(here, 1, 0), pltpu.roll(here, window - 1, 0)]
            near = functools.reduce(jnp.add, near)
            for k in range(K):
                dens[k, j] = logits[k]
                number = lax.shift_right_logical(near, jnp.full_like(near, k * FIELD))
                logits[k] = logits[k] + (number & (2**FIELD - 1)).astype(jnp.float32)
            inside = (code < float(K)).astype(jnp.float32)
            for k, value in enumerate(soft(logits, inside)):
                one[k, j] = value
    for sb in range(ns):
        for rb in range(nr):
            j = rb * ns + sb
            logits = []
            for k in range(K):
                here = one[k, j]
                near = around(lambda a, b: one[k, b * ns + a], sb, rb, grid, rows, 0.0)
                near = near + [pltpu.roll(here, 1, 0), pltpu.roll(here, window - 1, 0)]
                logits.append(dens[k, j] + functools.reduce(jnp.add, near))
            inside = (codes[j] < float(K)).astype(jnp.float32)
            for k, value in enumerate(soft(logits, inside)):
                two[k, j] = value
    for sb in range(ns):
        for rb in range(nr):
            j = rb * ns + sb
            totals = []
            for k in range(K):
                near = around(
                    lambda a, b: two[k, b * ns + a, EDGE : EDGE + core, :], sb, rb, grid, rows, 0.0
                )
                near = near + [
                    two[k, j, EDGE - 1 : EDGE - 1 + core, :],
                    two[k, j, EDGE + 1 : EDGE + 1 + core, :],
                ]
                totals.append(functools.reduce(jnp.add, near))
            for k in range(K - 1):
                send[j, k * core : (k + 1) * core, :] = totals[k] - totals[K - 1]
    sums = []
    for k in range(K):
        line = [jnp.zeros((SUB, LANES), jnp.float32) for _ in range(STATS)]
        for j in range(peers):
            here = two[k, j, EDGE : EDGE + core, :]
            keep[k, j] = here
            line[0] = line[0] + fold(here)
            for m in range(M):
                field = shaded[j, m, EDGE : EDGE + core, :]
                value = here * field
                line[1 + m] = line[1 + m] + fold(value)
                line[1 + M + m] = line[1 + M + m] + fold(value * field)
        sums.append([jnp.sum(x, axis=0, keepdims=True) for x in line])
    row = stat_row(sums)
    for p in range(peers):
        send[p, (K - 1) * core : (K - 1) * core + 1, :] = row


def residual_kernel(
    pack, grid, stat_a, stat_b, keep, raw, slab_table, row_table, send, first, second
):
    ns, nr = grid
    core = pack.core
    means = mean_rows(stat_a[...] + stat_b[...])
    for sb in range(ns):
        for rb in range(nr):
            j = rb * ns + sb
            for m in range(M):
                base = m * pack.wide + 2
                field = raw[j, base : base + core, :]
                total = jnp.zeros_like(field)
                for k in range(K):
                    total = total + keep[k, j] * (field - means[m][k : k + 1, :])
                base = (rb * M + m) * core
                first[base : base + core, sb * LANES : (sb + 1) * LANES] = total
    rows = M * core
    done = slab_row_filter(rows, slab_table, row_table, first, second, grid)
    for sb in range(ns):
        for rb in range(nr):
            send[rb * ns + sb] = done[sb * rows : (sb + 1) * rows, rb * LANES : (rb + 1) * LANES]


def columns_of(ref, m, core):
    return ref[:, m * core : (m + 1) * core, :].reshape(LANES, LANES).T


def half_kernel(got, near, table, field, around):
    core = got.shape[1] // M
    for m in range(M):
        field[m] = dot(columns_of(got, m, core), (table[0, :LANES, :], table[1, :LANES, :]))
    for k in range(K - 1):
        around[k] = columns_of(near, k, core)


def third_kernel(
    rows,
    field,
    got,
    near,
    own,
    stat_a,
    stat_b,
    table,
    place,
    bias,
    centers,
    dens,
    belief,
    up,
    down,
    side,
    edge,
):
    core = got.shape[1] // M
    slabs = LANES // rows
    means, halves, shift = class_stats(stat_a[...] + stat_b[...])
    for m in range(M):
        centers[:, m : m + 1] = means[m][:, :1]
        bias[m] = field[m] + dot(
            columns_of(got, m, core), (table[0, LANES:, :], table[1, LANES:, :])
        )
    lane = lax.broadcasted_iota(jnp.int32, (1, LANES), 1)
    even = place[0, 0:1, :] == 0
    shiftback = jnp.where(place[2, 0:1, :] == 0, 1, 0)
    marks = [(lane + shiftback) % LANES == k for k in range(K)]
    for s in range(slabs):
        low, high = s * rows, (s + 1) * rows
        corrected = [own[m, low:high, :] - bias[m, low:high, :] for m in range(M)]
        logits = log_terms(corrected, means, halves, shift)
        for k in range(K):
            dens[k, low:high, :] = logits[k]
            if k < K - 1:
                logits[k] = logits[k] + near[k, low:high, :]
        inside = (own[M, low:high, :] < float(K)).astype(jnp.float32)
        column = jnp.zeros((rows, LANES), jnp.float32)
        for k, value in enumerate(soft(logits, inside)):
            belief[k, low:high, :] = value
            column = jnp.where(marks[k], pltpu.roll(value, k, 1), column)
        edge[low:high, :] = column
    for k in range(K):
        first = belief[k, :rows, :]
        final = belief[k, LANES - rows :, :]
        up[k] = jnp.where(even, final, first)
        down[k] = jnp.where(even, first, final)
    lead = place[1, 0:1, :] == 0
    for k in range(K):
        head = belief[k, pl.ds(0, slabs, rows), :]
        tail = belief[k, pl.ds(rows - 1, slabs, rows), :]
        side[k] = jnp.where(lead, tail, head)


def inner_kernel(rows, dens, belief, bias, logits, bias_h, sems):
    copy = pltpu.make_async_copy(bias, bias_h, sems.at[0])
    copy.start()
    lane = lax.broadcasted_iota(jnp.int32, (1, LANES), 1)
    line = lax.broadcasted_iota(jnp.int32, (rows, 1), 0)
    for k in range(K):
        for low in range(0, LANES, rows):
            here = belief[k, low : low + rows, :]
            total = dens[k, low : low + rows, :]
            if low > 0:
                total = total + belief[k, low - rows : low, :]
            if low + rows < LANES:
                total = total + belief[k, low + rows : low + 2 * rows, :]
            total = total + jnp.where(line > 0, pltpu.roll(here, 1, 0), 0.0)
            total = total + jnp.where(line < rows - 1, pltpu.roll(here, rows - 1, 0), 0.0)
            total = total + jnp.where(lane > 0, pltpu.roll(here, 1, 1), 0.0)
            total = total + jnp.where(lane < LANES - 1, pltpu.roll(here, LANES - 1, 1), 0.0)
            logits[k, low : low + rows, :] = total
    copy.wait()


def last_kernel(rows, inner, own, up, down, side, edge, place, post_h, post, sems):
    slabs = LANES // rows
    lane = lax.broadcasted_iota(jnp.int32, (1, LANES), 1)
    line = lax.broadcasted_iota(jnp.int32, (rows, 1), 0)
    even = place[0, 0:1, :] == 0
    left = place[2, 0:1, :] == 0
    spot = lane == jnp.where(left, LANES - 1, 0)
    face = line == jnp.where(place[1, 0:1, :] == 0, rows - 1, 0)
    copies = []
    for s in range(slabs):
        low, high = s * rows, (s + 1) * rows
        column = edge[low:high, :]
        column = jnp.where(left, column, pltpu.roll(column, 2, 1))
        logits = []
        for k in range(K):
            total = inner[k, low:high, :]
            if s == 0:
                total = total + jnp.where(even, down[k], up[k])
            if s == slabs - 1:
                total = total + jnp.where(even, up[k], down[k])
            total = total + jnp.where(face, side[k, s : s + 1, :], 0.0)
            total = total + jnp.where(spot, pltpu.roll(column, LANES - 1 - k, 1), 0.0)
            logits.append(total)
        inside = (own[M, low:high, :] < float(K)).astype(jnp.float32)
        for k, value in enumerate(soft(logits, inside)):
            post[k, low:high, :] = value.astype(jnp.bfloat16)
        span = pl.ds(low, rows)
        copies.append(
            pltpu.make_async_copy(post.at[:, span, :], post_h.at[:, span, :], sems.at[s])
        )
        copies[-1].start()
    for copy in copies:
        copy.wait()


class Pack(typing.NamedTuple):
    core: int
    wide: int
    code: int
    stat: int


def padded(rows):
    return -(-rows // SUB) * SUB


def call(kernel, outs, scratch=(), micros=1, far_out=()):
    vmem = pl.BlockSpec(memory_space=pltpu.VMEM)
    far = pl.BlockSpec(memory_space=pltpu.HBM)
    shapes = [jax.ShapeDtypeStruct(shape, kind) for shape, kind in outs]

    def run(*args):
        return pl.pallas_call(
            kernel,
            out_shape=shapes,
            in_specs=[vmem] * len(args),
            out_specs=[far if i in far_out else vmem for i in range(len(shapes))],
            scratch_shapes=[
                pltpu.VMEM(x, jnp.float32) if isinstance(x, tuple) else x for x in scratch
            ],
            compiler_params=pltpu.CompilerParams(vmem_limit_bytes=VMEM_BYTES),
            cost_estimate=pl.CostEstimate(
                flops=micros * 10_000_000, bytes_accessed=2**20, transcendentals=0
            ),
            name=(kernel.func if isinstance(kernel, functools.partial) else kernel).__name__,
        )(*args)

    return run


def pencils(image, brain_mask, labels):
    _, slabs, rows, columns = image.shape
    ns, nr, nc = (lax.axis_size(a) for a in ("slab", "row", "col"))
    grid = (ns, nr)
    peers = ns * nr
    core = columns // peers
    window = core + 2 * EDGE
    wide_rows = core + 4
    pack = Pack(core, wide_rows, M * wide_rows, M * wide_rows + core + 2)
    f32 = jnp.float32
    place = jnp.stack([lax.axis_index("slab") % 2, lax.axis_index("row"), lax.axis_index("col")])
    place = jnp.broadcast_to(place.astype(jnp.int32)[:, None, None], (3, SUB, LANES))
    swap = [(0, 1), (1, 0)]

    taps = impulse(columns * nc)
    reach = np.arange(-MARGIN, columns + MARGIN)
    source = np.concatenate([np.arange(columns), np.arange(columns) + columns])
    spread = taps[(reach[:, None] - source[None, :]) % (columns * nc)]
    gather = table_of(spread[MARGIN : MARGIN + columns].T)
    spread = table_of(spread)
    slab_table = table_of(np.kron(dense(slabs * ns), np.eye(rows)))
    row_table = np.einsum(
        "arbq,st->asrbtq", dense(rows * nr).reshape(nr, rows, nr, rows), np.eye(slabs)
    )
    row_table = table_of(row_table.reshape(nr * LANES, nr * LANES))

    code = jnp.where(brain_mask > 0, labels, K).astype(f32)
    own = jnp.concatenate([image, code[None]]).reshape(M + 1, LANES, columns)
    image_o = lax.ppermute(image.reshape(M, LANES, columns), "col", swap)
    mask_o = lax.ppermute(brain_mask.reshape(LANES, columns), "col", swap)
    labels_o = lax.ppermute(labels.reshape(LANES, columns), "col", swap)

    def trade(x):
        return lax.all_to_all(x, ("row", "slab"), split_axis=0, concat_axis=0, tiled=True)

    turned, stat = call(
        own_kernel, [((M + 1, columns, LANES), f32), ((SUB, LANES), f32)]
    )(own)
    sent, rest, code_o = call(
        functools.partial(prepare_kernel, pack),
        [
            ((peers, padded(pack.stat + 1), LANES), f32),
            ((peers, SUB, LANES), f32),
            ((LANES, columns), f32),
        ],
        [(M + 1, columns + 2 * MARGIN, LANES)],
    )(turned, stat, image_o, mask_o, labels_o, place)
    raw = trade(sent)
    (sent,) = call(
        functools.partial(column_kernel, pack),
        [((peers, padded(pack.code + 4), LANES), f32)],
        [(M * LANES, 2 * columns), (columns + 2 * MARGIN, M * LANES)],
    )(own, image_o, code_o, raw, rest, spread)
    got = trade(sent)
    sent, keep = call(
        functools.partial(pencil_kernel, pack, grid, rows),
        [
            ((peers, padded((K - 1) * core + 1), LANES), f32),
            ((K, peers, core, LANES), f32),
        ],
        [
            (nr * M * window, ns * LANES),
            (ns * M * window, nr * LANES),
            (ns * M * window, nr * LANES),
            (peers, window, LANES),
            pltpu.VMEM((peers, window, LANES), jnp.int32),
            (peers, M, window, LANES),
            (K, peers, window, LANES),
            (K, peers, window, LANES),
            (K, peers, window, LANES),
        ],
        micros=4,
    )(got, raw, slab_table, row_table)
    near = trade(sent)
    stat_a = jnp.sum(near[:, (K - 1) * core : (K - 1) * core + 1, :], axis=0)
    stat_b = lax.ppermute(stat_a, "col", swap)
    (sent,) = call(
        functools.partial(residual_kernel, pack, grid),
        [((peers, M * core, LANES), f32)],
        [(nr * M * core, ns * LANES), (ns * M * core, nr * LANES)],
    )(stat_a, stat_b, keep, raw, slab_table, row_table)
    got = trade(sent)
    yours = lax.ppermute(got, "col", swap)
    field, near = call(
        half_kernel, [((M, LANES, columns), f32), ((K - 1, LANES, columns), f32)]
    )(got, near, gather)
    bias, centers, dens, belief, up, down, side, edge = call(
        functools.partial(third_kernel, rows),
        [
            ((M, LANES, columns), f32),
            ((K, M), f32),
            ((K, LANES, columns), f32),
            ((K, LANES, columns), f32),
            ((K, rows, columns), f32),
            ((K, rows, columns), f32),
            ((K, slabs, columns), f32),
            ((LANES, LANES), f32),
        ],
        micros=2,
    )(field, yours, near, own, stat_a, stat_b, gather, place)
    pairs = [(i, i + 1) for i in range(0, ns - 1, 2)]
    between = [(i, i + 1) for i in range(1, ns - 1, 2)]
    up = lax.ppermute(up, "slab", pairs + [(b, a) for a, b in pairs])
    down = lax.ppermute(down, "slab", between + [(b, a) for a, b in between])
    side = lax.ppermute(side, "row", swap)
    edge = lax.ppermute(edge, "col", swap)
    inner, bias = call(
        functools.partial(inner_kernel, rows),
        [((K, LANES, columns), f32), ((M, LANES, columns), f32)],
        [pltpu.SemaphoreType.DMA((1,))],
        far_out=(1,),
    )(dens, belief, bias)
    (post,) = call(
        functools.partial(last_kernel, rows),
        [((K, LANES, columns), jnp.bfloat16)],
        [
            pltpu.VMEM((K, LANES, columns), jnp.bfloat16),
            pltpu.SemaphoreType.DMA((slabs,)),
        ],
        far_out=(0,),
    )(inner, own, up, down, side, edge, place)
    shape = (slabs, rows, columns)
    return post.reshape((K,) + shape), bias.reshape((M,) + shape), centers


def local(image, brain_mask, labels):
    _, slabs, rows, columns = image.shape
    peers = lax.axis_size("slab") * lax.axis_size("row")
    fits = slabs * rows == LANES and columns == LANES and slabs % SUB == 0 and rows % SUB == 0
    fits = fits and lax.axis_size("row") == 2 and lax.axis_size("col") == 2
    fits = fits and columns % (SUB * peers) == 0
    return (pencils if fits else general)(image, brain_mask, labels)


def solution(mesh):
    placed = (
        P(None, ("grp", "slab"), "row", "col"),
        P(("grp", "slab"), "row", "col"),
        P(("grp", "slab"), "row", "col"),
    )
    return jax.shard_map(
        local,
        mesh=mesh,
        in_specs=placed,
        out_specs=(
            P(None, ("grp", "slab"), "row", "col"),
            P(None, ("grp", "slab"), "row", "col"),
            P("grp", None),
        ),
        check_vma=False,
    )
```

```python
import functools
import math
import typing

import jax
import jax.numpy as jnp
import numpy as np
from jax import lax
from jax.experimental import pallas as pl
from jax.experimental.pallas import tpu as pltpu
from jax.sharding import PartitionSpec as P

M = 3
K = 8
EM_ITERS = 2
MF_PASSES = 2


highest = lax.Precision.HIGHEST
coupling = 1.0
breadth = 8.0


def extended(cells, sides, width):
    for axis, dim in sides:
        count = lax.axis_size(axis)
        ends = count - 1
        head = lax.slice_in_dim(cells, 0, width, axis=dim)
        tail = lax.slice_in_dim(cells, cells.shape[dim] - width, cells.shape[dim], axis=dim)
        cells = jnp.concatenate(
            [
                lax.ppermute(tail, axis, [(i, (i + 1) % count) for i in range(ends)]),
                cells,
                lax.ppermute(head, axis, [((i + 1) % count, i) for i in range(ends)]),
            ],
            axis=dim,
        )
    return cells


def circulant(length):
    index = jnp.arange(length, dtype=jnp.int32)
    folded = jnp.minimum(index, length - index).astype(jnp.float32) / length
    response = jnp.exp(-2.0 * math.pi**2 * (length / breadth) ** 2 * folded * folded)
    product = index[:, None] * index[None, :] % length
    angles = 2.0 * math.pi / length * product.astype(jnp.float32)
    cosine = jnp.cos(angles)
    sine = jnp.sin(angles)
    even_part = jnp.dot(cosine * response[None, :], cosine.T, precision=highest)
    odd_part = jnp.dot(sine * response[None, :], sine.T, precision=highest)
    return (even_part + odd_part) / length


def neighbour_sum(belief):
    padded = extended(belief, (("slab", 1), ("row", 2), ("col", 3)), 1)
    total = padded[:, 2:, 1:-1, 1:-1] + padded[:, :-2, 1:-1, 1:-1]
    total = total + padded[:, 1:-1, 2:, 1:-1] + padded[:, 1:-1, :-2, 1:-1]
    total = total + padded[:, 1:-1, 1:-1, 2:] + padded[:, 1:-1, 1:-1, :-2]
    return total


def class_moments(belief, corrected):
    flat = belief.reshape(K, -1)
    values = corrected.reshape(M, -1)
    count, first, squares = lax.psum(
        (
            jnp.sum(flat, axis=1),
            jnp.dot(flat, values.T, precision=highest),
            jnp.dot(flat, (values * values).T, precision=highest),
        ),
        ("slab", "row", "col"),
    )
    means = first / (count + 1.0)[:, None]
    spread = squares - 2.0 * means * first + means * means * count[:, None]
    variance = (spread + 1.0) / (count + 1.0)[:, None]
    return (count, means, variance)


def log_density(corrected, means, variance, prior):
    offset = corrected[None] - means[:, :, None, None, None]
    terms = (
        offset * offset / variance[:, :, None, None, None]
        + jnp.log(variance)[:, :, None, None, None]
    )
    return jnp.log(prior)[:, None, None, None] - 0.5 * jnp.sum(terms, axis=1)


def smoothed(residual, column_local, row_table, slab_table):
    across = jnp.einsum(
        "msrc,cd->msrd",
        lax.all_gather(residual, "col", axis=3, tiled=True),
        column_local,
        precision=highest,
    )
    mixed = jnp.einsum(
        "msrc,rq->msqc",
        lax.all_to_all(across, "row", split_axis=1, concat_axis=2, tiled=True),
        row_table,
        precision=highest,
    )
    across = lax.all_to_all(mixed, "row", split_axis=2, concat_axis=1, tiled=True)
    mixed = jnp.einsum(
        "msrc,sq->mqrc",
        lax.all_to_all(across, "slab", split_axis=2, concat_axis=1, tiled=True),
        slab_table,
        precision=highest,
    )
    return lax.all_to_all(mixed, "slab", split_axis=1, concat_axis=2, tiled=True)


def general(image, brain_mask, labels):
    channels, slabs, rows, columns = image.shape
    inside = brain_mask.astype(jnp.float32)
    kinds = jnp.arange(K, dtype=jnp.int32)
    belief = (labels[None] == kinds[:, None, None, None]).astype(jnp.float32) * inside[None]
    column_table = circulant(columns * lax.axis_size("col"))
    column_local = lax.dynamic_slice_in_dim(
        column_table, lax.axis_index("col") * columns, columns, 1
    )
    row_table = circulant(rows * lax.axis_size("row"))
    slab_table = circulant(slabs * lax.axis_size("slab"))
    bias_field = jnp.zeros_like(image)
    means = jnp.zeros((K, channels), jnp.float32)
    for iteration in range(EM_ITERS):
        corrected = image - bias_field
        count, means, variance = class_moments(belief, corrected)
        prior = (count + 1.0) / (jnp.sum(count) + K)
        total = jnp.sum(belief, axis=0)
        removed = jnp.dot(means.T, belief.reshape(K, -1), precision=highest).reshape(image.shape)
        residual = image * total[None] - removed
        bias_field = smoothed(residual, column_local, row_table, slab_table)
        corrected = image - bias_field
        density = log_density(corrected, means, variance, prior)
        for sweep_index in range(MF_PASSES):
            belief = (
                jax.nn.softmax(density + coupling * neighbour_sum(belief), axis=0) * inside[None]
            )
    return (belief.astype(jnp.bfloat16), bias_field, means)


LANES = 128
SUB = 8
EDGE = 4
MARGIN = 8
FIELD = 4
STATS = 1 + 2 * M
VMEM_BYTES = 16 * 2**20


def impulse(length):
    index = np.arange(length)
    folded = np.minimum(index, length - index) / length
    response = np.exp(-2.0 * np.pi**2 * (length / breadth) ** 2 * folded * folded)
    angles = 2.0 * np.pi / length * (index[:, None] * index[None, :] % length)
    return np.cos(angles) @ response / length


def dense(length):
    index = np.arange(length)
    return impulse(length)[(index[:, None] - index[None, :]) % length]


def halves_of(x):
    high = x.astype(jnp.bfloat16)
    return high, (x - high.astype(jnp.float32)).astype(jnp.bfloat16)


def table_of(x):
    high = x.astype(jnp.bfloat16)
    low = (x - high.astype(np.float64)).astype(jnp.bfloat16)
    return np.stack([high, low])


def dot(left, right, dims=((1,), (0,))):
    left, right = (x if isinstance(x, tuple) else halves_of(x) for x in (left, right))

    def one(a, b):
        return lax.dot_general(a, b, (dims, ((), ())), preferred_element_type=jnp.float32)

    return one(left[0], right[0]) + (one(left[1], right[0]) + one(left[0], right[1]))


def wide(row, shape=(SUB, LANES)):
    return jnp.broadcast_to(row, shape)


def stat_row(sums):
    sub = lax.broadcasted_iota(jnp.int32, (SUB, LANES), 0)
    lane = lax.broadcasted_iota(jnp.int32, (SUB, LANES), 1)
    tile = jnp.zeros((SUB, LANES), jnp.float32)
    for q in range(STATS):
        rows = jnp.zeros((SUB, LANES), jnp.float32)
        for k in range(K):
            line = jnp.sum(sums[k][q], axis=0, keepdims=True)
            rows = jnp.where(sub == k, line, rows)
        tile = jnp.where(lane == q * K + sub, jnp.sum(rows, axis=1, keepdims=True), tile)
    return jnp.sum(tile, axis=0, keepdims=True)


def stat_columns(row, number):
    sub = lax.broadcasted_iota(jnp.int32, (SUB, LANES), 0)
    lane = lax.broadcasted_iota(jnp.int32, (SUB, LANES), 1)
    return [
        jnp.sum(jnp.where(lane == q * K + sub, row, 0.0), axis=1, keepdims=True)
        for q in range(number)
    ]


def fold(x):
    return jnp.sum(x.reshape(x.shape[0] // SUB, SUB, LANES), axis=0)


def class_stats(row):
    count, *rest = stat_columns(row, STATS)
    means, halves = [], []
    shift = jnp.zeros_like(count)
    for m in range(M):
        first, squares = rest[m], rest[M + m]
        mean = first / (count + 1.0)
        spread = squares - 2.0 * mean * first + mean * mean * count
        variance = (spread + 1.0) / (count + 1.0)
        means.append(wide(mean))
        halves.append(wide(0.5 / variance))
        shift = shift - 0.5 * jnp.log(variance)
    prior = (count + 1.0) / (jnp.sum(count, axis=0, keepdims=True) + K)
    return means, halves, wide(jnp.log(prior) + shift)


def mean_rows(row):
    count, *rest = stat_columns(row, 1 + M)
    return [wide(x / (count + 1.0)) for x in rest]


def log_terms(corrected, means, halves, shift):
    out = []
    for k in range(K):
        total = wide(shift[k : k + 1, :], corrected[0].shape)
        for m in range(M):
            offset = corrected[m] - means[m][k : k + 1, :]
            total = total - offset * offset * halves[m][k : k + 1, :]
        out.append(total)
    return out


def soft(logits, inside):
    top = functools.reduce(jnp.maximum, logits)
    exps = [jnp.exp(x - top) for x in logits]
    scale = inside / functools.reduce(jnp.add, exps)
    return [x * scale for x in exps]


def peer_sum(ref, line):
    row = ref[0, line : line + 1, :]
    for j in range(1, ref.shape[0]):
        row = row + ref[j, line : line + 1, :]
    return row


def class_sums(code, image):
    sums = []
    for k in range(K):
        flag = (code == float(k)).astype(jnp.float32)
        line = [fold(flag)]
        weighted = [flag * image[m] for m in range(M)]
        line += [fold(x) for x in weighted]
        line += [fold(x * image[m]) for m, x in enumerate(weighted)]
        sums.append(line)
    return sums


def own_kernel(own, turned, stat):
    stat[...] = wide(stat_row(class_sums(own[M], own)))
    for f in range(M + 1):
        turned[f] = own[f].T


def prepare_kernel(
    pack, turned, stat, image_o, mask_o, labels_o, place, send, rest, code_o, ext
):
    peers = send.shape[0]
    step = LANES // peers
    first = place[2] == 0
    code_o[...] = jnp.where(mask_o[...] > 0, labels_o[...], K).astype(jnp.float32)
    row = stat[0:1, :] + stat_row(class_sums(code_o[...], image_o))
    for f in range(M + 1):
        blank = jnp.full((SUB, LANES), float(K) if f == M else 0.0, jnp.float32)
        other = (image_o[f] if f < M else code_o[...]).T
        ext[f, 0:MARGIN, :] = jnp.where(first, blank, other[LANES - MARGIN :, :])
        ext[f, MARGIN : MARGIN + LANES, :] = turned[f]
        ext[f, MARGIN + LANES :, :] = jnp.where(first, other[:MARGIN, :], blank)
    for p in range(peers):
        at = MARGIN + step * p
        for m in range(M):
            send[p, pack.wide * m : pack.wide * (m + 1), :] = ext[m, at - 2 : at + step + 2, :]
        send[p, pack.code : pack.stat, :] = ext[M, at - 1 : at + step + 1, :]
        send[p, pack.stat : pack.stat + 1, :] = row
        rest[p, 0:2, :] = ext[M, at - 3 : at - 1, :]
        rest[p, 2:4, :] = ext[M, at + step + 1 : at + step + 3, :]


def column_kernel(pack, own, image_o, code_o, got, rest, table, send, flat, out):
    peers = send.shape[0]
    step = LANES // peers
    means = mean_rows(peer_sum(got, pack.stat))
    for h, (ref, code) in enumerate(((own, own[M]), (image_o, code_o[...]))):
        flags = [code == float(k) for k in range(K)]
        for m in range(M):
            center = jnp.zeros_like(code)
            for k in range(K):
                center = jnp.where(flags[k], means[m][k : k + 1, :], center)
            flat[m * LANES : (m + 1) * LANES, h * LANES : (h + 1) * LANES] = jnp.where(
                code < float(K), ref[m] - center, 0.0
            )
    out[...] = dot((table[0], table[1]), flat[...], ((1,), (1,)))
    for p in range(peers):
        at = MARGIN + step * p
        send[p, pack.code : pack.code + 4, :] = rest[p, 0:4, :]
        for m in range(M):
            send[p, pack.wide * m : pack.wide * (m + 1), :] = out[
                at - 2 : at + step + 2, m * LANES : (m + 1) * LANES
            ]


def slab_row_filter(rows, slab_table, row_table, first, second, grid):
    ns, nr = grid
    mixed = dot(first[...], (slab_table[0], slab_table[1]))
    for sb in range(ns):
        for rb in range(nr):
            second[sb * rows : (sb + 1) * rows, rb * LANES : (rb + 1) * LANES] = mixed[
                rb * rows : (rb + 1) * rows, sb * LANES : (sb + 1) * LANES
            ]
    return dot(second[...], (row_table[0], row_table[1]))


def around(get, sb, rb, grid, rows, fill):
    ns, nr = grid
    lane = lax.broadcasted_iota(jnp.int32, (1, LANES), 1)
    place = lane % rows
    here = get(sb, rb)
    empty = jnp.full_like(here, fill)
    above = get(sb + 1, rb) if sb + 1 < ns else empty
    below = get(sb - 1, rb) if sb > 0 else empty
    out = [
        pltpu.roll(jnp.where(lane >= rows, here, above), LANES - rows, 1),
        pltpu.roll(jnp.where(lane < LANES - rows, here, below), rows, 1),
    ]
    right = pltpu.roll(get(sb, rb + 1), rows - 1, 1) if rb + 1 < nr else empty
    left = pltpu.roll(get(sb, rb - 1), LANES - rows + 1, 1) if rb > 0 else empty
    out.append(jnp.where(place < rows - 1, pltpu.roll(here, LANES - 1, 1), right))
    out.append(jnp.where(place > 0, pltpu.roll(here, 1, 1), left))
    return out


def pencil_kernel(
    pack,
    grid,
    rows,
    got,
    raw,
    slab_table,
    row_table,
    send,
    keep,
    first,
    second,
    bias,
    codes,
    marks,
    shaded,
    dens,
    one,
    two,
):
    ns, nr = grid
    peers = ns * nr
    core = pack.core
    window = core + 2 * EDGE
    means, halves, shift = class_stats(peer_sum(raw, pack.stat))
    first[...] = jnp.zeros_like(first)
    for sb in range(ns):
        for rb in range(nr):
            for m in range(M):
                base = (rb * M + m) * window + EDGE - 2
                first[base : base + pack.wide, sb * LANES : (sb + 1) * LANES] = got[
                    rb * ns + sb, m * pack.wide : (m + 1) * pack.wide, :
                ]
    bias[...] = slab_row_filter(M * window, slab_table, row_table, first, second, grid)
    blank = jnp.full((window, LANES), float(K), jnp.float32)
    for sb in range(ns):
        for rb in range(nr):
            j = rb * ns + sb
            codes[j] = blank
            codes[j, EDGE - 3 : EDGE - 1, :] = got[j, pack.code : pack.code + 2, :]
            codes[j, EDGE - 1 : EDGE + core + 1, :] = raw[j, pack.code : pack.stat, :]
            codes[j, EDGE + core + 1 : EDGE + core + 3, :] = got[j, pack.code + 2 : pack.code + 4, :]
            for m in range(M):
                base = (sb * M + m) * window
                shaded[j, m] = -bias[base : base + window, rb * LANES : (rb + 1) * LANES]
                shaded[j, m, EDGE - 2 : EDGE - 2 + pack.wide, :] += raw[
                    j, m * pack.wide : (m + 1) * pack.wide, :
                ]

    def bits(x):
        whole = x.astype(jnp.int32)
        return jnp.where(whole < K, lax.shift_left(jnp.ones_like(whole), whole * FIELD), 0)

    for j in range(peers):
        marks[j] = bits(codes[j])

    for sb in range(ns):
        for rb in range(nr):
            j = rb * ns + sb
            logits = log_terms([shaded[j, m] for m in range(M)], means, halves, shift)
            code = codes[j]
            here = marks[j]
            near = around(lambda a, b: marks[b * ns + a], sb, rb, grid, rows, 0)
            near = near + [pltpu.roll(here, 1, 0), pltpu.roll(here, window - 1, 0)]
            near = functools.reduce(jnp.add, near)
            for k in range(K):
                dens[k, j] = logits[k]
                number = lax.shift_right_logical(near, jnp.full_like(near, k * FIELD))
                logits[k] = logits[k] + (number & (2**FIELD - 1)).astype(jnp.float32)
            inside = (code < float(K)).astype(jnp.float32)
            for k, value in enumerate(soft(logits, inside)):
                one[k, j] = value
    for sb in range(ns):
        for rb in range(nr):
            j = rb * ns + sb
            logits = []
            for k in range(K):
                here = one[k, j]
                near = around(lambda a, b: one[k, b * ns + a], sb, rb, grid, rows, 0.0)
                near = near + [pltpu.roll(here, 1, 0), pltpu.roll(here, window - 1, 0)]
                logits.append(dens[k, j] + functools.reduce(jnp.add, near))
            inside = (codes[j] < float(K)).astype(jnp.float32)
            for k, value in enumerate(soft(logits, inside)):
                two[k, j] = value
    for sb in range(ns):
        for rb in range(nr):
            j = rb * ns + sb
            totals = []
            for k in range(K):
                near = around(
                    lambda a, b: two[k, b * ns + a, EDGE : EDGE + core, :], sb, rb, grid, rows, 0.0
                )
                near = near + [
                    two[k, j, EDGE - 1 : EDGE - 1 + core, :],
                    two[k, j, EDGE + 1 : EDGE + 1 + core, :],
                ]
                totals.append(functools.reduce(jnp.add, near))
            for k in range(K - 1):
                send[j, k * core : (k + 1) * core, :] = totals[k] - totals[K - 1]
    sums = []
    for k in range(K):
        line = [jnp.zeros((SUB, LANES), jnp.float32) for _ in range(STATS)]
        for j in range(peers):
            here = two[k, j, EDGE : EDGE + core, :]
            keep[k, j] = here
            line[0] = line[0] + fold(here)
            for m in range(M):
                field = shaded[j, m, EDGE : EDGE + core, :]
                value = here * field
                line[1 + m] = line[1 + m] + fold(value)
                line[1 + M + m] = line[1 + M + m] + fold(value * field)
        sums.append([jnp.sum(x, axis=0, keepdims=True) for x in line])
    row = stat_row(sums)
    for p in range(peers):
        send[p, (K - 1) * core : (K - 1) * core + 1, :] = row


def residual_kernel(
    pack, grid, stat_a, stat_b, keep, raw, slab_table, row_table, send, first, second
):
    ns, nr = grid
    core = pack.core
    means = mean_rows(stat_a[...] + stat_b[...])
    for sb in range(ns):
        for rb in range(nr):
            j = rb * ns + sb
            for m in range(M):
                base = m * pack.wide + 2
                field = raw[j, base : base + core, :]
                total = jnp.zeros_like(field)
                for k in range(K):
                    total = total + keep[k, j] * (field - means[m][k : k + 1, :])
                base = (rb * M + m) * core
                first[base : base + core, sb * LANES : (sb + 1) * LANES] = total
    rows = M * core
    done = slab_row_filter(rows, slab_table, row_table, first, second, grid)
    for sb in range(ns):
        for rb in range(nr):
            send[rb * ns + sb] = done[sb * rows : (sb + 1) * rows, rb * LANES : (rb + 1) * LANES]


def columns_of(ref, m, core):
    return ref[:, m * core : (m + 1) * core, :].reshape(LANES, LANES).T


def half_kernel(got, near, table, field, around):
    core = got.shape[1] // M
    for m in range(M):
        field[m] = dot(columns_of(got, m, core), (table[0, :LANES, :], table[1, :LANES, :]))
    for k in range(K - 1):
        around[k] = columns_of(near, k, core)


def third_kernel(
    rows,
    field,
    got,
    near,
    own,
    stat_a,
    stat_b,
    table,
    place,
    bias,
    centers,
    dens,
    belief,
    up,
    down,
    side,
    edge,
):
    core = got.shape[1] // M
    slabs = LANES // rows
    means, halves, shift = class_stats(stat_a[...] + stat_b[...])
    for m in range(M):
        centers[:, m : m + 1] = means[m][:, :1]
        bias[m] = field[m] + dot(
            columns_of(got, m, core), (table[0, LANES:, :], table[1, LANES:, :])
        )
    lane = lax.broadcasted_iota(jnp.int32, (1, LANES), 1)
    even = place[0, 0:1, :] == 0
    shiftback = jnp.where(place[2, 0:1, :] == 0, 1, 0)
    marks = [(lane + shiftback) % LANES == k for k in range(K - 1)]
    for s in range(slabs):
        low, high = s * rows, (s + 1) * rows
        corrected = [own[m, low:high, :] - bias[m, low:high, :] for m in range(M)]
        logits = log_terms(corrected, means, halves, shift)
        for k in range(K):
            dens[k, low:high, :] = logits[k]
            if k < K - 1:
                logits[k] = logits[k] + near[k, low:high, :]
        inside = (own[M, low:high, :] < float(K)).astype(jnp.float32)
        column = jnp.zeros((rows, LANES), jnp.float32)
        shares = soft(logits, inside)
        for k in range(K - 1):
            value = shares[k] - shares[K - 1]
            belief[k, low:high, :] = value
            column = jnp.where(marks[k], pltpu.roll(value, k, 1), column)
        edge[low:high, :] = column
    for k in range(K - 1):
        first = belief[k, :rows, :]
        final = belief[k, LANES - rows :, :]
        up[k] = jnp.where(even, final, first)
        down[k] = jnp.where(even, first, final)
    lead = place[1, 0:1, :] == 0
    for k in range(K - 1):
        head = belief[k, pl.ds(0, slabs, rows), :]
        tail = belief[k, pl.ds(rows - 1, slabs, rows), :]
        side[k] = jnp.where(lead, tail, head)


def inner_kernel(rows, dens, belief, bias, logits, bias_h, sems):
    copy = pltpu.make_async_copy(bias, bias_h, sems.at[0])
    copy.start()
    lane = lax.broadcasted_iota(jnp.int32, (1, LANES), 1)
    line = lax.broadcasted_iota(jnp.int32, (rows, 1), 0)
    for k in range(K - 1):
        for low in range(0, LANES, rows):
            here = belief[k, low : low + rows, :]
            total = dens[k, low : low + rows, :]
            if low > 0:
                total = total + belief[k, low - rows : low, :]
            if low + rows < LANES:
                total = total + belief[k, low + rows : low + 2 * rows, :]
            total = total + jnp.where(line > 0, pltpu.roll(here, 1, 0), 0.0)
            total = total + jnp.where(line < rows - 1, pltpu.roll(here, rows - 1, 0), 0.0)
            total = total + jnp.where(lane > 0, pltpu.roll(here, 1, 1), 0.0)
            total = total + jnp.where(lane < LANES - 1, pltpu.roll(here, LANES - 1, 1), 0.0)
            logits[k, low : low + rows, :] = total
    copy.wait()


def last_kernel(rows, inner, dens, own, up, down, side, edge, place, post_h, post, sems):
    slabs = LANES // rows
    lane = lax.broadcasted_iota(jnp.int32, (1, LANES), 1)
    line = lax.broadcasted_iota(jnp.int32, (rows, 1), 0)
    even = place[0, 0:1, :] == 0
    left = place[2, 0:1, :] == 0
    bottom = place[3, 0:1, :] == 0
    top = place[4, 0:1, :] == 0
    spot = lane == jnp.where(left, LANES - 1, 0)
    face = line == jnp.where(place[1, 0:1, :] == 0, rows - 1, 0)
    copies = []
    for s in range(slabs):
        low, high = s * rows, (s + 1) * rows
        column = edge[low:high, :]
        column = jnp.where(left, column, pltpu.roll(column, 2, 1))
        logits = []
        for k in range(K - 1):
            total = inner[k, low:high, :]
            if s == 0:
                total = total + jnp.where(bottom, 0.0, jnp.where(even, down[k], up[k]))
            if s == slabs - 1:
                total = total + jnp.where(top, 0.0, jnp.where(even, up[k], down[k]))
            total = total + jnp.where(face, side[k, s : s + 1, :], 0.0)
            total = total + jnp.where(spot, pltpu.roll(column, LANES - 1 - k, 1), 0.0)
            logits.append(total)
        logits.append(dens[K - 1, low:high, :])
        inside = (own[M, low:high, :] < float(K)).astype(jnp.float32)
        for k, value in enumerate(soft(logits, inside)):
            post[k, low:high, :] = value.astype(jnp.bfloat16)
        span = pl.ds(low, rows)
        copies.append(
            pltpu.make_async_copy(post.at[:, span, :], post_h.at[:, span, :], sems.at[s])
        )
        copies[-1].start()
    for copy in copies:
        copy.wait()


class Pack(typing.NamedTuple):
    core: int
    wide: int
    code: int
    stat: int


def padded(rows):
    return -(-rows // SUB) * SUB


def call(kernel, outs, scratch=(), micros=1, far_out=()):
    vmem = pl.BlockSpec(memory_space=pltpu.VMEM)
    far = pl.BlockSpec(memory_space=pltpu.HBM)
    shapes = [jax.ShapeDtypeStruct(shape, kind) for shape, kind in outs]

    def run(*args):
        return pl.pallas_call(
            kernel,
            out_shape=shapes,
            in_specs=[vmem] * len(args),
            out_specs=[far if i in far_out else vmem for i in range(len(shapes))],
            scratch_shapes=[
                pltpu.VMEM(x, jnp.float32) if isinstance(x, tuple) else x for x in scratch
            ],
            compiler_params=pltpu.CompilerParams(vmem_limit_bytes=VMEM_BYTES),
            cost_estimate=pl.CostEstimate(
                flops=micros * 10_000_000, bytes_accessed=2**20, transcendentals=0
            ),
            name=(kernel.func if isinstance(kernel, functools.partial) else kernel).__name__,
        )(*args)

    return run


def both_ways(pairs, count):
    steps = []
    for i in range(count):
        other = [b if a == i else a for a, b in pairs if i in (a, b)]
        for side in range(2):
            target = other[0] * 2 + side if other else i * 2 + 1 - side
            steps.append((i * 2 + side, target))
    return steps


def pencils(image, brain_mask, labels):
    _, slabs, rows, columns = image.shape
    ns, nr, nc = (lax.axis_size(a) for a in ("slab", "row", "col"))
    grid = (ns, nr)
    peers = ns * nr
    core = columns // peers
    window = core + 2 * EDGE
    wide_rows = core + 4
    pack = Pack(core, wide_rows, M * wide_rows, M * wide_rows + core + 2)
    f32 = jnp.float32
    slab = lax.axis_index("slab")
    place = [slab % 2, lax.axis_index("row"), lax.axis_index("col"), slab, ns - 1 - slab]
    place = jnp.broadcast_to(jnp.stack(place).astype(jnp.int32)[:, None, None], (5, SUB, LANES))
    swap = [(0, 1), (1, 0)]

    taps = impulse(columns * nc)
    reach = np.arange(-MARGIN, columns + MARGIN)
    source = np.concatenate([np.arange(columns), np.arange(columns) + columns])
    spread = taps[(reach[:, None] - source[None, :]) % (columns * nc)]
    gather = table_of(spread[MARGIN : MARGIN + columns].T)
    spread = table_of(spread)
    slab_table = table_of(np.kron(dense(slabs * ns), np.eye(rows)))
    row_table = np.einsum(
        "arbq,st->asrbtq", dense(rows * nr).reshape(nr, rows, nr, rows), np.eye(slabs)
    )
    row_table = table_of(row_table.reshape(nr * LANES, nr * LANES))

    code = jnp.where(brain_mask > 0, labels, K).astype(f32)
    own = jnp.concatenate([image, code[None]]).reshape(M + 1, LANES, columns)
    image_o = lax.ppermute(image.reshape(M, LANES, columns), "col", swap)
    mask_o = lax.ppermute(brain_mask.reshape(LANES, columns), "col", swap)
    labels_o = lax.ppermute(labels.reshape(LANES, columns), "col", swap)

    def trade(x):
        return lax.all_to_all(x, ("row", "slab"), split_axis=0, concat_axis=0, tiled=True)

    turned, stat = call(
        own_kernel, [((M + 1, columns, LANES), f32), ((SUB, LANES), f32)]
    )(own)
    sent, rest, code_o = call(
        functools.partial(prepare_kernel, pack),
        [
            ((peers, padded(pack.stat + 1), LANES), f32),
            ((peers, SUB, LANES), f32),
            ((LANES, columns), f32),
        ],
        [(M + 1, columns + 2 * MARGIN, LANES)],
    )(turned, stat, image_o, mask_o, labels_o, place)
    raw = trade(sent)
    (sent,) = call(
        functools.partial(column_kernel, pack),
        [((peers, padded(pack.code + 4), LANES), f32)],
        [(M * LANES, 2 * columns), (columns + 2 * MARGIN, M * LANES)],
    )(own, image_o, code_o, raw, rest, spread)
    got = trade(sent)
    sent, keep = call(
        functools.partial(pencil_kernel, pack, grid, rows),
        [
            ((peers, padded((K - 1) * core + 1), LANES), f32),
            ((K, peers, core, LANES), f32),
        ],
        [
            (nr * M * window, ns * LANES),
            (ns * M * window, nr * LANES),
            (ns * M * window, nr * LANES),
            (peers, window, LANES),
            pltpu.VMEM((peers, window, LANES), jnp.int32),
            (peers, M, window, LANES),
            (K, peers, window, LANES),
            (K, peers, window, LANES),
            (K, peers, window, LANES),
        ],
        micros=4,
    )(got, raw, slab_table, row_table)
    near = trade(sent)
    stat_a = jnp.sum(near[:, (K - 1) * core : (K - 1) * core + 1, :], axis=0)
    stat_b = lax.ppermute(stat_a, "col", swap)
    (sent,) = call(
        functools.partial(residual_kernel, pack, grid),
        [((peers, M * core, LANES), f32)],
        [(nr * M * core, ns * LANES), (ns * M * core, nr * LANES)],
    )(stat_a, stat_b, keep, raw, slab_table, row_table)
    got = trade(sent)
    yours = lax.ppermute(got, "col", swap)
    field, near = call(
        half_kernel, [((M, LANES, columns), f32), ((K - 1, LANES, columns), f32)]
    )(got, near, gather)
    bias, centers, dens, belief, up, down, side, edge = call(
        functools.partial(third_kernel, rows),
        [
            ((M, LANES, columns), f32),
            ((K, M), f32),
            ((K, LANES, columns), f32),
            ((K - 1, LANES, columns), f32),
            ((K - 1, rows, columns), f32),
            ((K - 1, rows, columns), f32),
            ((K - 1, slabs, columns), f32),
            ((LANES, LANES), f32),
        ],
        micros=2,
    )(field, yours, near, own, stat_a, stat_b, gather, place)
    pairs = [(i, i + 1) for i in range(0, ns - 1, 2)]
    between = [(i, i + 1) for i in range(1, ns - 1, 2)]
    up = lax.ppermute(up, ("slab", "col"), both_ways(pairs, ns))
    down = lax.ppermute(down, ("slab", "col"), both_ways(between, ns))
    side = lax.ppermute(side, "row", swap)
    edge = lax.ppermute(edge, "col", swap)
    inner, bias = call(
        functools.partial(inner_kernel, rows),
        [((K - 1, LANES, columns), f32), ((M, LANES, columns), f32)],
        [pltpu.SemaphoreType.DMA((1,))],
        far_out=(1,),
    )(dens, belief, bias)
    (post,) = call(
        functools.partial(last_kernel, rows),
        [((K, LANES, columns), jnp.bfloat16)],
        [
            pltpu.VMEM((K, LANES, columns), jnp.bfloat16),
            pltpu.SemaphoreType.DMA((slabs,)),
        ],
        far_out=(0,),
    )(inner, dens, own, up, down, side, edge, place)
    shape = (slabs, rows, columns)
    return post.reshape((K,) + shape), bias.reshape((M,) + shape), centers


def local(image, brain_mask, labels):
    _, slabs, rows, columns = image.shape
    peers = lax.axis_size("slab") * lax.axis_size("row")
    fits = slabs * rows == LANES and columns == LANES and slabs % SUB == 0 and rows % SUB == 0
    fits = fits and lax.axis_size("row") == 2 and lax.axis_size("col") == 2
    fits = fits and columns % (SUB * peers) == 0
    return (pencils if fits else general)(image, brain_mask, labels)


def solution(mesh):
    placed = (
        P(None, ("grp", "slab"), "row", "col"),
        P(("grp", "slab"), "row", "col"),
        P(("grp", "slab"), "row", "col"),
    )
    return jax.shard_map(
        local,
        mesh=mesh,
        in_specs=placed,
        out_specs=(
            P(None, ("grp", "slab"), "row", "col"),
            P(None, ("grp", "slab"), "row", "col"),
            P("grp", None),
        ),
        check_vma=False,
    )
```

```python
import functools
import math
import typing

import jax
import jax.numpy as jnp
import numpy as np
from jax import lax
from jax.experimental import pallas as pl
from jax.experimental.pallas import tpu as pltpu
from jax.sharding import PartitionSpec as P

M = 3
K = 8
EM_ITERS = 2
MF_PASSES = 2


highest = lax.Precision.HIGHEST
coupling = 1.0
breadth = 8.0


def extended(cells, sides, width):
    for axis, dim in sides:
        count = lax.axis_size(axis)
        ends = count - 1
        head = lax.slice_in_dim(cells, 0, width, axis=dim)
        tail = lax.slice_in_dim(cells, cells.shape[dim] - width, cells.shape[dim], axis=dim)
        cells = jnp.concatenate(
            [
                lax.ppermute(tail, axis, [(i, (i + 1) % count) for i in range(ends)]),
                cells,
                lax.ppermute(head, axis, [((i + 1) % count, i) for i in range(ends)]),
            ],
            axis=dim,
        )
    return cells


def circulant(length):
    index = jnp.arange(length, dtype=jnp.int32)
    folded = jnp.minimum(index, length - index).astype(jnp.float32) / length
    response = jnp.exp(-2.0 * math.pi**2 * (length / breadth) ** 2 * folded * folded)
    product = index[:, None] * index[None, :] % length
    angles = 2.0 * math.pi / length * product.astype(jnp.float32)
    cosine = jnp.cos(angles)
    sine = jnp.sin(angles)
    even_part = jnp.dot(cosine * response[None, :], cosine.T, precision=highest)
    odd_part = jnp.dot(sine * response[None, :], sine.T, precision=highest)
    return (even_part + odd_part) / length


def neighbour_sum(belief):
    padded = extended(belief, (("slab", 1), ("row", 2), ("col", 3)), 1)
    total = padded[:, 2:, 1:-1, 1:-1] + padded[:, :-2, 1:-1, 1:-1]
    total = total + padded[:, 1:-1, 2:, 1:-1] + padded[:, 1:-1, :-2, 1:-1]
    total = total + padded[:, 1:-1, 1:-1, 2:] + padded[:, 1:-1, 1:-1, :-2]
    return total


def class_moments(belief, corrected):
    flat = belief.reshape(K, -1)
    values = corrected.reshape(M, -1)
    count, first, squares = lax.psum(
        (
            jnp.sum(flat, axis=1),
            jnp.dot(flat, values.T, precision=highest),
            jnp.dot(flat, (values * values).T, precision=highest),
        ),
        ("slab", "row", "col"),
    )
    means = first / (count + 1.0)[:, None]
    spread = squares - 2.0 * means * first + means * means * count[:, None]
    variance = (spread + 1.0) / (count + 1.0)[:, None]
    return (count, means, variance)


def log_density(corrected, means, variance, prior):
    offset = corrected[None] - means[:, :, None, None, None]
    terms = (
        offset * offset / variance[:, :, None, None, None]
        + jnp.log(variance)[:, :, None, None, None]
    )
    return jnp.log(prior)[:, None, None, None] - 0.5 * jnp.sum(terms, axis=1)


def smoothed(residual, column_local, row_table, slab_table):
    across = jnp.einsum(
        "msrc,cd->msrd",
        lax.all_gather(residual, "col", axis=3, tiled=True),
        column_local,
        precision=highest,
    )
    mixed = jnp.einsum(
        "msrc,rq->msqc",
        lax.all_to_all(across, "row", split_axis=1, concat_axis=2, tiled=True),
        row_table,
        precision=highest,
    )
    across = lax.all_to_all(mixed, "row", split_axis=2, concat_axis=1, tiled=True)
    mixed = jnp.einsum(
        "msrc,sq->mqrc",
        lax.all_to_all(across, "slab", split_axis=2, concat_axis=1, tiled=True),
        slab_table,
        precision=highest,
    )
    return lax.all_to_all(mixed, "slab", split_axis=1, concat_axis=2, tiled=True)


def general(image, brain_mask, labels):
    channels, slabs, rows, columns = image.shape
    inside = brain_mask.astype(jnp.float32)
    kinds = jnp.arange(K, dtype=jnp.int32)
    belief = (labels[None] == kinds[:, None, None, None]).astype(jnp.float32) * inside[None]
    column_table = circulant(columns * lax.axis_size("col"))
    column_local = lax.dynamic_slice_in_dim(
        column_table, lax.axis_index("col") * columns, columns, 1
    )
    row_table = circulant(rows * lax.axis_size("row"))
    slab_table = circulant(slabs * lax.axis_size("slab"))
    bias_field = jnp.zeros_like(image)
    means = jnp.zeros((K, channels), jnp.float32)
    for iteration in range(EM_ITERS):
        corrected = image - bias_field
        count, means, variance = class_moments(belief, corrected)
        prior = (count + 1.0) / (jnp.sum(count) + K)
        total = jnp.sum(belief, axis=0)
        removed = jnp.dot(means.T, belief.reshape(K, -1), precision=highest).reshape(image.shape)
        residual = image * total[None] - removed
        bias_field = smoothed(residual, column_local, row_table, slab_table)
        corrected = image - bias_field
        density = log_density(corrected, means, variance, prior)
        for sweep_index in range(MF_PASSES):
            belief = (
                jax.nn.softmax(density + coupling * neighbour_sum(belief), axis=0) * inside[None]
            )
    return (belief.astype(jnp.bfloat16), bias_field, means)


LANES = 128
SUB = 8
EDGE = 4
MARGIN = 8
FIELD = 4
STATS = 1 + 2 * M
VMEM_BYTES = 16 * 2**20


def impulse(length):
    index = np.arange(length)
    folded = np.minimum(index, length - index) / length
    response = np.exp(-2.0 * np.pi**2 * (length / breadth) ** 2 * folded * folded)
    angles = 2.0 * np.pi / length * (index[:, None] * index[None, :] % length)
    return np.cos(angles) @ response / length


def dense(length):
    index = np.arange(length)
    return impulse(length)[(index[:, None] - index[None, :]) % length]


def halves_of(x):
    high = x.astype(jnp.bfloat16)
    return high, (x - high.astype(jnp.float32)).astype(jnp.bfloat16)


def table_of(x):
    high = x.astype(jnp.bfloat16)
    low = (x - high.astype(np.float64)).astype(jnp.bfloat16)
    return np.stack([high, low])


def dot(left, right, dims=((1,), (0,))):
    left, right = (x if isinstance(x, tuple) else halves_of(x) for x in (left, right))

    def one(a, b):
        return lax.dot_general(a, b, (dims, ((), ())), preferred_element_type=jnp.float32)

    return one(left[0], right[0]) + (one(left[1], right[0]) + one(left[0], right[1]))


def wide(row, shape=(SUB, LANES)):
    return jnp.broadcast_to(row, shape)


def stat_row(sums):
    sub = lax.broadcasted_iota(jnp.int32, (SUB, LANES), 0)
    lane = lax.broadcasted_iota(jnp.int32, (SUB, LANES), 1)
    tile = jnp.zeros((SUB, LANES), jnp.float32)
    for q in range(STATS):
        rows = jnp.zeros((SUB, LANES), jnp.float32)
        for k in range(K):
            line = jnp.sum(sums[k][q], axis=0, keepdims=True)
            rows = jnp.where(sub == k, line, rows)
        tile = jnp.where(lane == q * K + sub, jnp.sum(rows, axis=1, keepdims=True), tile)
    return jnp.sum(tile, axis=0, keepdims=True)


def stat_columns(row, number):
    sub = lax.broadcasted_iota(jnp.int32, (SUB, LANES), 0)
    lane = lax.broadcasted_iota(jnp.int32, (SUB, LANES), 1)
    return [
        jnp.sum(jnp.where(lane == q * K + sub, row, 0.0), axis=1, keepdims=True)
        for q in range(number)
    ]


def fold(x):
    return jnp.sum(x.reshape(x.shape[0] // SUB, SUB, LANES), axis=0)


def class_stats(row):
    count, *rest = stat_columns(row, STATS)
    means, halves = [], []
    shift = jnp.zeros_like(count)
    for m in range(M):
        first, squares = rest[m], rest[M + m]
        mean = first / (count + 1.0)
        spread = squares - 2.0 * mean * first + mean * mean * count
        variance = (spread + 1.0) / (count + 1.0)
        means.append(wide(mean))
        halves.append(wide(0.5 / variance))
        shift = shift - 0.5 * jnp.log(variance)
    prior = (count + 1.0) / (jnp.sum(count, axis=0, keepdims=True) + K)
    return means, halves, wide(jnp.log(prior) + shift)


def mean_rows(row):
    count, *rest = stat_columns(row, 1 + M)
    return [wide(x / (count + 1.0)) for x in rest]


def log_terms(corrected, means, halves, shift):
    out = []
    for k in range(K):
        total = wide(shift[k : k + 1, :], corrected[0].shape)
        for m in range(M):
            offset = corrected[m] - means[m][k : k + 1, :]
            total = total - offset * offset * halves[m][k : k + 1, :]
        out.append(total)
    return out


def soft(logits, inside):
    top = functools.reduce(jnp.maximum, logits)
    exps = [jnp.exp(x - top) for x in logits]
    scale = inside / functools.reduce(jnp.add, exps)
    return [x * scale for x in exps]


def peer_sum(ref, line):
    row = ref[0, line : line + 1, :]
    for j in range(1, ref.shape[0]):
        row = row + ref[j, line : line + 1, :]
    return row


def class_sums(code, image):
    sums = []
    for k in range(K):
        flag = (code == float(k)).astype(jnp.float32)
        line = [fold(flag)]
        weighted = [flag * image[m] for m in range(M)]
        line += [fold(x) for x in weighted]
        line += [fold(x * image[m]) for m, x in enumerate(weighted)]
        sums.append(line)
    return sums


def own_kernel(own, turned, stat):
    stat[...] = wide(stat_row(class_sums(own[M], own)))
    for f in range(M + 1):
        turned[f] = own[f].T


def prepare_kernel(
    pack, turned, stat, image_o, mask_o, labels_o, send, rest, code_o, ext
):
    peers = send.shape[0]
    step = LANES // peers
    first = jnp.full((SUB, LANES), lax.axis_index("col"), jnp.int32) == 0
    code_o[...] = jnp.where(mask_o[...] > 0, labels_o[...], K).astype(jnp.float32)
    row = stat[0:1, :] + stat_row(class_sums(code_o[...], image_o))
    for f in range(M + 1):
        blank = jnp.full((SUB, LANES), float(K) if f == M else 0.0, jnp.float32)
        other = (image_o[f] if f < M else code_o[...]).T
        ext[f, 0:MARGIN, :] = jnp.where(first, blank, other[LANES - MARGIN :, :])
        ext[f, MARGIN : MARGIN + LANES, :] = turned[f]
        ext[f, MARGIN + LANES :, :] = jnp.where(first, other[:MARGIN, :], blank)
    for p in range(peers):
        at = MARGIN + step * p
        for m in range(M):
            send[p, pack.wide * m : pack.wide * (m + 1), :] = ext[m, at - 2 : at + step + 2, :]
        send[p, pack.code : pack.stat, :] = ext[M, at - 1 : at + step + 1, :]
        send[p, pack.stat : pack.stat + 1, :] = row
        rest[p, 0:2, :] = ext[M, at - 3 : at - 1, :]
        rest[p, 2:4, :] = ext[M, at + step + 1 : at + step + 3, :]


def column_kernel(pack, own, image_o, code_o, got, rest, table, send, flat, out):
    peers = send.shape[0]
    step = LANES // peers
    means = mean_rows(peer_sum(got, pack.stat))
    for h, (ref, code) in enumerate(((own, own[M]), (image_o, code_o[...]))):
        flags = [code == float(k) for k in range(K)]
        for m in range(M):
            center = jnp.zeros_like(code)
            for k in range(K):
                center = jnp.where(flags[k], means[m][k : k + 1, :], center)
            flat[m * LANES : (m + 1) * LANES, h * LANES : (h + 1) * LANES] = jnp.where(
                code < float(K), ref[m] - center, 0.0
            )
    out[...] = dot((table[0], table[1]), flat[...], ((1,), (1,)))
    for p in range(peers):
        at = MARGIN + step * p
        send[p, pack.code : pack.code + 4, :] = rest[p, 0:4, :]
        for m in range(M):
            send[p, pack.wide * m : pack.wide * (m + 1), :] = out[
                at - 2 : at + step + 2, m * LANES : (m + 1) * LANES
            ]


def slab_row_filter(rows, slab_table, row_table, first, second, grid):
    ns, nr = grid
    mixed = dot(first[...], (slab_table[0], slab_table[1]))
    for sb in range(ns):
        for rb in range(nr):
            second[sb * rows : (sb + 1) * rows, rb * LANES : (rb + 1) * LANES] = mixed[
                rb * rows : (rb + 1) * rows, sb * LANES : (sb + 1) * LANES
            ]
    return dot(second[...], (row_table[0], row_table[1]))


def around(get, sb, rb, grid, rows, fill):
    ns, nr = grid
    lane = lax.broadcasted_iota(jnp.int32, (1, LANES), 1)
    place = lane % rows
    here = get(sb, rb)
    empty = jnp.full_like(here, fill)
    above = get(sb + 1, rb) if sb + 1 < ns else empty
    below = get(sb - 1, rb) if sb > 0 else empty
    out = [
        pltpu.roll(jnp.where(lane >= rows, here, above), LANES - rows, 1),
        pltpu.roll(jnp.where(lane < LANES - rows, here, below), rows, 1),
    ]
    right = pltpu.roll(get(sb, rb + 1), rows - 1, 1) if rb + 1 < nr else empty
    left = pltpu.roll(get(sb, rb - 1), LANES - rows + 1, 1) if rb > 0 else empty
    out.append(jnp.where(place < rows - 1, pltpu.roll(here, LANES - 1, 1), right))
    out.append(jnp.where(place > 0, pltpu.roll(here, 1, 1), left))
    return out


def pencil_kernel(
    pack,
    grid,
    rows,
    got,
    raw,
    slab_table,
    row_table,
    send,
    keep,
    first,
    second,
    bias,
    codes,
    marks,
    shaded,
    dens,
    one,
    two,
):
    ns, nr = grid
    peers = ns * nr
    core = pack.core
    window = core + 2 * EDGE
    means, halves, shift = class_stats(peer_sum(raw, pack.stat))
    first[...] = jnp.zeros_like(first)
    for sb in range(ns):
        for rb in range(nr):
            for m in range(M):
                base = (rb * M + m) * window + EDGE - 2
                first[base : base + pack.wide, sb * LANES : (sb + 1) * LANES] = got[
                    rb * ns + sb, m * pack.wide : (m + 1) * pack.wide, :
                ]
    bias[...] = slab_row_filter(M * window, slab_table, row_table, first, second, grid)
    blank = jnp.full((window, LANES), float(K), jnp.float32)
    for sb in range(ns):
        for rb in range(nr):
            j = rb * ns + sb
            codes[j] = blank
            codes[j, EDGE - 3 : EDGE - 1, :] = got[j, pack.code : pack.code + 2, :]
            codes[j, EDGE - 1 : EDGE + core + 1, :] = raw[j, pack.code : pack.stat, :]
            codes[j, EDGE + core + 1 : EDGE + core + 3, :] = got[j, pack.code + 2 : pack.code + 4, :]
            for m in range(M):
                base = (sb * M + m) * window
                shaded[j, m] = -bias[base : base + window, rb * LANES : (rb + 1) * LANES]
                shaded[j, m, EDGE - 2 : EDGE - 2 + pack.wide, :] += raw[
                    j, m * pack.wide : (m + 1) * pack.wide, :
                ]

    def bits(x):
        whole = x.astype(jnp.int32)
        return jnp.where(whole < K, lax.shift_left(jnp.ones_like(whole), whole * FIELD), 0)

    for j in range(peers):
        marks[j] = bits(codes[j])

    for sb in range(ns):
        for rb in range(nr):
            j = rb * ns + sb
            logits = log_terms([shaded[j, m] for m in range(M)], means, halves, shift)
            code = codes[j]
            here = marks[j]
            near = around(lambda a, b: marks[b * ns + a], sb, rb, grid, rows, 0)
            near = near + [pltpu.roll(here, 1, 0), pltpu.roll(here, window - 1, 0)]
            near = functools.reduce(jnp.add, near)
            for k in range(K):
                dens[k, j] = logits[k]
                number = lax.shift_right_logical(near, jnp.full_like(near, k * FIELD))
                logits[k] = logits[k] + (number & (2**FIELD - 1)).astype(jnp.float32)
            inside = (code < float(K)).astype(jnp.float32)
            for k, value in enumerate(soft(logits, inside)):
                one[k, j] = value
    for sb in range(ns):
        for rb in range(nr):
            j = rb * ns + sb
            logits = []
            for k in range(K):
                here = one[k, j]
                near = around(lambda a, b: one[k, b * ns + a], sb, rb, grid, rows, 0.0)
                near = near + [pltpu.roll(here, 1, 0), pltpu.roll(here, window - 1, 0)]
                logits.append(dens[k, j] + functools.reduce(jnp.add, near))
            inside = (codes[j] < float(K)).astype(jnp.float32)
            for k, value in enumerate(soft(logits, inside)):
                two[k, j] = value
    for sb in range(ns):
        for rb in range(nr):
            j = rb * ns + sb
            totals = []
            for k in range(K):
                near = around(
                    lambda a, b: two[k, b * ns + a, EDGE : EDGE + core, :], sb, rb, grid, rows, 0.0
                )
                near = near + [
                    two[k, j, EDGE - 1 : EDGE - 1 + core, :],
                    two[k, j, EDGE + 1 : EDGE + 1 + core, :],
                ]
                totals.append(functools.reduce(jnp.add, near))
            for k in range(K - 1):
                send[j, k * core : (k + 1) * core, :] = totals[k] - totals[K - 1]
    sums = []
    for k in range(K):
        line = [jnp.zeros((SUB, LANES), jnp.float32) for _ in range(STATS)]
        for j in range(peers):
            here = two[k, j, EDGE : EDGE + core, :]
            keep[k, j] = here
            line[0] = line[0] + fold(here)
            for m in range(M):
                field = shaded[j, m, EDGE : EDGE + core, :]
                value = here * field
                line[1 + m] = line[1 + m] + fold(value)
                line[1 + M + m] = line[1 + M + m] + fold(value * field)
        sums.append([jnp.sum(x, axis=0, keepdims=True) for x in line])
    row = stat_row(sums)
    for p in range(peers):
        send[p, (K - 1) * core : (K - 1) * core + 1, :] = row


def residual_kernel(
    pack, grid, stat_a, stat_b, keep, raw, slab_table, row_table, send, first, second
):
    ns, nr = grid
    core = pack.core
    means = mean_rows(stat_a[...] + stat_b[...])
    for sb in range(ns):
        for rb in range(nr):
            j = rb * ns + sb
            for m in range(M):
                base = m * pack.wide + 2
                field = raw[j, base : base + core, :]
                total = jnp.zeros_like(field)
                for k in range(K):
                    total = total + keep[k, j] * (field - means[m][k : k + 1, :])
                base = (rb * M + m) * core
                first[base : base + core, sb * LANES : (sb + 1) * LANES] = total
    rows = M * core
    done = slab_row_filter(rows, slab_table, row_table, first, second, grid)
    for sb in range(ns):
        for rb in range(nr):
            send[rb * ns + sb] = done[sb * rows : (sb + 1) * rows, rb * LANES : (rb + 1) * LANES]


def columns_of(ref, m, core):
    return ref[:, m * core : (m + 1) * core, :].reshape(LANES, LANES).T


def half_kernel(got, near, table, field, around):
    core = got.shape[1] // M
    for m in range(M):
        field[m] = dot(columns_of(got, m, core), (table[0, :LANES, :], table[1, :LANES, :]))
    for k in range(K - 1):
        around[k] = columns_of(near, k, core)


def third_kernel(
    rows,
    field,
    got,
    near,
    own,
    stat_a,
    stat_b,
    table,
    place,
    bias,
    centers,
    dens,
    belief,
    up,
    down,
    side,
    edge,
):
    core = got.shape[1] // M
    slabs = LANES // rows
    means, halves, shift = class_stats(stat_a[...] + stat_b[...])
    for m in range(M):
        centers[:, m : m + 1] = means[m][:, :1]
        bias[m] = field[m] + dot(
            columns_of(got, m, core), (table[0, LANES:, :], table[1, LANES:, :])
        )
    lane = lax.broadcasted_iota(jnp.int32, (1, LANES), 1)
    even = place[0, 0:1, :] == 0
    shiftback = jnp.where(place[2, 0:1, :] == 0, 1, 0)
    marks = [(lane + shiftback) % LANES == k for k in range(K - 1)]
    for s in range(slabs):
        low, high = s * rows, (s + 1) * rows
        corrected = [own[m, low:high, :] - bias[m, low:high, :] for m in range(M)]
        logits = log_terms(corrected, means, halves, shift)
        for k in range(K):
            dens[k, low:high, :] = logits[k]
            if k < K - 1:
                logits[k] = logits[k] + near[k, low:high, :]
        inside = (own[M, low:high, :] < float(K)).astype(jnp.float32)
        column = jnp.zeros((rows, LANES), jnp.float32)
        shares = soft(logits, inside)
        for k in range(K - 1):
            value = shares[k] - shares[K - 1]
            belief[k, low:high, :] = value
            column = jnp.where(marks[k], pltpu.roll(value, k, 1), column)
        edge[low:high, :] = column
    for k in range(K - 1):
        first = belief[k, :rows, :]
        final = belief[k, LANES - rows :, :]
        up[k] = jnp.where(even, final, first)
        down[k] = jnp.where(even, first, final)
    lead = place[1, 0:1, :] == 0
    for k in range(K - 1):
        head = belief[k, pl.ds(0, slabs, rows), :]
        tail = belief[k, pl.ds(rows - 1, slabs, rows), :]
        side[k] = jnp.where(lead, tail, head)


def inner_kernel(rows, dens, belief, bias, logits, bias_h, sems):
    copy = pltpu.make_async_copy(bias, bias_h, sems.at[0])
    copy.start()
    lane = lax.broadcasted_iota(jnp.int32, (1, LANES), 1)
    line = lax.broadcasted_iota(jnp.int32, (rows, 1), 0)
    for k in range(K - 1):
        for low in range(0, LANES, rows):
            here = belief[k, low : low + rows, :]
            total = dens[k, low : low + rows, :]
            if low > 0:
                total = total + belief[k, low - rows : low, :]
            if low + rows < LANES:
                total = total + belief[k, low + rows : low + 2 * rows, :]
            total = total + jnp.where(line > 0, pltpu.roll(here, 1, 0), 0.0)
            total = total + jnp.where(line < rows - 1, pltpu.roll(here, rows - 1, 0), 0.0)
            total = total + jnp.where(lane > 0, pltpu.roll(here, 1, 1), 0.0)
            total = total + jnp.where(lane < LANES - 1, pltpu.roll(here, LANES - 1, 1), 0.0)
            logits[k, low : low + rows, :] = total
    copy.wait()


def last_kernel(rows, inner, dens, own, up, down, side, edge, place, post_h, post, sems):
    slabs = LANES // rows
    lane = lax.broadcasted_iota(jnp.int32, (1, LANES), 1)
    line = lax.broadcasted_iota(jnp.int32, (rows, 1), 0)
    even = place[0, 0:1, :] == 0
    left = place[2, 0:1, :] == 0
    bottom = place[3, 0:1, :] == 0
    top = place[4, 0:1, :] == 0
    spot = lane == jnp.where(left, LANES - 1, 0)
    face = line == jnp.where(place[1, 0:1, :] == 0, rows - 1, 0)
    copies = []
    for s in range(slabs):
        low, high = s * rows, (s + 1) * rows
        column = edge[low:high, :]
        column = jnp.where(left, column, pltpu.roll(column, 2, 1))
        logits = []
        for k in range(K - 1):
            total = inner[k, low:high, :]
            if s == 0:
                total = total + jnp.where(bottom, 0.0, jnp.where(even, down[k], up[k]))
            if s == slabs - 1:
                total = total + jnp.where(top, 0.0, jnp.where(even, up[k], down[k]))
            total = total + jnp.where(face, side[k, s : s + 1, :], 0.0)
            total = total + jnp.where(spot, pltpu.roll(column, LANES - 1 - k, 1), 0.0)
            logits.append(total)
        logits.append(dens[K - 1, low:high, :])
        inside = (own[M, low:high, :] < float(K)).astype(jnp.float32)
        for k, value in enumerate(soft(logits, inside)):
            post[k, low:high, :] = value.astype(jnp.bfloat16)
        span = pl.ds(low, rows)
        copies.append(
            pltpu.make_async_copy(post.at[:, span, :], post_h.at[:, span, :], sems.at[s])
        )
        copies[-1].start()
    for copy in copies:
        copy.wait()


class Pack(typing.NamedTuple):
    core: int
    wide: int
    code: int
    stat: int


def padded(rows):
    return -(-rows // SUB) * SUB


def call(kernel, outs, scratch=(), micros=1, far_out=()):
    vmem = pl.BlockSpec(memory_space=pltpu.VMEM)
    far = pl.BlockSpec(memory_space=pltpu.HBM)
    shapes = [jax.ShapeDtypeStruct(shape, kind) for shape, kind in outs]

    def run(*args):
        return pl.pallas_call(
            kernel,
            out_shape=shapes,
            in_specs=[vmem] * len(args),
            out_specs=[far if i in far_out else vmem for i in range(len(shapes))],
            scratch_shapes=[
                pltpu.VMEM(x, jnp.float32) if isinstance(x, tuple) else x for x in scratch
            ],
            compiler_params=pltpu.CompilerParams(vmem_limit_bytes=VMEM_BYTES),
            cost_estimate=pl.CostEstimate(
                flops=micros * 10_000_000, bytes_accessed=2**20, transcendentals=0
            ),
            name=(kernel.func if isinstance(kernel, functools.partial) else kernel).__name__,
        )(*args)

    return run


def both_ways(pairs, count):
    steps = []
    for i in range(count):
        other = [b if a == i else a for a, b in pairs if i in (a, b)]
        for side in range(2):
            target = other[0] * 2 + side if other else i * 2 + 1 - side
            steps.append((i * 2 + side, target))
    return steps


def pencils(image, brain_mask, labels):
    _, slabs, rows, columns = image.shape
    ns, nr, nc = (lax.axis_size(a) for a in ("slab", "row", "col"))
    grid = (ns, nr)
    peers = ns * nr
    core = columns // peers
    window = core + 2 * EDGE
    wide_rows = core + 4
    pack = Pack(core, wide_rows, M * wide_rows, M * wide_rows + core + 2)
    f32 = jnp.float32
    slab = lax.axis_index("slab")
    place = [slab % 2, lax.axis_index("row"), lax.axis_index("col"), slab, ns - 1 - slab]
    place = jnp.broadcast_to(jnp.stack(place).astype(jnp.int32)[:, None, None], (5, SUB, LANES))
    swap = [(0, 1), (1, 0)]

    taps = impulse(columns * nc)
    reach = np.arange(-MARGIN, columns + MARGIN)
    source = np.concatenate([np.arange(columns), np.arange(columns) + columns])
    spread = taps[(reach[:, None] - source[None, :]) % (columns * nc)]
    gather = table_of(spread[MARGIN : MARGIN + columns].T)
    spread = table_of(spread)
    slab_table = table_of(np.kron(dense(slabs * ns), np.eye(rows)))
    row_table = np.einsum(
        "arbq,st->asrbtq", dense(rows * nr).reshape(nr, rows, nr, rows), np.eye(slabs)
    )
    row_table = table_of(row_table.reshape(nr * LANES, nr * LANES))

    code = jnp.where(brain_mask > 0, labels, K).astype(f32)
    own = jnp.concatenate([image, code[None]]).reshape(M + 1, LANES, columns)
    image_o = lax.ppermute(image.reshape(M, LANES, columns), "col", swap)
    mask_o = lax.ppermute(brain_mask.reshape(LANES, columns), "col", swap)
    labels_o = lax.ppermute(labels.reshape(LANES, columns), "col", swap)

    def trade(x):
        return lax.all_to_all(x, ("row", "slab"), split_axis=0, concat_axis=0, tiled=True)

    turned, stat = call(
        own_kernel, [((M + 1, columns, LANES), f32), ((SUB, LANES), f32)]
    )(own)
    sent, rest, code_o = call(
        functools.partial(prepare_kernel, pack),
        [
            ((peers, padded(pack.stat + 1), LANES), f32),
            ((peers, SUB, LANES), f32),
            ((LANES, columns), f32),
        ],
        [(M + 1, columns + 2 * MARGIN, LANES)],
    )(turned, stat, image_o, mask_o, labels_o)
    raw = trade(sent)
    (sent,) = call(
        functools.partial(column_kernel, pack),
        [((peers, padded(pack.code + 4), LANES), f32)],
        [(M * LANES, 2 * columns), (columns + 2 * MARGIN, M * LANES)],
    )(own, image_o, code_o, raw, rest, spread)
    got = trade(sent)
    sent, keep = call(
        functools.partial(pencil_kernel, pack, grid, rows),
        [
            ((peers, padded((K - 1) * core + 1), LANES), f32),
            ((K, peers, core, LANES), f32),
        ],
        [
            (nr * M * window, ns * LANES),
            (ns * M * window, nr * LANES),
            (ns * M * window, nr * LANES),
            (peers, window, LANES),
            pltpu.VMEM((peers, window, LANES), jnp.int32),
            (peers, M, window, LANES),
            (K, peers, window, LANES),
            (K, peers, window, LANES),
            (K, peers, window, LANES),
        ],
        micros=4,
    )(got, raw, slab_table, row_table)
    near = trade(sent)
    stat_a = jnp.sum(near[:, (K - 1) * core : (K - 1) * core + 1, :], axis=0)
    stat_b = lax.ppermute(stat_a, "col", swap)
    (sent,) = call(
        functools.partial(residual_kernel, pack, grid),
        [((peers, M * core, LANES), f32)],
        [(nr * M * core, ns * LANES), (ns * M * core, nr * LANES)],
    )(stat_a, stat_b, keep, raw, slab_table, row_table)
    got = trade(sent)
    yours = lax.ppermute(got, "col", swap)
    field, near = call(
        half_kernel, [((M, LANES, columns), f32), ((K - 1, LANES, columns), f32)]
    )(got, near, gather)
    bias, centers, dens, belief, up, down, side, edge = call(
        functools.partial(third_kernel, rows),
        [
            ((M, LANES, columns), f32),
            ((K, M), f32),
            ((K, LANES, columns), f32),
            ((K - 1, LANES, columns), f32),
            ((K - 1, rows, columns), f32),
            ((K - 1, rows, columns), f32),
            ((K - 1, slabs, columns), f32),
            ((LANES, LANES), f32),
        ],
        micros=2,
    )(field, yours, near, own, stat_a, stat_b, gather, place)
    pairs = [(i, i + 1) for i in range(0, ns - 1, 2)]
    between = [(i, i + 1) for i in range(1, ns - 1, 2)]
    up = lax.ppermute(up, ("slab", "col"), both_ways(pairs, ns))
    down = lax.ppermute(down, ("slab", "col"), both_ways(between, ns))
    side = lax.ppermute(side, "row", swap)
    edge = lax.ppermute(edge, "col", swap)
    inner, bias = call(
        functools.partial(inner_kernel, rows),
        [((K - 1, LANES, columns), f32), ((M, LANES, columns), f32)],
        [pltpu.SemaphoreType.DMA((1,))],
        far_out=(1,),
    )(dens, belief, bias)
    (post,) = call(
        functools.partial(last_kernel, rows),
        [((K, LANES, columns), jnp.bfloat16)],
        [
            pltpu.VMEM((K, LANES, columns), jnp.bfloat16),
            pltpu.SemaphoreType.DMA((slabs,)),
        ],
        far_out=(0,),
    )(inner, dens, own, up, down, side, edge, place)
    shape = (slabs, rows, columns)
    return post.reshape((K,) + shape), bias.reshape((M,) + shape), centers


def local(image, brain_mask, labels):
    _, slabs, rows, columns = image.shape
    peers = lax.axis_size("slab") * lax.axis_size("row")
    fits = slabs * rows == LANES and columns == LANES and slabs % SUB == 0 and rows % SUB == 0
    fits = fits and lax.axis_size("row") == 2 and lax.axis_size("col") == 2
    fits = fits and columns % (SUB * peers) == 0
    return (pencils if fits else general)(image, brain_mask, labels)


def solution(mesh):
    placed = (
        P(None, ("grp", "slab"), "row", "col"),
        P(("grp", "slab"), "row", "col"),
        P(("grp", "slab"), "row", "col"),
    )
    return jax.shard_map(
        local,
        mesh=mesh,
        in_specs=placed,
        out_specs=(
            P(None, ("grp", "slab"), "row", "col"),
            P(None, ("grp", "slab"), "row", "col"),
            P("grp", None),
        ),
        check_vma=False,
    )
```

```python
import functools
import math
import typing

import jax
import jax.numpy as jnp
import numpy as np
from jax import lax
from jax.experimental import pallas as pl
from jax.experimental.pallas import tpu as pltpu
from jax.sharding import PartitionSpec as P

M = 3
K = 8
EM_ITERS = 2
MF_PASSES = 2


highest = lax.Precision.HIGHEST
coupling = 1.0
breadth = 8.0


def extended(cells, sides, width):
    for axis, dim in sides:
        count = lax.axis_size(axis)
        ends = count - 1
        head = lax.slice_in_dim(cells, 0, width, axis=dim)
        tail = lax.slice_in_dim(cells, cells.shape[dim] - width, cells.shape[dim], axis=dim)
        cells = jnp.concatenate(
            [
                lax.ppermute(tail, axis, [(i, (i + 1) % count) for i in range(ends)]),
                cells,
                lax.ppermute(head, axis, [((i + 1) % count, i) for i in range(ends)]),
            ],
            axis=dim,
        )
    return cells


def circulant(length):
    index = jnp.arange(length, dtype=jnp.int32)
    folded = jnp.minimum(index, length - index).astype(jnp.float32) / length
    response = jnp.exp(-2.0 * math.pi**2 * (length / breadth) ** 2 * folded * folded)
    product = index[:, None] * index[None, :] % length
    angles = 2.0 * math.pi / length * product.astype(jnp.float32)
    cosine = jnp.cos(angles)
    sine = jnp.sin(angles)
    even_part = jnp.dot(cosine * response[None, :], cosine.T, precision=highest)
    odd_part = jnp.dot(sine * response[None, :], sine.T, precision=highest)
    return (even_part + odd_part) / length


def neighbour_sum(belief):
    padded = extended(belief, (("slab", 1), ("row", 2), ("col", 3)), 1)
    total = padded[:, 2:, 1:-1, 1:-1] + padded[:, :-2, 1:-1, 1:-1]
    total = total + padded[:, 1:-1, 2:, 1:-1] + padded[:, 1:-1, :-2, 1:-1]
    total = total + padded[:, 1:-1, 1:-1, 2:] + padded[:, 1:-1, 1:-1, :-2]
    return total


def class_moments(belief, corrected):
    flat = belief.reshape(K, -1)
    values = corrected.reshape(M, -1)
    count, first, squares = lax.psum(
        (
            jnp.sum(flat, axis=1),
            jnp.dot(flat, values.T, precision=highest),
            jnp.dot(flat, (values * values).T, precision=highest),
        ),
        ("slab", "row", "col"),
    )
    means = first / (count + 1.0)[:, None]
    spread = squares - 2.0 * means * first + means * means * count[:, None]
    variance = (spread + 1.0) / (count + 1.0)[:, None]
    return (count, means, variance)


def log_density(corrected, means, variance, prior):
    offset = corrected[None] - means[:, :, None, None, None]
    terms = (
        offset * offset / variance[:, :, None, None, None]
        + jnp.log(variance)[:, :, None, None, None]
    )
    return jnp.log(prior)[:, None, None, None] - 0.5 * jnp.sum(terms, axis=1)


def smoothed(residual, column_local, row_table, slab_table):
    across = jnp.einsum(
        "msrc,cd->msrd",
        lax.all_gather(residual, "col", axis=3, tiled=True),
        column_local,
        precision=highest,
    )
    mixed = jnp.einsum(
        "msrc,rq->msqc",
        lax.all_to_all(across, "row", split_axis=1, concat_axis=2, tiled=True),
        row_table,
        precision=highest,
    )
    across = lax.all_to_all(mixed, "row", split_axis=2, concat_axis=1, tiled=True)
    mixed = jnp.einsum(
        "msrc,sq->mqrc",
        lax.all_to_all(across, "slab", split_axis=2, concat_axis=1, tiled=True),
        slab_table,
        precision=highest,
    )
    return lax.all_to_all(mixed, "slab", split_axis=1, concat_axis=2, tiled=True)


def general(image, brain_mask, labels):
    channels, slabs, rows, columns = image.shape
    inside = brain_mask.astype(jnp.float32)
    kinds = jnp.arange(K, dtype=jnp.int32)
    belief = (labels[None] == kinds[:, None, None, None]).astype(jnp.float32) * inside[None]
    column_table = circulant(columns * lax.axis_size("col"))
    column_local = lax.dynamic_slice_in_dim(
        column_table, lax.axis_index("col") * columns, columns, 1
    )
    row_table = circulant(rows * lax.axis_size("row"))
    slab_table = circulant(slabs * lax.axis_size("slab"))
    bias_field = jnp.zeros_like(image)
    means = jnp.zeros((K, channels), jnp.float32)
    for iteration in range(EM_ITERS):
        corrected = image - bias_field
        count, means, variance = class_moments(belief, corrected)
        prior = (count + 1.0) / (jnp.sum(count) + K)
        total = jnp.sum(belief, axis=0)
        removed = jnp.dot(means.T, belief.reshape(K, -1), precision=highest).reshape(image.shape)
        residual = image * total[None] - removed
        bias_field = smoothed(residual, column_local, row_table, slab_table)
        corrected = image - bias_field
        density = log_density(corrected, means, variance, prior)
        for sweep_index in range(MF_PASSES):
            belief = (
                jax.nn.softmax(density + coupling * neighbour_sum(belief), axis=0) * inside[None]
            )
    return (belief.astype(jnp.bfloat16), bias_field, means)


LANES = 128
SUB = 8
EDGE = 4
MARGIN = 8
FIELD = 4
STATS = 1 + 2 * M
VMEM_BYTES = 16 * 2**20


def impulse(length):
    index = np.arange(length)
    folded = np.minimum(index, length - index) / length
    response = np.exp(-2.0 * np.pi**2 * (length / breadth) ** 2 * folded * folded)
    angles = 2.0 * np.pi / length * (index[:, None] * index[None, :] % length)
    return np.cos(angles) @ response / length


def dense(length):
    index = np.arange(length)
    return impulse(length)[(index[:, None] - index[None, :]) % length]


def halves_of(x):
    high = x.astype(jnp.bfloat16)
    return high, (x - high.astype(jnp.float32)).astype(jnp.bfloat16)


def table_of(x):
    high = x.astype(jnp.bfloat16)
    low = (x - high.astype(np.float64)).astype(jnp.bfloat16)
    return np.stack([high, low])


def dot(left, right, dims=((1,), (0,))):
    left, right = (x if isinstance(x, tuple) else halves_of(x) for x in (left, right))

    def one(a, b):
        return lax.dot_general(a, b, (dims, ((), ())), preferred_element_type=jnp.float32)

    return one(left[0], right[0]) + (one(left[1], right[0]) + one(left[0], right[1]))


def wide(row, shape=(SUB, LANES)):
    return jnp.broadcast_to(row, shape)


def stat_row(sums):
    sub = lax.broadcasted_iota(jnp.int32, (SUB, LANES), 0)
    lane = lax.broadcasted_iota(jnp.int32, (SUB, LANES), 1)
    tile = jnp.zeros((SUB, LANES), jnp.float32)
    for q in range(STATS):
        rows = jnp.zeros((SUB, LANES), jnp.float32)
        for k in range(K):
            line = jnp.sum(sums[k][q], axis=0, keepdims=True)
            rows = jnp.where(sub == k, line, rows)
        tile = jnp.where(lane == q * K + sub, jnp.sum(rows, axis=1, keepdims=True), tile)
    return jnp.sum(tile, axis=0, keepdims=True)


def stat_columns(row, number):
    sub = lax.broadcasted_iota(jnp.int32, (SUB, LANES), 0)
    lane = lax.broadcasted_iota(jnp.int32, (SUB, LANES), 1)
    return [
        jnp.sum(jnp.where(lane == q * K + sub, row, 0.0), axis=1, keepdims=True)
        for q in range(number)
    ]


def fold(x):
    return jnp.sum(x.reshape(x.shape[0] // SUB, SUB, LANES), axis=0)


def class_stats(row):
    count, *rest = stat_columns(row, STATS)
    means, halves = [], []
    shift = jnp.zeros_like(count)
    for m in range(M):
        first, squares = rest[m], rest[M + m]
        mean = first / (count + 1.0)
        spread = squares - 2.0 * mean * first + mean * mean * count
        variance = (spread + 1.0) / (count + 1.0)
        means.append(wide(mean))
        halves.append(wide(0.5 / variance))
        shift = shift - 0.5 * jnp.log(variance)
    prior = (count + 1.0) / (jnp.sum(count, axis=0, keepdims=True) + K)
    return means, halves, wide(jnp.log(prior) + shift)


def mean_rows(row):
    count, *rest = stat_columns(row, 1 + M)
    return [wide(x / (count + 1.0)) for x in rest]


def log_terms(corrected, means, halves, shift):
    out = []
    for k in range(K):
        total = wide(shift[k : k + 1, :], corrected[0].shape)
        for m in range(M):
            offset = corrected[m] - means[m][k : k + 1, :]
            total = total - offset * offset * halves[m][k : k + 1, :]
        out.append(total)
    return out


def soft(logits, inside):
    top = functools.reduce(jnp.maximum, logits)
    exps = [jnp.exp(x - top) for x in logits]
    scale = inside / functools.reduce(jnp.add, exps)
    return [x * scale for x in exps]


def peer_sum(ref, line):
    row = ref[0, line : line + 1, :]
    for j in range(1, ref.shape[0]):
        row = row + ref[j, line : line + 1, :]
    return row


def class_sums(code, image):
    sums = []
    for k in range(K):
        flag = (code == float(k)).astype(jnp.float32)
        line = [fold(flag)]
        weighted = [flag * image[m] for m in range(M)]
        line += [fold(x) for x in weighted]
        line += [fold(x * image[m]) for m, x in enumerate(weighted)]
        sums.append(line)
    return sums


def own_kernel(own, turned, stat):
    stat[...] = wide(stat_row(class_sums(own[M], own)))
    for f in range(M + 1):
        turned[f] = own[f].T


def prepare_kernel(
    pack, turned, stat, image_o, mask_o, labels_o, send, rest, code_o, ext
):
    peers = send.shape[0]
    step = LANES // peers
    first = jnp.full((SUB, LANES), lax.axis_index("col"), jnp.int32) == 0
    code_o[...] = jnp.where(mask_o[...] > 0, labels_o[...], K).astype(jnp.float32)
    row = stat[0:1, :] + stat_row(class_sums(code_o[...], image_o))
    for f in range(M + 1):
        blank = jnp.full((SUB, LANES), float(K) if f == M else 0.0, jnp.float32)
        other = (image_o[f] if f < M else code_o[...]).T
        ext[f, 0:MARGIN, :] = jnp.where(first, blank, other[LANES - MARGIN :, :])
        ext[f, MARGIN : MARGIN + LANES, :] = turned[f]
        ext[f, MARGIN + LANES :, :] = jnp.where(first, other[:MARGIN, :], blank)
    for p in range(peers):
        at = MARGIN + step * p
        for m in range(M):
            send[p, pack.wide * m : pack.wide * (m + 1), :] = ext[m, at - 2 : at + step + 2, :]
        send[p, pack.code : pack.stat, :] = ext[M, at - 1 : at + step + 1, :]
        send[p, pack.stat : pack.stat + 1, :] = row
        rest[p, 0:2, :] = ext[M, at - 3 : at - 1, :]
        rest[p, 2:4, :] = ext[M, at + step + 1 : at + step + 3, :]


def column_kernel(pack, own, image_o, code_o, got, rest, table, send, flat, out):
    peers = send.shape[0]
    step = LANES // peers
    means = mean_rows(peer_sum(got, pack.stat))
    for h, (ref, code) in enumerate(((own, own[M]), (image_o, code_o[...]))):
        flags = [code == float(k) for k in range(K)]
        for m in range(M):
            center = jnp.zeros_like(code)
            for k in range(K):
                center = jnp.where(flags[k], means[m][k : k + 1, :], center)
            flat[m * LANES : (m + 1) * LANES, h * LANES : (h + 1) * LANES] = jnp.where(
                code < float(K), ref[m] - center, 0.0
            )
    out[...] = dot((table[0], table[1]), flat[...], ((1,), (1,)))
    for p in range(peers):
        at = MARGIN + step * p
        send[p, pack.code : pack.code + 4, :] = rest[p, 0:4, :]
        for m in range(M):
            send[p, pack.wide * m : pack.wide * (m + 1), :] = out[
                at - 2 : at + step + 2, m * LANES : (m + 1) * LANES
            ]


def slab_row_filter(rows, slab_table, row_table, first, second, grid):
    ns, nr = grid
    mixed = dot(first[...], (slab_table[0], slab_table[1]))
    for sb in range(ns):
        for rb in range(nr):
            second[sb * rows : (sb + 1) * rows, rb * LANES : (rb + 1) * LANES] = mixed[
                rb * rows : (rb + 1) * rows, sb * LANES : (sb + 1) * LANES
            ]
    return dot(second[...], (row_table[0], row_table[1]))


def around(get, sb, rb, grid, rows, fill):
    ns, nr = grid
    lane = lax.broadcasted_iota(jnp.int32, (1, LANES), 1)
    place = lane % rows
    here = get(sb, rb)
    empty = jnp.full_like(here, fill)
    above = get(sb + 1, rb) if sb + 1 < ns else empty
    below = get(sb - 1, rb) if sb > 0 else empty
    out = [
        pltpu.roll(jnp.where(lane >= rows, here, above), LANES - rows, 1),
        pltpu.roll(jnp.where(lane < LANES - rows, here, below), rows, 1),
    ]
    right = pltpu.roll(get(sb, rb + 1), rows - 1, 1) if rb + 1 < nr else empty
    left = pltpu.roll(get(sb, rb - 1), LANES - rows + 1, 1) if rb > 0 else empty
    out.append(jnp.where(place < rows - 1, pltpu.roll(here, LANES - 1, 1), right))
    out.append(jnp.where(place > 0, pltpu.roll(here, 1, 1), left))
    return out


def pencil_kernel(
    pack,
    grid,
    rows,
    got,
    raw,
    slab_table,
    row_table,
    send,
    keep,
    first,
    second,
    bias,
    codes,
    marks,
    shaded,
    dens,
    one,
    two,
):
    ns, nr = grid
    peers = ns * nr
    core = pack.core
    window = core + 2 * EDGE
    means, halves, shift = class_stats(peer_sum(raw, pack.stat))
    first[...] = jnp.zeros_like(first)
    for sb in range(ns):
        for rb in range(nr):
            for m in range(M):
                base = (rb * M + m) * window + EDGE - 2
                first[base : base + pack.wide, sb * LANES : (sb + 1) * LANES] = got[
                    rb * ns + sb, m * pack.wide : (m + 1) * pack.wide, :
                ]
    bias[...] = slab_row_filter(M * window, slab_table, row_table, first, second, grid)
    blank = jnp.full((window, LANES), float(K), jnp.float32)
    for sb in range(ns):
        for rb in range(nr):
            j = rb * ns + sb
            codes[j] = blank
            codes[j, EDGE - 3 : EDGE - 1, :] = got[j, pack.code : pack.code + 2, :]
            codes[j, EDGE - 1 : EDGE + core + 1, :] = raw[j, pack.code : pack.stat, :]
            codes[j, EDGE + core + 1 : EDGE + core + 3, :] = got[j, pack.code + 2 : pack.code + 4, :]
            for m in range(M):
                base = (sb * M + m) * window
                shaded[j, m] = -bias[base : base + window, rb * LANES : (rb + 1) * LANES]
                shaded[j, m, EDGE - 2 : EDGE - 2 + pack.wide, :] += raw[
                    j, m * pack.wide : (m + 1) * pack.wide, :
                ]

    def bits(x):
        whole = x.astype(jnp.int32)
        return jnp.where(whole < K, lax.shift_left(jnp.ones_like(whole), whole * FIELD), 0)

    for j in range(peers):
        marks[j] = bits(codes[j])

    for sb in range(ns):
        for rb in range(nr):
            j = rb * ns + sb
            logits = log_terms([shaded[j, m] for m in range(M)], means, halves, shift)
            code = codes[j]
            here = marks[j]
            near = around(lambda a, b: marks[b * ns + a], sb, rb, grid, rows, 0)
            near = near + [pltpu.roll(here, 1, 0), pltpu.roll(here, window - 1, 0)]
            near = functools.reduce(jnp.add, near)
            for k in range(K):
                dens[k, j] = logits[k]
                number = lax.shift_right_logical(near, jnp.full_like(near, k * FIELD))
                logits[k] = logits[k] + (number & (2**FIELD - 1)).astype(jnp.float32)
            inside = (code < float(K)).astype(jnp.float32)
            for k, value in enumerate(soft(logits, inside)):
                one[k, j] = value
    for sb in range(ns):
        for rb in range(nr):
            j = rb * ns + sb
            logits = []
            for k in range(K):
                here = one[k, j]
                near = around(lambda a, b: one[k, b * ns + a], sb, rb, grid, rows, 0.0)
                near = near + [pltpu.roll(here, 1, 0), pltpu.roll(here, window - 1, 0)]
                logits.append(dens[k, j] + functools.reduce(jnp.add, near))
            inside = (codes[j] < float(K)).astype(jnp.float32)
            for k, value in enumerate(soft(logits, inside)):
                two[k, j] = value
    for sb in range(ns):
        for rb in range(nr):
            j = rb * ns + sb
            totals = []
            for k in range(K):
                near = around(
                    lambda a, b: two[k, b * ns + a, EDGE : EDGE + core, :], sb, rb, grid, rows, 0.0
                )
                near = near + [
                    two[k, j, EDGE - 1 : EDGE - 1 + core, :],
                    two[k, j, EDGE + 1 : EDGE + 1 + core, :],
                ]
                totals.append(functools.reduce(jnp.add, near))
            for k in range(K - 1):
                send[j, k * core : (k + 1) * core, :] = totals[k] - totals[K - 1]
    sums = []
    for k in range(K):
        line = [jnp.zeros((SUB, LANES), jnp.float32) for _ in range(STATS)]
        for j in range(peers):
            here = two[k, j, EDGE : EDGE + core, :]
            keep[k, j] = here
            line[0] = line[0] + fold(here)
            for m in range(M):
                field = shaded[j, m, EDGE : EDGE + core, :]
                value = here * field
                line[1 + m] = line[1 + m] + fold(value)
                line[1 + M + m] = line[1 + M + m] + fold(value * field)
        sums.append([jnp.sum(x, axis=0, keepdims=True) for x in line])
    row = stat_row(sums)
    for p in range(peers):
        send[p, (K - 1) * core : (K - 1) * core + 1, :] = row


def residual_kernel(
    pack, grid, stat_a, stat_b, keep, raw, slab_table, row_table, send, first, second
):
    ns, nr = grid
    core = pack.core
    means = mean_rows(stat_a[...] + stat_b[...])
    for sb in range(ns):
        for rb in range(nr):
            j = rb * ns + sb
            for m in range(M):
                base = m * pack.wide + 2
                field = raw[j, base : base + core, :]
                total = jnp.zeros_like(field)
                for k in range(K):
                    total = total + keep[k, j] * (field - means[m][k : k + 1, :])
                base = (rb * M + m) * core
                first[base : base + core, sb * LANES : (sb + 1) * LANES] = total
    rows = M * core
    done = slab_row_filter(rows, slab_table, row_table, first, second, grid)
    for sb in range(ns):
        for rb in range(nr):
            send[rb * ns + sb] = done[sb * rows : (sb + 1) * rows, rb * LANES : (rb + 1) * LANES]


def columns_of(ref, m, core):
    return ref[:, m * core : (m + 1) * core, :].reshape(LANES, LANES).T


def half_kernel(got, near, table, field, around):
    core = got.shape[1] // M
    for m in range(M):
        field[m] = dot(columns_of(got, m, core), (table[0, :LANES, :], table[1, :LANES, :]))
    for k in range(K - 1):
        around[k] = columns_of(near, k, core)


def third_kernel(
    rows,
    field,
    got,
    near,
    own,
    stat_a,
    stat_b,
    table,
    bias,
    centers,
    dens,
    belief,
    up,
    down,
    side,
    edge,
):
    core = got.shape[1] // M
    slabs = LANES // rows
    means, halves, shift = class_stats(stat_a[...] + stat_b[...])
    for m in range(M):
        centers[:, m : m + 1] = means[m][:, :1]
        bias[m] = field[m] + dot(
            columns_of(got, m, core), (table[0, LANES:, :], table[1, LANES:, :])
        )
    lane = lax.broadcasted_iota(jnp.int32, (1, LANES), 1)
    even = lanes_of(lax.rem(lax.axis_index("slab"), 2)) == 0
    shiftback = jnp.where(lanes_of(lax.axis_index("col")) == 0, 1, 0)
    marks = [(lane + shiftback) % LANES == k for k in range(K - 1)]
    for s in range(slabs):
        low, high = s * rows, (s + 1) * rows
        corrected = [own[m, low:high, :] - bias[m, low:high, :] for m in range(M)]
        logits = log_terms(corrected, means, halves, shift)
        for k in range(K):
            dens[k, low:high, :] = logits[k]
            if k < K - 1:
                logits[k] = logits[k] + near[k, low:high, :]
        inside = (own[M, low:high, :] < float(K)).astype(jnp.float32)
        column = jnp.zeros((rows, LANES), jnp.float32)
        shares = soft(logits, inside)
        for k in range(K - 1):
            value = shares[k] - shares[K - 1]
            belief[k, low:high, :] = value
            column = jnp.where(marks[k], pltpu.roll(value, k, 1), column)
        edge[low:high, :] = column
    for k in range(K - 1):
        first = belief[k, :rows, :]
        final = belief[k, LANES - rows :, :]
        up[k] = jnp.where(even, final, first)
        down[k] = jnp.where(even, first, final)
    lead = lanes_of(lax.axis_index("row")) == 0
    for k in range(K - 1):
        head = belief[k, pl.ds(0, slabs, rows), :]
        tail = belief[k, pl.ds(rows - 1, slabs, rows), :]
        side[k] = jnp.where(lead, tail, head)


def inner_kernel(rows, dens, belief, bias, logits, bias_h, sems):
    copy = pltpu.make_async_copy(bias, bias_h, sems.at[0])
    copy.start()
    lane = lax.broadcasted_iota(jnp.int32, (1, LANES), 1)
    line = lax.broadcasted_iota(jnp.int32, (rows, 1), 0)
    for k in range(K - 1):
        for low in range(0, LANES, rows):
            here = belief[k, low : low + rows, :]
            total = dens[k, low : low + rows, :]
            if low > 0:
                total = total + belief[k, low - rows : low, :]
            if low + rows < LANES:
                total = total + belief[k, low + rows : low + 2 * rows, :]
            total = total + jnp.where(line > 0, pltpu.roll(here, 1, 0), 0.0)
            total = total + jnp.where(line < rows - 1, pltpu.roll(here, rows - 1, 0), 0.0)
            total = total + jnp.where(lane > 0, pltpu.roll(here, 1, 1), 0.0)
            total = total + jnp.where(lane < LANES - 1, pltpu.roll(here, LANES - 1, 1), 0.0)
            logits[k, low : low + rows, :] = total
    copy.wait()


def last_kernel(rows, inner, dens, own, up, down, side, edge, post_h, post, sems):
    slabs = LANES // rows
    lane = lax.broadcasted_iota(jnp.int32, (1, LANES), 1)
    line = lax.broadcasted_iota(jnp.int32, (rows, 1), 0)
    even = lanes_of(lax.rem(lax.axis_index("slab"), 2)) == 0
    left = lanes_of(lax.axis_index("col")) == 0
    bottom = lanes_of(lax.axis_index("slab")) == 0
    top = lanes_of(lax.axis_size("slab") - 1 - lax.axis_index("slab")) == 0
    spot = lane == jnp.where(left, LANES - 1, 0)
    face = line == jnp.where(lanes_of(lax.axis_index("row")) == 0, rows - 1, 0)
    copies = []
    for s in range(slabs):
        low, high = s * rows, (s + 1) * rows
        column = edge[low:high, :]
        column = jnp.where(left, column, pltpu.roll(column, 2, 1))
        logits = []
        for k in range(K - 1):
            total = inner[k, low:high, :]
            if s == 0:
                total = total + jnp.where(bottom, 0.0, jnp.where(even, down[k], up[k]))
            if s == slabs - 1:
                total = total + jnp.where(top, 0.0, jnp.where(even, up[k], down[k]))
            total = total + jnp.where(face, side[k, s : s + 1, :], 0.0)
            total = total + jnp.where(spot, pltpu.roll(column, LANES - 1 - k, 1), 0.0)
            logits.append(total)
        logits.append(dens[K - 1, low:high, :])
        inside = (own[M, low:high, :] < float(K)).astype(jnp.float32)
        for k, value in enumerate(soft(logits, inside)):
            post[k, low:high, :] = value.astype(jnp.bfloat16)
        span = pl.ds(low, rows)
        copies.append(
            pltpu.make_async_copy(post.at[:, span, :], post_h.at[:, span, :], sems.at[s])
        )
        copies[-1].start()
    for copy in copies:
        copy.wait()


def lanes_of(value):
    return jnp.full((1, LANES), value, jnp.int32)


class Pack(typing.NamedTuple):
    core: int
    wide: int
    code: int
    stat: int


def padded(rows):
    return -(-rows // SUB) * SUB


def call(kernel, outs, scratch=(), micros=1, far_out=()):
    vmem = pl.BlockSpec(memory_space=pltpu.VMEM)
    far = pl.BlockSpec(memory_space=pltpu.HBM)
    shapes = [jax.ShapeDtypeStruct(shape, kind) for shape, kind in outs]

    def run(*args):
        return pl.pallas_call(
            kernel,
            out_shape=shapes,
            in_specs=[vmem] * len(args),
            out_specs=[far if i in far_out else vmem for i in range(len(shapes))],
            scratch_shapes=[
                pltpu.VMEM(x, jnp.float32) if isinstance(x, tuple) else x for x in scratch
            ],
            compiler_params=pltpu.CompilerParams(vmem_limit_bytes=VMEM_BYTES),
            cost_estimate=pl.CostEstimate(
                flops=micros * 10_000_000, bytes_accessed=2**20, transcendentals=0
            ),
            name=(kernel.func if isinstance(kernel, functools.partial) else kernel).__name__,
        )(*args)

    return run


def both_ways(pairs, count):
    steps = []
    for i in range(count):
        other = [b if a == i else a for a, b in pairs if i in (a, b)]
        for side in range(2):
            target = other[0] * 2 + side if other else i * 2 + 1 - side
            steps.append((i * 2 + side, target))
    return steps


def pencils(image, brain_mask, labels):
    _, slabs, rows, columns = image.shape
    ns, nr, nc = (lax.axis_size(a) for a in ("slab", "row", "col"))
    grid = (ns, nr)
    peers = ns * nr
    core = columns // peers
    window = core + 2 * EDGE
    wide_rows = core + 4
    pack = Pack(core, wide_rows, M * wide_rows, M * wide_rows + core + 2)
    f32 = jnp.float32
    swap = [(0, 1), (1, 0)]

    taps = impulse(columns * nc)
    reach = np.arange(-MARGIN, columns + MARGIN)
    source = np.concatenate([np.arange(columns), np.arange(columns) + columns])
    spread = taps[(reach[:, None] - source[None, :]) % (columns * nc)]
    gather = table_of(spread[MARGIN : MARGIN + columns].T)
    spread = table_of(spread)
    slab_table = table_of(np.kron(dense(slabs * ns), np.eye(rows)))
    row_table = np.einsum(
        "arbq,st->asrbtq", dense(rows * nr).reshape(nr, rows, nr, rows), np.eye(slabs)
    )
    row_table = table_of(row_table.reshape(nr * LANES, nr * LANES))

    code = jnp.where(brain_mask > 0, labels, K).astype(f32)
    own = jnp.concatenate([image, code[None]]).reshape(M + 1, LANES, columns)
    image_o = lax.ppermute(image.reshape(M, LANES, columns), "col", swap)
    mask_o = lax.ppermute(brain_mask.reshape(LANES, columns), "col", swap)
    labels_o = lax.ppermute(labels.reshape(LANES, columns), "col", swap)

    def trade(x):
        return lax.all_to_all(x, ("row", "slab"), split_axis=0, concat_axis=0, tiled=True)

    turned, stat = call(
        own_kernel, [((M + 1, columns, LANES), f32), ((SUB, LANES), f32)]
    )(own)
    sent, rest, code_o = call(
        functools.partial(prepare_kernel, pack),
        [
            ((peers, padded(pack.stat + 1), LANES), f32),
            ((peers, SUB, LANES), f32),
            ((LANES, columns), f32),
        ],
        [(M + 1, columns + 2 * MARGIN, LANES)],
    )(turned, stat, image_o, mask_o, labels_o)
    raw = trade(sent)
    (sent,) = call(
        functools.partial(column_kernel, pack),
        [((peers, padded(pack.code + 4), LANES), f32)],
        [(M * LANES, 2 * columns), (columns + 2 * MARGIN, M * LANES)],
    )(own, image_o, code_o, raw, rest, spread)
    got = trade(sent)
    sent, keep = call(
        functools.partial(pencil_kernel, pack, grid, rows),
        [
            ((peers, padded((K - 1) * core + 1), LANES), f32),
            ((K, peers, core, LANES), f32),
        ],
        [
            (nr * M * window, ns * LANES),
            (ns * M * window, nr * LANES),
            (ns * M * window, nr * LANES),
            (peers, window, LANES),
            pltpu.VMEM((peers, window, LANES), jnp.int32),
            (peers, M, window, LANES),
            (K, peers, window, LANES),
            (K, peers, window, LANES),
            (K, peers, window, LANES),
        ],
        micros=4,
    )(got, raw, slab_table, row_table)
    near = trade(sent)
    stat_a = jnp.sum(near[:, (K - 1) * core : (K - 1) * core + 1, :], axis=0)
    stat_b = lax.ppermute(stat_a, "col", swap)
    (sent,) = call(
        functools.partial(residual_kernel, pack, grid),
        [((peers, M * core, LANES), f32)],
        [(nr * M * core, ns * LANES), (ns * M * core, nr * LANES)],
    )(stat_a, stat_b, keep, raw, slab_table, row_table)
    got = trade(sent)
    yours = lax.ppermute(got, "col", swap)
    field, near = call(
        half_kernel, [((M, LANES, columns), f32), ((K - 1, LANES, columns), f32)]
    )(got, near, gather)
    bias, centers, dens, belief, up, down, side, edge = call(
        functools.partial(third_kernel, rows),
        [
            ((M, LANES, columns), f32),
            ((K, M), f32),
            ((K, LANES, columns), f32),
            ((K - 1, LANES, columns), f32),
            ((K - 1, rows, columns), f32),
            ((K - 1, rows, columns), f32),
            ((K - 1, slabs, columns), f32),
            ((LANES, LANES), f32),
        ],
        micros=2,
    )(field, yours, near, own, stat_a, stat_b, gather)
    pairs = [(i, i + 1) for i in range(0, ns - 1, 2)]
    between = [(i, i + 1) for i in range(1, ns - 1, 2)]
    up = lax.ppermute(up, ("slab", "col"), both_ways(pairs, ns))
    down = lax.ppermute(down, ("slab", "col"), both_ways(between, ns))
    side = lax.ppermute(side, "row", swap)
    edge = lax.ppermute(edge, "col", swap)
    inner, bias = call(
        functools.partial(inner_kernel, rows),
        [((K - 1, LANES, columns), f32), ((M, LANES, columns), f32)],
        [pltpu.SemaphoreType.DMA((1,))],
        far_out=(1,),
    )(dens, belief, bias)
    (post,) = call(
        functools.partial(last_kernel, rows),
        [((K, LANES, columns), jnp.bfloat16)],
        [
            pltpu.VMEM((K, LANES, columns), jnp.bfloat16),
            pltpu.SemaphoreType.DMA((slabs,)),
        ],
        far_out=(0,),
    )(inner, dens, own, up, down, side, edge)
    shape = (slabs, rows, columns)
    return post.reshape((K,) + shape), bias.reshape((M,) + shape), centers


def local(image, brain_mask, labels):
    _, slabs, rows, columns = image.shape
    peers = lax.axis_size("slab") * lax.axis_size("row")
    fits = slabs * rows == LANES and columns == LANES and slabs % SUB == 0 and rows % SUB == 0
    fits = fits and lax.axis_size("row") == 2 and lax.axis_size("col") == 2
    fits = fits and columns % (SUB * peers) == 0
    return (pencils if fits else general)(image, brain_mask, labels)


def solution(mesh):
    placed = (
        P(None, ("grp", "slab"), "row", "col"),
        P(("grp", "slab"), "row", "col"),
        P(("grp", "slab"), "row", "col"),
    )
    return jax.shard_map(
        local,
        mesh=mesh,
        in_specs=placed,
        out_specs=(
            P(None, ("grp", "slab"), "row", "col"),
            P(None, ("grp", "slab"), "row", "col"),
            P("grp", None),
        ),
        check_vma=False,
    )
```
